32 devices in a mesh: slab: 8 (over z, y), sub: 4 (over x, core).
Axes of the slice: x: 2, y: 2, z: 4, core: 2. Of those that a mesh axis runs over, the one named last changes fastest.
Arguments:
- orbitals: bfloat16 [32, 16, 110592], P(('slab', 'sub')), may hold values from -0.25 to 0.25
- occupations: int32 [32, 16], P(('slab', 'sub')), may hold values from 0 to 2, as said below
- patch_sign: int32 [32], P(('slab', 'sub')), may hold values from -1 to 1, as said below
- corners: int32 [32, 3], replicated, may hold values from 0 to 255, as said below
- core_span: int32 [32, 6], P(('slab', 'sub')), may hold values from 8 to 32, as said below
- outer_density: float32 [32, 256, 256], P('slab', 'sub'), may hold values from 0 to 0.3, as said below
Outputs:
- box_potential: float32 [32, 110592], P(('slab', 'sub'))
- potential: float32 [32, 256, 256], P('slab', 'sub')
The draws below stay inside these ranges and needn't reach their ends.
Inputs may be any that keep to these rules, and one draw needn't show every extreme that they name: Each fragment's occupations sum to 16. patch_sign[f] is -1 raised to the number of dimensions along which fragment f's core is 16 cells long. corners[f, 0] lies in [4 * (f // 4), that + 4), the planes of the slab index that holds fragment f; corners[f, 1] lies in [0, 256) and corners[f, 2] in [0, 256). `core_span`: each core lies inside its box and is 16 or 32 cells long along each dimension; fragments 8 j to 8 j + 7 are the eight kinds of core that start at one common grid cell, a corner of the fragment division; along the second and third dimensions these corners lie at different points of one lattice of spacing 16. `outer_density`: nonnegative; zero exactly on the cells where the fragments given here have signed coverage one.
All inputs are finite; a program needn't handle non-finite values.
Results may differ from the reference program's by a relative error of at most 0.0003.
Values sent between devices are 32-bit elements; how exact they have to be, the bound alone decides.
No kernel may reach another device: no remote copies, remote signals or barrier semaphores. Data moves between devices by JAX's collectives and lax.ppermute only.
A program may use at most 64 MiB of HBM per device.

```python
import math
import jax
import jax.numpy as jnp
from jax import lax

BOX = 48
ORB = 16
NX = 256
NY = 256
Z_DEV = 4
NZ = 32
FRAGS = 32


def fragment_layout(key):
    base = jax.random.fold_in(key, 11)
    keys = jax.random.split(base, 4)
    piece = BOX // 3
    half = piece // 2
    pairs = FRAGS // 8
    pair_index = jnp.arange(pairs, dtype=jnp.int32)
    upper = Z_DEV * (2 * pair_index + 1) + jax.random.randint(keys[0], (pairs,), 0, Z_DEV, dtype=jnp.int32)
    across = NY // piece
    slots = jax.random.permutation(keys[1], NX // piece * across)[:pairs].astype(jnp.int32)
    offsets = jax.random.randint(keys[2], (2,), 0, piece, dtype=jnp.int32)
    core_x = slots // across * piece + offsets[0]
    core_y = slots % across * piece + offsets[1]
    kind_keys = jax.random.split(keys[3], FRAGS // 4)
    orders = jax.vmap(lambda k: jax.random.permutation(k, 4))(kind_keys).astype(jnp.int32).reshape(FRAGS)
    fragment = jnp.arange(FRAGS, dtype=jnp.int32)
    slab_index = fragment // 4
    owner = slab_index // 2
    thick_z = 1 + slab_index % 2
    thick_x = 1 + orders // 2
    thick_y = 1 + orders % 2
    start_z = jnp.where(thick_z == 2, upper[owner], upper[owner] - Z_DEV)
    first_z = jnp.where(thick_z == 2, half, half + Z_DEV)
    first_x = jnp.where(thick_x == 2, half, piece)
    first_y = jnp.where(thick_y == 2, half, piece)
    start_x = (core_x[owner] - first_x) % NX
    start_y = (core_y[owner] - first_y) % NY
    signs = (2 * thick_z - 3) * (2 * thick_x - 3) * (2 * thick_y - 3)
    corner_table = jnp.stack([start_z, start_x, start_y], axis=1).astype(jnp.int32)
    span_table = jnp.stack([first_z, first_x, first_y, piece * thick_z, piece * thick_x, piece * thick_y], axis=1).astype(jnp.int32)
    return (corner_table, span_table, signs.astype(jnp.int32), upper + half, core_x, core_y)


def draw_corners(key, part):
    return fragment_layout(key)[0]


def draw_core_span(key, part):
    return fragment_layout(key)[1]


def draw_patch_sign(key, part):
    return fragment_layout(key)[2]


def draw_occupations(key, part):
    keys = jax.random.split(jax.random.fold_in(key, 23), FRAGS + 1)
    ranks = jax.vmap(lambda k: jax.random.permutation(k, ORB))(keys[:FRAGS]).astype(jnp.int32)
    doubled = jax.random.randint(keys[FRAGS], (FRAGS, 1), 1, ORB // 2 + 1, dtype=jnp.int32)
    filled = jnp.where(ranks < doubled, 2, jnp.where(ranks < 2 * doubled, 0, 1))
    return filled.astype(jnp.int32)


def cover_factor(first, count, piece):
    cells = jnp.arange(count, dtype=jnp.int32)
    distance = (cells[None, :] - first[:, None]) % count

    def hits(length):
        return jnp.where(distance < length, (length - 1 - distance) // count + 1, 0)
    return (hits(2 * piece) - hits(piece)).astype(jnp.float32)


def draw_outer_density(key, part):
    layout = fragment_layout(key)
    piece = BOX // 3
    pairs = FRAGS // 8
    factor_z = cover_factor(layout[3], NZ, piece)
    factor_x = cover_factor(layout[4], NX, piece)
    factor_y = cover_factor(layout[5], NY, piece)
    plane = (factor_x[:, :, None] * factor_y[:, None, :]).reshape(pairs, NX * NY)
    coverage = jnp.dot(factor_z.T, plane).reshape(NZ, NX, NY)
    noise_key = jax.random.fold_in(key, 31)
    values = 0.0256 * jnp.exp(0.6 * jnp.clip(jax.random.normal(noise_key, (NZ, NX, NY), jnp.float32), -4.0, 4.0))
    return (values * (1.0 - coverage)).astype(jnp.float32)


def level_of(own_key, extent, cuts, low, top_value):
    factor_of, own = 1.0, jax.random.fold_in(own_key, 6)
    for dim, blocks in cuts:
        steps = jnp.exp(jax.random.uniform(jax.random.fold_in(own, dim), (blocks,), jnp.float32, low / len(cuts), top_value / len(cuts)))
        factor_of = factor_of * jnp.repeat(steps, extent[dim] // blocks).reshape([-1 if axis == dim else 1 for axis in range(len(extent))])
    return factor_of


def centred(rng, shape, width, limit, pieces=(), kind=jnp.bfloat16):
    level = level_of(rng, shape, pieces, -0.22, 0.18) if pieces else 1.0
    values = jax.random.normal(rng, shape, jnp.float32) * width * level
    return jnp.minimum(jnp.maximum(values, -limit), limit).astype(kind)


def setup_inputs(seed: int = 0) -> dict:
    seeds = jax.random.split(jax.random.key(seed), 7)
    return {
        "orbitals": centred(seeds[0], (FRAGS, ORB, BOX * BOX * BOX), 0.04, 0.25, ((0, 32),)),
        "occupations": draw_occupations(jax.random.fold_in(seeds[6], 71), 0),
        "patch_sign": draw_patch_sign(jax.random.fold_in(seeds[6], 71), 0),
        "corners": draw_corners(jax.random.fold_in(seeds[6], 71), 0),
        "core_span": draw_core_span(jax.random.fold_in(seeds[6], 71), 0),
        "outer_density": draw_outer_density(jax.random.fold_in(seeds[6], 71), 0),
    }


spacing = 0.35
floor_density = 0.001


def wave_squares(index, count):
    folded = jnp.where(index > count // 2, index - count, index)
    wave = (2.0 * math.pi / (count * spacing)) * folded.astype(jnp.float32)
    return wave * wave


def exchange_correlation(density):
    clipped = jnp.maximum(density, floor_density)
    radius = jnp.cbrt(3.0 / (4.0 * math.pi * clipped))
    exchange = -jnp.cbrt(3.0 * clipped / math.pi)
    correlation = -0.44 / (radius + 7.8) - 0.44 * radius / (3.0 * (radius + 7.8) ** 2)
    return exchange + correlation


def reference(orbitals, occupations, patch_sign, corners, core_span, outer_density):
    copies = (BOX - 1) // NZ + 2
    cell = jnp.arange(BOX, dtype=jnp.int32)

    def add_box(fragment, grid):
        fragment = fragment.astype(jnp.int32)
        orbital_values = orbitals[fragment].astype(jnp.float32)
        weights = occupations[fragment].astype(jnp.float32)
        box_density = patch_sign[fragment].astype(jnp.float32) * jnp.sum(weights[:, None] * orbital_values * orbital_values, axis=0)
        span = core_span[fragment].astype(jnp.int32)
        inside_z = (cell >= span[0]) & (cell < span[0] + span[3])
        inside_x = (cell >= span[1]) & (cell < span[1] + span[4])
        inside_y = (cell >= span[2]) & (cell < span[2] + span[5])
        inside = (inside_z[:, None, None] & inside_x[None, :, None] & inside_y[None, None, :]).astype(jnp.float32)
        cube = box_density.reshape(BOX, BOX, BOX) * inside
        planes = jnp.pad(cube, ((0, 0), (0, NX - BOX), (0, NY - BOX)))
        planes = jnp.roll(planes, corners[fragment, 1], axis=1)
        planes = jnp.roll(planes, corners[fragment, 2], axis=2)
        start_z = corners[fragment, 0].astype(jnp.int32)
        current = lax.dynamic_slice_in_dim(grid, start_z, BOX, 0)
        return lax.dynamic_update_slice_in_dim(grid, current + planes, start_z, 0)

    extended = lax.fori_loop(0, FRAGS, add_box, jnp.zeros((copies * NZ, NX, NY), jnp.float32))
    density = jnp.sum(extended.reshape(copies, NZ, NX, NY), axis=0) + outer_density
    square = (wave_squares(jnp.arange(NZ, dtype=jnp.int32), NZ)[:, None, None]
              + wave_squares(jnp.arange(NX, dtype=jnp.int32), NX)[None, :, None]
              + wave_squares(jnp.arange(NY, dtype=jnp.int32), NY)[None, None, :])
    safe_square = jnp.where(square > 0, square, 1.0)
    kernel = jnp.where(square > 0, 4.0 * math.pi / safe_square, 0.0)
    spectrum = jnp.fft.fftn(density)
    hartree = jnp.real(jnp.fft.ifftn(spectrum * kernel)).astype(jnp.float32)
    potential = hartree + exchange_correlation(density)
    tiled = jnp.concatenate([potential] * copies, axis=0)

    def cut_box(fragment):
        start_z = corners[fragment, 0].astype(jnp.int32)
        planes = lax.dynamic_slice_in_dim(tiled, start_z, BOX, 0)
        planes = jnp.roll(planes, -corners[fragment, 1], axis=1)
        planes = jnp.roll(planes, -corners[fragment, 2], axis=2)
        return planes[:, :BOX, :BOX].reshape(BOX * BOX * BOX)

    boxes = lax.map(cut_box, jnp.arange(FRAGS, dtype=jnp.int32))
    return boxes, potential
```

```python
import math

import jax
import jax.numpy as jnp
import numpy as np
from jax import lax
from jax.experimental import pallas as pl
from jax.experimental.pallas import tpu as pltpu
from jax.sharding import PartitionSpec as P

BOX = 48
CORE = 32
PLANE = BOX * BOX
GROUPS = 6
WIDE = PLANE // GROUPS
PACK = CORE * CORE
LANES = 128
PIECE = PACK + LANES
KINDS = 8

spacing = 0.35
floor_density = 0.001

AXES = ("slab", "sub")


def exchange_correlation(density):
    clipped = jnp.maximum(density, floor_density)
    radius = jnp.cbrt(3.0 / (4.0 * math.pi * clipped))
    exchange = -jnp.cbrt(3.0 * clipped / math.pi)
    correlation = -0.44 / (radius + 7.8) - 0.44 * radius / (3.0 * (radius + 7.8) ** 2)
    return exchange + correlation


def split_table(table):
    high = table.astype(np.float32).astype(jnp.bfloat16)
    low = (table - high.astype(np.float64)).astype(np.float32).astype(jnp.bfloat16)
    return np.stack([high, low])


def hartley(count, repeat=1):
    index = np.arange(count)
    angle = 2.0 * np.pi / count * (np.outer(index, index) % count)
    return split_table(np.kron(np.cos(angle) + np.sin(angle), np.eye(repeat)))


def parts(values):
    high = values.astype(jnp.bfloat16)
    low = (values - high.astype(jnp.float32)).astype(jnp.bfloat16)
    return high, low


def product(a, b):
    return jnp.dot(a, b, preferred_element_type=jnp.float32)


def table_times(table, values):
    high, low = parts(values)
    return product(table[0], high) + (product(table[0], low) + product(table[1], high))


def times_table(values, table):
    high, low = parts(values)
    return product(high, table[0]) + (product(high, table[1]) + product(low, table[0]))


def core_kernel(place, weights, orbitals, out, sums, rows):
    depth, base, slots = place[0], place[1], out.shape[0]
    first_z, first_x, first_y = place[2], place[3], place[4]
    len_z, len_x, len_y = place[5], place[6], place[7]
    start_z, start_x, start_y = place[8], place[9], place[10]
    weight = weights[...]

    def add_plane(p, carry):
        i = jnp.minimum(first_z + p, BOX - 1)
        values = orbitals[0, :, pl.ds(pl.multiple_of(i * PLANE, LANES), PLANE)].astype(jnp.float32)
        total = jnp.sum(values * values * weight, axis=0, keepdims=True)
        for g in range(GROUPS):
            sums[pl.ds(p * GROUPS + g, 1), :] = total[:, g * WIDE : (g + 1) * WIDE]
        return carry

    lax.fori_loop(0, CORE, add_plane, 0)
    count = CORE * GROUPS
    for r in range(8):
        rows[pl.ds(r, count, stride=8), 0:BOX] = sums[:, r * BOX : (r + 1) * BOX]

    row = lax.broadcasted_iota(jnp.int32, (8, LANES), 0)
    lane = lax.broadcasted_iota(jnp.int32, (8, LANES), 1)

    def pack(k, carry):
        p = lax.rem(base + k - start_z + 2 * depth, depth)
        held = p < len_z
        p = jnp.minimum(p, CORE - 1)
        cells = rows[pl.ds(p * BOX + first_x, CORE), :]
        packed = jnp.zeros((8, LANES), jnp.float32)
        for q in range(4):
            turned = pltpu.roll(cells[8 * q : 8 * q + 8], lax.rem(32 * q - first_y + LANES, LANES), 1)
            keep = (row + 8 * q < len_x) & (lane >= 32 * q) & (lane < 32 * q + len_y) & held
            packed = jnp.where(keep, turned, packed)
        for s in range(8):
            out[k, :, s * LANES : (s + 1) * LANES] = packed[s : s + 1]
        first = jnp.where(lane[0:1] == 0, start_x, start_y)
        out[k, :, PACK:PIECE] = first.astype(jnp.float32)
        return carry

    lax.fori_loop(0, slots, pack, 0)


def core_pieces(orbitals, weights, place, slots):
    return pl.pallas_call(
        core_kernel,
        out_shape=jax.ShapeDtypeStruct((slots, 1, PIECE), jnp.float32),
        in_specs=[
            pl.BlockSpec(memory_space=pltpu.SMEM),
            pl.BlockSpec(memory_space=pltpu.VMEM),
            pl.BlockSpec(memory_space=pltpu.VMEM),
        ],
        out_specs=pl.BlockSpec(memory_space=pltpu.VMEM),
        scratch_shapes=[
            pltpu.VMEM((CORE * GROUPS, WIDE), jnp.float32),
            pltpu.VMEM((CORE * BOX + CORE, LANES), jnp.float32),
        ],
        cost_estimate=pl.CostEstimate(flops=40_000_000, bytes_accessed=4_000_000, transcendentals=0),
        name="core_pieces",
    )(place, weights, orbitals)


def plane_kernel(group, pieces, outer, table_x, table_y, spectrum, density, packed):
    slots = pieces.shape[0]
    count_x, count_y = outer.shape
    groups = slots // group
    column = lax.broadcasted_iota(jnp.int32, (count_x, CORE), 1)
    cell_x = lax.broadcasted_iota(jnp.int32, (count_x, CORE), 0)
    row = lax.broadcasted_iota(jnp.int32, (CORE, count_y), 0)
    cell_y = lax.broadcasted_iota(jnp.int32, (CORE, count_y), 1)
    lefts, rights = [], []
    for j in range(groups):
        total = pieces[j * group, :, 0:PACK]
        for m in range(1, group):
            total = total + pieces[j * group + m, :, 0:PACK]
        for s in range(8):
            packed[8 * j + s : 8 * j + s + 1, :] = total[:, s * LANES : (s + 1) * LANES]
        tile = packed[8 * j : 8 * j + 8, :]
        square = jnp.concatenate([tile[:, 32 * q : 32 * q + 32] for q in range(4)], axis=0)
        first = pieces[j * group, :, PACK : PACK + LANES].astype(jnp.int32)
        away_x = cell_x - first[:, 0:1]
        away_y = cell_y - first[:, 1:2]
        left = jnp.where(away_x < 0, away_x + count_x, away_x) == column
        right = jnp.where(away_y < 0, away_y + count_y, away_y) == row
        right = jnp.where(right, 1.0, 0.0).astype(jnp.bfloat16)
        high = square.astype(jnp.bfloat16)
        rest = square - high.astype(jnp.float32)
        middle = rest.astype(jnp.bfloat16)
        low = (rest - middle.astype(jnp.float32)).astype(jnp.bfloat16)
        lefts.append(jnp.where(left, 1.0, 0.0).astype(jnp.bfloat16))
        rights.append([product(part, right).astype(jnp.bfloat16) for part in (high, middle, low)])
    left = jnp.concatenate(lefts, axis=1)
    placed = outer[...]
    for part in range(2, -1, -1):
        placed = placed + product(left, jnp.concatenate([r[part] for r in rights], axis=0))
    density[...] = placed
    spectrum[...] = times_table(table_times(table_x, placed), table_y)


def plane_spectrum(pieces, group, outer, table_x, table_y):
    shape = jax.ShapeDtypeStruct(outer.shape, jnp.float32)
    return pl.pallas_call(
        lambda *refs: plane_kernel(group, *refs),
        out_shape=(shape, shape),
        in_specs=[pl.BlockSpec(memory_space=pltpu.VMEM)] * 4,
        out_specs=(pl.BlockSpec(memory_space=pltpu.VMEM),) * 2,
        scratch_shapes=[pltpu.VMEM((8 * (pieces.shape[0] // group), LANES), jnp.float32)],
        name="plane_spectrum",
    )(pieces, outer, table_x, table_y)


def wave_squares(index, count):
    folded = jnp.where(index > count // 2, index - count, index)
    wave = 2.0 * math.pi / (count * spacing) * folded.astype(jnp.float32)
    return wave * wave


def column_kernel(count_z, count_x, count_y, device, values, table, out):
    rows, lanes = values.shape
    deep = rows // count_z
    transformed = table_times(table, values[...])
    row = lax.broadcasted_iota(jnp.int32, (rows, lanes), 0)
    lane = lax.broadcasted_iota(jnp.int32, (rows, lanes), 1)
    cell = (device[0] * deep + row % deep) * lanes + lane
    square = (
        wave_squares(row // deep, count_z)
        + wave_squares(cell // count_y, count_x)
        + wave_squares(cell % count_y, count_y)
    )
    scale = 4.0 * math.pi / float(count_z * count_x * count_y)
    kernel = jnp.where(square > 0, scale / jnp.where(square > 0, square, 1.0), 0.0)
    out[...] = table_times(table, transformed * kernel)


def column_hartree(values, table, device, counts):
    return pl.pallas_call(
        lambda *refs: column_kernel(*counts, *refs),
        out_shape=jax.ShapeDtypeStruct(values.shape, jnp.float32),
        in_specs=[
            pl.BlockSpec(memory_space=pltpu.SMEM),
            pl.BlockSpec(memory_space=pltpu.VMEM),
            pl.BlockSpec(memory_space=pltpu.VMEM),
        ],
        out_specs=pl.BlockSpec(memory_space=pltpu.VMEM),
        name="column_hartree",
    )(device, values, table)


def window_kernel(corners, spectrum, exchange, table_x, table_y, potential, out, wide, cut):
    slots = out.shape[0]
    count_x, count_y = spectrum.shape
    plane = times_table(table_times(table_x, spectrum[...]), table_y) + exchange[...]
    potential[...] = plane
    tall = count_x + BOX
    tiles = count_y // LANES
    for t in range(tiles):
        part = plane[:, t * LANES : (t + 1) * LANES]
        wide[t * tall : t * tall + count_x, :] = part
        wide[t * tall + count_x : (t + 1) * tall, :] = part[0:BOX]
    lane = lax.broadcasted_iota(jnp.int32, (BOX, LANES), 1)

    def cut_window(k, carry):
        x, y = corners[k, 0], corners[k, 1]
        tile = y // LANES
        over = y - tile * LANES
        near = wide[pl.ds(tile * tall + x, BOX), :]
        far = wide[pl.ds(lax.rem(tile + 1, tiles) * tall + x, BOX), :]
        turned = pltpu.roll(jnp.where(lane < over, far, near), lax.rem(LANES - over, LANES), 1)
        cut[pl.ds(pl.multiple_of(k * BOX, 8), BOX), :] = turned
        return carry

    lax.fori_loop(0, slots, cut_window, 0)
    count = slots * GROUPS
    flat = jnp.concatenate(
        [cut[pl.ds(r, count, stride=8), :][:, 0:BOX] for r in range(8)], axis=1
    )
    for k in range(slots):
        for g in range(GROUPS):
            out[k, :, g * WIDE : (g + 1) * WIDE] = flat[k * GROUPS + g : k * GROUPS + g + 1, :]


def plane_windows(spectrum, exchange, table_x, table_y, corners):
    slots = corners.shape[0]
    count_x, count_y = spectrum.shape
    return pl.pallas_call(
        window_kernel,
        out_shape=(
            jax.ShapeDtypeStruct(spectrum.shape, jnp.float32),
            jax.ShapeDtypeStruct((slots, 1, PLANE), jnp.float32),
        ),
        in_specs=[pl.BlockSpec(memory_space=pltpu.SMEM)]
        + [pl.BlockSpec(memory_space=pltpu.VMEM)] * 4,
        out_specs=(pl.BlockSpec(memory_space=pltpu.VMEM),) * 2,
        scratch_shapes=[
            pltpu.VMEM((count_y // LANES * (count_x + BOX), LANES), jnp.float32),
            pltpu.VMEM((slots * BOX, LANES), jnp.float32),
        ],
        name="plane_windows",
    )(corners, spectrum, exchange, table_x, table_y)


def box_kernel(first, windows, out):
    depth = windows.shape[0]

    def copy_plane(i, carry):
        z = lax.rem(first[0] + i, depth)
        out[i] = windows[z]
        return carry

    lax.fori_loop(0, BOX, copy_plane, 0)


def box_planes(windows, first):
    return pl.pallas_call(
        box_kernel,
        out_shape=jax.ShapeDtypeStruct((BOX, 1, PLANE), jnp.float32),
        in_specs=[pl.BlockSpec(memory_space=pltpu.SMEM), pl.BlockSpec(memory_space=pltpu.VMEM)],
        out_specs=pl.BlockSpec(memory_space=pltpu.VMEM),
        name="box_planes",
    )(first, windows)


def body(orbitals, occupations, patch_sign, corners, core_span, outer_density):
    slab_count = lax.axis_size("slab")
    sub_count = lax.axis_size("sub")
    devices = slab_count * sub_count
    z_dev, x_dev, count_y = outer_density.shape
    count_x = x_dev * sub_count
    count_z = z_dev * slab_count
    device = lax.axis_index("slab") * sub_count + lax.axis_index("sub")
    table_x = hartley(count_x)
    table_y = hartley(count_y)
    per_device = count_x * count_y // devices
    deep = max(1, per_device // count_y)
    table_z = hartley(count_z, deep)

    own = lax.dynamic_index_in_dim(corners, device, 0, False)
    span = core_span[0]
    start = (own + span[:3]) % jnp.array([count_z, count_x, count_y], jnp.int32)
    place = jnp.concatenate([jnp.array([count_z, 0], jnp.int32), span, start])
    weights = (occupations[0] * patch_sign[0]).astype(jnp.float32)
    weights = jnp.broadcast_to(weights[:, None], (weights.shape[0], 1))

    outer = lax.all_to_all(outer_density, "sub", 0, 0, tiled=True).reshape(count_x, count_y)
    pieces = core_pieces(orbitals, weights, place, devices)
    pieces = lax.all_to_all(pieces, AXES, 0, 0, tiled=True)
    spectrum, density = plane_spectrum(pieces, KINDS, outer, table_x, table_y)
    chunk = (devices, deep, per_device // deep)
    spectrum = lax.all_to_all(spectrum.reshape(chunk), AXES, 0, 0, tiled=True)
    exchange = exchange_correlation(density)
    spectrum = column_hartree(
        spectrum.reshape(devices * deep, per_device // deep),
        table_z,
        jnp.reshape(device, (1,)),
        (count_z, count_x, count_y),
    )
    spectrum = lax.all_to_all(spectrum.reshape(chunk), AXES, 0, 0, tiled=True)
    potential, windows = plane_windows(
        spectrum.reshape(count_x, count_y), exchange, table_x, table_y, corners[:, 1:3]
    )
    windows = lax.all_to_all(windows, AXES, 0, 0, tiled=True)
    potential = lax.all_to_all(potential.reshape(z_dev, x_dev, count_y), "sub", 0, 0, tiled=True)
    box = box_planes(windows, own[0:1])
    return (box.reshape(1, BOX * PLANE), potential)


def solution(mesh):
    placed = (
        P(("slab", "sub"), None, None),
        P(("slab", "sub"), None),
        P(("slab", "sub")),
        P(),
        P(("slab", "sub"), None),
        P("slab", "sub", None),
    )
    return jax.shard_map(
        body,
        mesh=mesh,
        in_specs=placed,
        out_specs=(P(("slab", "sub"), None), P("slab", "sub", None)),
        check_vma=False,
    )
```

```python
import math

import jax
import jax.numpy as jnp
import numpy as np
from jax import lax
from jax.experimental import pallas as pl
from jax.experimental.pallas import tpu as pltpu
from jax.sharding import PartitionSpec as P

BOX = 48
CORE = 32
PLANE = BOX * BOX
GROUPS = 6
WIDE = PLANE // GROUPS
PACK = CORE * CORE
LANES = 128
PIECE = PACK + LANES
KINDS = 8

spacing = 0.35
floor_density = 0.001

AXES = ("slab", "sub")


def exchange_correlation(density):
    clipped = jnp.maximum(density, floor_density)
    radius = jnp.cbrt(3.0 / (4.0 * math.pi * clipped))
    exchange = -jnp.cbrt(3.0 * clipped / math.pi)
    correlation = -0.44 / (radius + 7.8) - 0.44 * radius / (3.0 * (radius + 7.8) ** 2)
    return exchange + correlation


def split_table(table):
    high = table.astype(np.float32).astype(jnp.bfloat16)
    low = (table - high.astype(np.float64)).astype(np.float32).astype(jnp.bfloat16)
    return np.stack([high, low])


def hartley(count, repeat=1):
    index = np.arange(count)
    angle = 2.0 * np.pi / count * (np.outer(index, index) % count)
    return split_table(np.kron(np.cos(angle) + np.sin(angle), np.eye(repeat)))


def parts(values):
    high = values.astype(jnp.bfloat16)
    low = (values - high.astype(jnp.float32)).astype(jnp.bfloat16)
    return high, low


def product(a, b):
    return jnp.dot(a, b, preferred_element_type=jnp.float32)


def table_times(table, values):
    high, low = parts(values)
    return product(table[0], high) + (product(table[0], low) + product(table[1], high))


def times_table(values, table):
    high, low = parts(values)
    return product(high, table[0]) + (product(high, table[1]) + product(low, table[0]))


def small_call(kernel, name, megabytes, **kwargs):
    limit = pltpu.CompilerParams(vmem_limit_bytes=megabytes * 2**20)
    return pl.pallas_call(kernel, compiler_params=limit, name=name, **kwargs)


def in_vmem(count):
    return [pl.BlockSpec(memory_space=pltpu.VMEM)] * count


def in_smem(count):
    return [pl.BlockSpec(memory_space=pltpu.SMEM)] * count


def anywhere(count):
    return [pl.BlockSpec(memory_space=pl.ANY)] * count


def row_sums(tiles):
    row = lax.broadcasted_iota(jnp.int32, (8, LANES), 0)
    top = row < 4
    fours = [
        jnp.where(top, tiles[i], tiles[i + 4])
        + pltpu.roll(jnp.where(top, tiles[i + 4], tiles[i]), 4, 0)
        for i in range(4)
    ]
    for step in (2, 1):
        early = (row % (2 * step)) < step
        fours = [
            jnp.where(
                early,
                fours[i] + pltpu.roll(fours[i], 8 - step, 0),
                fours[i + step] + pltpu.roll(fours[i + step], step, 0),
            )
            for i in range(step)
        ]
    return fours[0]


CHUNK = 8
UNROLL = 4


def core_kernel(
    base, depth, count_x, count_y, device, corners, span, occupations, sign, orbitals, out,
    buffer, sums, rows, arrived,
):
    own, slots, orbital_count = device[0], out.shape[0], orbitals.shape[1]
    first_z, first_x, first_y = span[0, 0], span[0, 1], span[0, 2]
    len_z, len_x, len_y = span[0, 3], span[0, 4], span[0, 5]
    begin = jnp.minimum(first_z, BOX - CORE)
    chunks = CORE // CHUNK
    copies = [
        pltpu.make_async_copy(
            orbitals.at[0, :, pl.ds(pl.multiple_of((begin + c * CHUNK) * PLANE, LANES), CHUNK * PLANE)],
            buffer.at[c],
            arrived.at[c],
        )
        for c in range(chunks)
    ]
    for copy in copies:
        copy.start()
    orbital = lax.broadcasted_iota(jnp.int32, (orbital_count, LANES), 0)
    weight = jnp.zeros((orbital_count, LANES), jnp.int32)
    for o in range(orbital_count):
        weight = jnp.where(orbital == o, occupations[0, o], weight)
    weight = (weight * sign[0]).astype(jnp.float32)
    groups = CHUNK * GROUPS // 8
    tiles = WIDE // LANES
    for c in range(chunks):
        copies[c].wait()

        def add_rows(b, carry, c=c):
            for q in range(tiles):
                cells = []
                for s in range(8):
                    lane = pl.multiple_of((8 * b + s) * WIDE + q * LANES, LANES)
                    values = buffer[c, :, pl.ds(lane, LANES)].astype(jnp.float32)
                    values = values * values * weight
                    cells.append(sum(values[8 * h : 8 * h + 8] for h in range(orbital_count // 8)))
                at = pl.multiple_of((c * groups + b) * 8, 8)
                sums[pl.ds(at, 8), q * LANES : (q + 1) * LANES] = row_sums(cells)
            return carry

        lax.fori_loop(0, groups, add_rows, 0)
    count = CORE * GROUPS
    for r in range(8):
        rows[pl.ds(r, count, stride=8), 0:BOX] = sums[:, r * BOX : (r + 1) * BOX]

    start_z = lax.rem(corners[0, own] + first_z, depth) - base(own)
    start_x = lax.rem(corners[1, own] + first_x, count_x)
    start_y = lax.rem(corners[2, own] + first_y, count_y)
    row = lax.broadcasted_iota(jnp.int32, (8, LANES), 0)
    lane = lax.broadcasted_iota(jnp.int32, (8, LANES), 1)
    first = jnp.where(lane[0:1] == 0, start_x, start_y).astype(jnp.float32)

    def pack(step, carry):
        turned = []
        for h in range(UNROLL):
            p = lax.rem(UNROLL * step + h - start_z + depth, depth)
            local = jnp.minimum(p + first_z - begin, CORE - 1)
            cells = rows[pl.ds(local * BOX + first_x, CORE), :]
            for q in range(4):
                turn = lax.rem(32 * q - first_y + LANES, LANES)
                turned.append(pltpu.roll(cells[8 * q : 8 * q + 8], turn, 1))
        for h in range(UNROLL):
            k = UNROLL * step + h
            held = lax.rem(k - start_z + depth, depth) < len_z
            packed = jnp.zeros((8, LANES), jnp.float32)
            for q in range(4):
                keep = (row + 8 * q < len_x) & (lane >= 32 * q) & (lane < 32 * q + len_y) & held
                packed = jnp.where(keep, turned[4 * h + q], packed)
            for s in range(8):
                out[k, :, s * LANES : (s + 1) * LANES] = packed[s : s + 1]
            out[k, :, PACK:PIECE] = first
        return carry

    lax.fori_loop(0, slots // UNROLL, pack, 0)


def core_pieces(device, corners, span, occupations, sign, orbitals, slots, base, counts):
    orbital_count = orbitals.shape[1]
    return small_call(
        lambda *refs: core_kernel(base, *counts, *refs),
        "core_pieces",
        8,
        out_shape=jax.ShapeDtypeStruct((slots, 1, PIECE), jnp.float32),
        in_specs=in_smem(5) + anywhere(1),
        out_specs=in_vmem(1)[0],
        scratch_shapes=[
            pltpu.VMEM((CORE // CHUNK, orbital_count, CHUNK * PLANE), orbitals.dtype),
            pltpu.VMEM((CORE * GROUPS, WIDE), jnp.float32),
            pltpu.VMEM((CORE * BOX + CORE, LANES), jnp.float32),
            pltpu.SemaphoreType.DMA((CORE // CHUNK,)),
        ],
        cost_estimate=pl.CostEstimate(flops=40_000_000, bytes_accessed=4_000_000, transcendentals=0),
    )(device, corners, span, occupations, sign, orbitals)


def plane_kernel(group, pieces, outer, table_x, table_y, spectrum, density, packed):
    slots = pieces.shape[0]
    count_x, count_y = outer.shape
    groups = slots // group
    column = lax.broadcasted_iota(jnp.int32, (count_x, CORE), 1)
    cell_x = lax.broadcasted_iota(jnp.int32, (count_x, CORE), 0)
    row = lax.broadcasted_iota(jnp.int32, (CORE, count_y), 0)
    cell_y = lax.broadcasted_iota(jnp.int32, (CORE, count_y), 1)
    lefts, rights = [], []
    for j in range(groups):
        total = pieces[j * group, :, 0:PACK]
        for m in range(1, group):
            total = total + pieces[j * group + m, :, 0:PACK]
        for s in range(8):
            packed[8 * j + s : 8 * j + s + 1, :] = total[:, s * LANES : (s + 1) * LANES]
        tile = packed[8 * j : 8 * j + 8, :]
        square = jnp.concatenate([tile[:, 32 * q : 32 * q + 32] for q in range(4)], axis=0)
        first = pieces[j * group, :, PACK : PACK + LANES].astype(jnp.int32)
        away_x = cell_x - first[:, 0:1]
        away_y = cell_y - first[:, 1:2]
        left = jnp.where(away_x < 0, away_x + count_x, away_x) == column
        right = jnp.where(away_y < 0, away_y + count_y, away_y) == row
        right = jnp.where(right, 1.0, 0.0).astype(jnp.bfloat16)
        high = square.astype(jnp.bfloat16)
        rest = square - high.astype(jnp.float32)
        middle = rest.astype(jnp.bfloat16)
        low = (rest - middle.astype(jnp.float32)).astype(jnp.bfloat16)
        lefts.append(jnp.where(left, 1.0, 0.0).astype(jnp.bfloat16))
        rights.append([product(part, right).astype(jnp.bfloat16) for part in (high, middle, low)])
    left = jnp.concatenate(lefts, axis=1)
    placed = outer[...]
    for part in range(2, -1, -1):
        placed = placed + product(left, jnp.concatenate([r[part] for r in rights], axis=0))
    density[...] = placed
    spectrum[...] = times_table(table_times(table_x, placed), table_y)


def plane_spectrum(pieces, group, outer, table_x, table_y):
    shape = jax.ShapeDtypeStruct(outer.shape, jnp.float32)
    return small_call(
        lambda *refs: plane_kernel(group, *refs),
        "plane_spectrum",
        12,
        out_shape=(shape, shape),
        in_specs=in_vmem(4),
        out_specs=in_vmem(2),
        scratch_shapes=[pltpu.VMEM((8 * (pieces.shape[0] // group), LANES), jnp.float32)],
    )(pieces, outer, table_x, table_y)


def wave_squares(index, count):
    folded = jnp.where(index > count // 2, index - count, index)
    wave = 2.0 * math.pi / (count * spacing) * folded.astype(jnp.float32)
    return wave * wave


def column_kernel(count_z, count_x, count_y, device, values, table, out):
    rows, lanes = values.shape
    deep = rows // count_z
    transformed = table_times(table, values[...])
    row = lax.broadcasted_iota(jnp.int32, (rows, lanes), 0)
    lane = lax.broadcasted_iota(jnp.int32, (rows, lanes), 1)
    cell = (device[0] * deep + row % deep) * lanes + lane
    square = (
        wave_squares(row // deep, count_z)
        + wave_squares(cell // count_y, count_x)
        + wave_squares(cell % count_y, count_y)
    )
    scale = 4.0 * math.pi / float(count_z * count_x * count_y)
    kernel = jnp.where(square > 0, scale / jnp.where(square > 0, square, 1.0), 0.0)
    out[...] = table_times(table, transformed * kernel)


def column_hartree(values, table, device, counts):
    return small_call(
        lambda *refs: column_kernel(*counts, *refs),
        "column_hartree",
        12,
        out_shape=jax.ShapeDtypeStruct(values.shape, jnp.float32),
        in_specs=in_smem(1) + in_vmem(2),
        out_specs=in_vmem(1)[0],
    )(device, values, table)


def window_kernel(fragment, device, corners, spectrum, exchange, table_x, table_y, *refs):
    *blocks, out, wide, cut = refs
    slots = out.shape[0]
    count_x, count_y = spectrum.shape
    x_dev = count_x // len(blocks)
    plane = times_table(table_times(table_x, spectrum[...]), table_y) + exchange[...]
    tall = count_x + BOX
    tiles = count_y // LANES
    for t in range(tiles):
        part = plane[:, t * LANES : (t + 1) * LANES]
        wide[t * tall : t * tall + count_x, :] = part
        wide[t * tall + count_x : (t + 1) * tall, :] = part[0:BOX]
    sub = lax.rem(device[0], len(blocks))
    for d, block in enumerate(blocks):
        for t in range(tiles):
            at = pl.multiple_of(t * tall + (sub ^ d) * x_dev, 8)
            block[:, t * LANES : (t + 1) * LANES] = wide[pl.ds(at, x_dev), :]
    lane = lax.broadcasted_iota(jnp.int32, (BOX, LANES), 1)

    def cut_windows(step, carry):
        turned = []
        for h in range(UNROLL):
            f = fragment(UNROLL * step + h, device[0])
            x, y = corners[1, f], corners[2, f]
            tile = y // LANES
            over = y - tile * LANES
            near = wide[pl.ds(tile * tall + x, BOX), :]
            far = wide[pl.ds(lax.rem(tile + 1, tiles) * tall + x, BOX), :]
            turn = lax.rem(LANES - over, LANES)
            turned.append(pltpu.roll(jnp.where(lane < over, far, near), turn, 1))
        for h in range(UNROLL):
            at = pl.multiple_of((UNROLL * step + h) * BOX, 8)
            cut[pl.ds(at, BOX), :] = turned[h]
        return carry

    lax.fori_loop(0, slots // UNROLL, cut_windows, 0)
    count = slots * GROUPS
    flat = jnp.concatenate(
        [cut[pl.ds(r, count, stride=8), :][:, 0:BOX] for r in range(8)], axis=1
    )
    for k in range(slots):
        for g in range(GROUPS):
            out[k, :, g * WIDE : (g + 1) * WIDE] = flat[k * GROUPS + g : k * GROUPS + g + 1, :]


def plane_windows(
    device, corners, spectrum, exchange, table_x, table_y, blocks, slots, fragment
):
    count_x, count_y = spectrum.shape
    block = jax.ShapeDtypeStruct((count_x // blocks, count_y), jnp.float32)
    return small_call(
        lambda *refs: window_kernel(fragment, *refs),
        "plane_windows",
        12,
        out_shape=[block] * blocks + [jax.ShapeDtypeStruct((slots, 1, PLANE), jnp.float32)],
        in_specs=in_smem(2) + in_vmem(4),
        out_specs=in_vmem(blocks + 1),
        scratch_shapes=[
            pltpu.VMEM((count_y // LANES * (count_x + BOX), LANES), jnp.float32),
            pltpu.VMEM((slots * BOX, LANES), jnp.float32),
        ],
    )(device, corners, spectrum, exchange, table_x, table_y)


def output_kernel(base, device, corners, windows, *refs):
    *blocks, box, potential, copied = refs
    depth = windows.shape[0]
    first = corners[0, device[0]] - base(device[0])
    sub = lax.rem(device[0], len(blocks))
    copies = [
        pltpu.make_async_copy(block, potential.at[sub ^ d], copied.at[BOX + d])
        for d, block in enumerate(blocks)
    ]
    for i in range(BOX):
        z = lax.rem(first + i, depth)
        copies.append(pltpu.make_async_copy(windows.at[z], box.at[i], copied.at[i]))
    for copy in copies:
        copy.start()
    for copy in copies:
        copy.wait()


def outputs(device, corners, windows, blocks, base):
    count = len(blocks)
    return small_call(
        lambda *refs: output_kernel(base, *refs),
        "outputs",
        4,
        out_shape=(
            jax.ShapeDtypeStruct((BOX, 1, PLANE), jnp.float32),
            jax.ShapeDtypeStruct((count,) + blocks[0].shape, jnp.float32),
        ),
        in_specs=in_smem(2) + anywhere(1 + count),
        out_specs=tuple(anywhere(2)),
        scratch_shapes=[pltpu.SemaphoreType.DMA((BOX + count,))],
    )(device, corners, windows, *blocks)


def body(orbitals, occupations, patch_sign, corners, core_span, outer_density):
    slab_count = lax.axis_size("slab")
    sub_count = lax.axis_size("sub")
    devices = slab_count * sub_count
    z_dev, x_dev, count_y = outer_density.shape
    count_x = x_dev * sub_count
    count_z = z_dev * slab_count
    device = lax.axis_index("slab") * sub_count + lax.axis_index("sub")
    table_x = hartley(count_x)
    table_y = hartley(count_y)
    per_device = count_x * count_y // devices
    deep = max(1, per_device // count_y)
    table_z = hartley(count_z, deep)

    device = jnp.reshape(device, (1,))
    assert z_dev == sub_count
    reach = (BOX + z_dev - 2) // z_dev + 1
    if slab_count <= reach:
        slots, group = devices, KINDS

        def base(own):
            return 0

        def fragment(slot, own):
            return slot

        def spread(pieces):
            return lax.all_to_all(pieces, AXES, 0, 0, tiled=True)

        collect = spread
    else:
        slots, group = reach * sub_count, sub_count

        def base(own):
            return own - lax.rem(own, sub_count)

        def fragment(slot, own):
            away = slot // sub_count * sub_count
            return lax.rem(base(own) - away + devices, devices) + lax.rem(slot, sub_count)

        def passed(pieces, sign):
            pieces = pieces.reshape((reach, sub_count) + pieces.shape[1:])
            pieces = lax.all_to_all(pieces, "sub", 1, 1, tiled=True)
            moved = [pieces[0]]
            for d in range(1, reach):
                ring = [(i, (i + sign * d) % slab_count) for i in range(slab_count)]
                moved.append(lax.ppermute(pieces[d], "slab", ring))
            return jnp.concatenate(moved, axis=0)

        def spread(pieces):
            return passed(pieces, 1)

        def collect(pieces):
            return passed(pieces, -1)

    corners, span, occupations, orbitals = (
        pltpu.with_memory_space_constraint(argument, pltpu.HBM)
        for argument in (corners.T, core_span, occupations, orbitals)
    )
    counts = (count_z, count_x, count_y)
    outer = lax.all_to_all(outer_density, "sub", 0, 0, tiled=True).reshape(count_x, count_y)
    pieces = core_pieces(
        device, corners, span, occupations, patch_sign, orbitals, slots, base, counts
    )
    pieces = spread(pieces)
    spectrum, density = plane_spectrum(pieces, group, outer, table_x, table_y)
    chunk = (devices, deep, per_device // deep)
    spectrum = lax.all_to_all(spectrum.reshape(chunk), AXES, 0, 0, tiled=True)
    exchange = exchange_correlation(density)
    spectrum = column_hartree(
        spectrum.reshape(devices * deep, per_device // deep), table_z, device, counts
    )
    spectrum = lax.all_to_all(spectrum.reshape(chunk), AXES, 0, 0, tiled=True)
    *blocks, windows = plane_windows(
        device,
        corners,
        spectrum.reshape(count_x, count_y),
        exchange,
        table_x,
        table_y,
        sub_count,
        slots,
        fragment,
    )
    blocks = [
        lax.ppermute(block, "sub", [(i, i ^ d) for i in range(sub_count)]) if d else block
        for d, block in enumerate(blocks)
    ]
    windows = collect(windows)
    box, potential = outputs(device, corners, windows, blocks, base)
    return (box.reshape(1, BOX * PLANE), potential)


def solution(mesh):
    placed = (
        P(("slab", "sub"), None, None),
        P(("slab", "sub"), None),
        P(("slab", "sub")),
        P(),
        P(("slab", "sub"), None),
        P("slab", "sub", None),
    )
    return jax.shard_map(
        body,
        mesh=mesh,
        in_specs=placed,
        out_specs=(P(("slab", "sub"), None), P("slab", "sub", None)),
        check_vma=False,
    )
```

```python
import math

import jax
import jax.numpy as jnp
import numpy as np
from jax import lax
from jax.experimental import pallas as pl
from jax.experimental.pallas import tpu as pltpu
from jax.sharding import PartitionSpec as P

BOX = 48
CORE = 32
PLANE = BOX * BOX
GROUPS = 6
WIDE = PLANE // GROUPS
PACK = CORE * CORE
LANES = 128
PIECE = PACK + LANES
KINDS = 8

spacing = 0.35
floor_density = 0.001

AXES = ("slab", "sub")


def exchange_correlation(density):
    clipped = jnp.maximum(density, floor_density)
    radius = jnp.cbrt(3.0 / (4.0 * math.pi * clipped))
    exchange = -jnp.cbrt(3.0 * clipped / math.pi)
    correlation = -0.44 / (radius + 7.8) - 0.44 * radius / (3.0 * (radius + 7.8) ** 2)
    return exchange + correlation


def split_table(table):
    high = table.astype(np.float32).astype(jnp.bfloat16)
    low = (table - high.astype(np.float64)).astype(np.float32).astype(jnp.bfloat16)
    return np.stack([high, low])


def hartley(count, repeat=1):
    index = np.arange(count)
    angle = 2.0 * np.pi / count * (np.outer(index, index) % count)
    return split_table(np.kron(np.cos(angle) + np.sin(angle), np.eye(repeat)))


def parts(values):
    high = values.astype(jnp.bfloat16)
    low = (values - high.astype(jnp.float32)).astype(jnp.bfloat16)
    return high, low


def product(a, b):
    return jnp.dot(a, b, preferred_element_type=jnp.float32)


def table_times(table, values):
    high, low = parts(values)
    return product(table[0], high) + (product(table[0], low) + product(table[1], high))


def times_table(values, table):
    high, low = parts(values)
    return product(high, table[0]) + (product(high, table[1]) + product(low, table[0]))


def small_call(kernel, name, megabytes, **kwargs):
    limit = pltpu.CompilerParams(vmem_limit_bytes=megabytes * 2**20)
    return pl.pallas_call(kernel, compiler_params=limit, name=name, **kwargs)


def in_vmem(count):
    return [pl.BlockSpec(memory_space=pltpu.VMEM)] * count


def in_smem(count):
    return [pl.BlockSpec(memory_space=pltpu.SMEM)] * count


def anywhere(count):
    return [pl.BlockSpec(memory_space=pl.ANY)] * count


def kept(shape):
    return pltpu.VMEM(shape, jnp.float32)


def row_sums(tiles):
    row = lax.broadcasted_iota(jnp.int32, (8, LANES), 0)
    top = row < 4
    fours = [
        jnp.where(top, tiles[i], tiles[i + 4])
        + pltpu.roll(jnp.where(top, tiles[i + 4], tiles[i]), 4, 0)
        for i in range(4)
    ]
    for step in (2, 1):
        early = (row % (2 * step)) < step
        fours = [
            jnp.where(
                early,
                fours[i] + pltpu.roll(fours[i], 8 - step, 0),
                fours[i + step] + pltpu.roll(fours[i + step], step, 0),
            )
            for i in range(step)
        ]
    return fours[0]


CORNERS = pltpu.HBM
CHUNK = 8
UNROLL = 4


def core_kernel(
    base, depth, count_x, count_y, device, corners, span, occupations, sign, orbitals, outer, out,
    *refs,
):
    *blocks, buffer, sums, rows, arrived, filled = refs
    own, slots, orbital_count = device[0], out.shape[0], orbitals.shape[1]
    first_z, first_x, first_y = span[0, 0], span[0, 1], span[0, 2]
    len_z, len_x, len_y = span[0, 3], span[0, 4], span[0, 5]
    begin = jnp.minimum(first_z, BOX - CORE)
    chunks = CORE // CHUNK
    copies = [
        pltpu.make_async_copy(
            orbitals.at[0, :, pl.ds(pl.multiple_of((begin + c * CHUNK) * PLANE, LANES), CHUNK * PLANE)],
            buffer.at[c],
            arrived.at[c],
        )
        for c in range(chunks)
    ]
    for copy in copies:
        copy.start()
    sub = lax.rem(own, len(blocks))
    fills = [
        pltpu.make_async_copy(outer.at[sub ^ d], block, filled.at[d])
        for d, block in enumerate(blocks)
    ]
    for fill in fills:
        fill.start()
    orbital = lax.broadcasted_iota(jnp.int32, (orbital_count, LANES), 0)
    weight = jnp.zeros((orbital_count, LANES), jnp.int32)
    for o in range(orbital_count):
        weight = jnp.where(orbital == o, occupations[0, o], weight)
    weight = (weight * sign[0]).astype(jnp.float32)
    groups = CHUNK * GROUPS // 8
    tiles = WIDE // LANES
    for c in range(chunks):
        copies[c].wait()

        def add_rows(b, carry, c=c):
            for q in range(tiles):
                cells = []
                for s in range(8):
                    lane = pl.multiple_of((8 * b + s) * WIDE + q * LANES, LANES)
                    values = buffer[c, :, pl.ds(lane, LANES)].astype(jnp.float32)
                    values = values * values * weight
                    cells.append(sum(values[8 * h : 8 * h + 8] for h in range(orbital_count // 8)))
                at = pl.multiple_of((c * groups + b) * 8, 8)
                sums[pl.ds(at, 8), q * LANES : (q + 1) * LANES] = row_sums(cells)
            return carry

        lax.fori_loop(0, groups, add_rows, 0, unroll=2)
    count = CORE * GROUPS
    for r in range(8):
        rows[pl.ds(r, count, stride=8), 0:BOX] = sums[:, r * BOX : (r + 1) * BOX]

    start_z = lax.rem(corners[0, own] + first_z, depth) - base(own)
    start_x = lax.rem(corners[1, own] + first_x, count_x)
    start_y = lax.rem(corners[2, own] + first_y, count_y)
    row = lax.broadcasted_iota(jnp.int32, (8, LANES), 0)
    lane = lax.broadcasted_iota(jnp.int32, (8, LANES), 1)
    first = jnp.where(lane[0:1] == 0, start_x, start_y).astype(jnp.float32)

    def pack(step, carry):
        turned = []
        for h in range(UNROLL):
            p = lax.rem(UNROLL * step + h - start_z + depth, depth)
            local = jnp.minimum(p + first_z - begin, CORE - 1)
            cells = rows[pl.ds(local * BOX + first_x, CORE), :]
            for q in range(4):
                turn = lax.rem(32 * q - first_y + LANES, LANES)
                turned.append(pltpu.roll(cells[8 * q : 8 * q + 8], turn, 1))
        for h in range(UNROLL):
            k = UNROLL * step + h
            held = lax.rem(k - start_z + depth, depth) < len_z
            packed = jnp.zeros((8, LANES), jnp.float32)
            for q in range(4):
                keep = (row + 8 * q < len_x) & (lane >= 32 * q) & (lane < 32 * q + len_y) & held
                packed = jnp.where(keep, turned[4 * h + q], packed)
            for s in range(8):
                out[k, :, s * LANES : (s + 1) * LANES] = packed[s : s + 1]
            out[k, :, PACK:PIECE] = first
        return carry

    lax.fori_loop(0, slots // UNROLL, pack, 0)
    for fill in fills:
        fill.wait()


def core_pieces(device, corners, span, occupations, sign, orbitals, outer, slots, base, counts):
    orbital_count = orbitals.shape[1]
    blocks = outer.shape[0]
    return small_call(
        lambda *refs: core_kernel(base, *counts, *refs),
        "core_pieces",
        8,
        out_shape=[kept((slots, 1, PIECE))] + [kept(outer.shape[1:])] * blocks,
        in_specs=in_smem(5) + anywhere(2),
        out_specs=in_vmem(1 + blocks),
        scratch_shapes=[
            pltpu.VMEM((CORE // CHUNK, orbital_count, CHUNK * PLANE), orbitals.dtype),
            pltpu.VMEM((CORE * GROUPS, WIDE), jnp.float32),
            pltpu.VMEM((CORE * BOX + CORE, LANES), jnp.float32),
            pltpu.SemaphoreType.DMA((CORE // CHUNK,)),
            pltpu.SemaphoreType.DMA((blocks,)),
        ],
        cost_estimate=pl.CostEstimate(flops=40_000_000, bytes_accessed=4_000_000, transcendentals=0),
    )(device, corners, span, occupations, sign, orbitals, outer)


def plane_kernel(group, device, pieces, table_x, table_y, *refs):
    *blocks, spectrum, density, packed = refs
    slots = pieces.shape[0]
    count_x, count_y = density.shape
    sub = lax.rem(device[0], len(blocks))
    x_dev = count_x // len(blocks)
    for d, block in enumerate(blocks):
        density[pl.ds(pl.multiple_of((sub ^ d) * x_dev, 8), x_dev), :] = block[...]
    groups = slots // group
    column = lax.broadcasted_iota(jnp.int32, (count_x, CORE), 1)
    cell_x = lax.broadcasted_iota(jnp.int32, (count_x, CORE), 0)
    row = lax.broadcasted_iota(jnp.int32, (CORE, count_y), 0)
    cell_y = lax.broadcasted_iota(jnp.int32, (CORE, count_y), 1)
    lefts, rights = [], []
    for j in range(groups):
        total = pieces[j * group, :, 0:PACK]
        for m in range(1, group):
            total = total + pieces[j * group + m, :, 0:PACK]
        for s in range(8):
            packed[8 * j + s : 8 * j + s + 1, :] = total[:, s * LANES : (s + 1) * LANES]
        tile = packed[8 * j : 8 * j + 8, :]
        square = jnp.concatenate([tile[:, 32 * q : 32 * q + 32] for q in range(4)], axis=0)
        first = pieces[j * group, :, PACK : PACK + LANES].astype(jnp.int32)
        away_x = cell_x - first[:, 0:1]
        away_y = cell_y - first[:, 1:2]
        left = jnp.where(away_x < 0, away_x + count_x, away_x) == column
        right = jnp.where(away_y < 0, away_y + count_y, away_y) == row
        right = jnp.where(right, 1.0, 0.0).astype(jnp.bfloat16)
        high = square.astype(jnp.bfloat16)
        rest = square - high.astype(jnp.float32)
        middle = rest.astype(jnp.bfloat16)
        low = (rest - middle.astype(jnp.float32)).astype(jnp.bfloat16)
        lefts.append(jnp.where(left, 1.0, 0.0).astype(jnp.bfloat16))
        rights.append([product(part, right).astype(jnp.bfloat16) for part in (high, middle, low)])
    left = jnp.concatenate(lefts, axis=1)
    placed = density[...]
    for part in range(2, -1, -1):
        placed = placed + product(left, jnp.concatenate([r[part] for r in rights], axis=0))
    density[...] = placed
    spectrum[...] = times_table(table_times(table_x, placed), table_y)


def plane_spectrum(device, pieces, group, table_x, table_y, blocks):
    shape = (blocks[0].shape[0] * len(blocks), blocks[0].shape[1])
    return small_call(
        lambda *refs: plane_kernel(group, *refs),
        "plane_spectrum",
        12,
        out_shape=(kept(shape), kept(shape)),
        in_specs=in_smem(1) + in_vmem(3 + len(blocks)),
        out_specs=in_vmem(2),
        scratch_shapes=[pltpu.VMEM((8 * (pieces.shape[0] // group), LANES), jnp.float32)],
    )(device, pieces, table_x, table_y, *blocks)


def wave_squares(index, count):
    folded = jnp.where(index > count // 2, index - count, index)
    wave = 2.0 * math.pi / (count * spacing) * folded.astype(jnp.float32)
    return wave * wave


def column_kernel(count_z, count_x, count_y, device, values, table, out):
    rows, lanes = values.shape
    deep = rows // count_z
    transformed = table_times(table, values[...])
    row = lax.broadcasted_iota(jnp.int32, (rows, lanes), 0)
    lane = lax.broadcasted_iota(jnp.int32, (rows, lanes), 1)
    cell = (device[0] * deep + row % deep) * lanes + lane
    square = (
        wave_squares(row // deep, count_z)
        + wave_squares(cell // count_y, count_x)
        + wave_squares(cell % count_y, count_y)
    )
    scale = 4.0 * math.pi / float(count_z * count_x * count_y)
    kernel = jnp.where(square > 0, scale / jnp.where(square > 0, square, 1.0), 0.0)
    out[...] = table_times(table, transformed * kernel)


def column_hartree(values, table, device, counts):
    return small_call(
        lambda *refs: column_kernel(*counts, *refs),
        "column_hartree",
        12,
        out_shape=kept(values.shape),
        in_specs=in_smem(1) + in_vmem(2),
        out_specs=in_vmem(1)[0],
    )(device, values, table)


def window_kernel(fragment, device, corners, spectrum, exchange, table_x, table_y, *refs):
    *blocks, out, wide, cut = refs
    slots = out.shape[0]
    count_x, count_y = spectrum.shape
    x_dev = count_x // len(blocks)
    plane = times_table(table_times(table_x, spectrum[...]), table_y) + exchange[...]
    tall = count_x + BOX
    tiles = count_y // LANES
    for t in range(tiles):
        part = plane[:, t * LANES : (t + 1) * LANES]
        wide[t * tall : t * tall + count_x, :] = part
        wide[t * tall + count_x : (t + 1) * tall, :] = part[0:BOX]
    sub = lax.rem(device[0], len(blocks))
    for d, block in enumerate(blocks):
        for t in range(tiles):
            at = pl.multiple_of(t * tall + (sub ^ d) * x_dev, 8)
            block[:, t * LANES : (t + 1) * LANES] = wide[pl.ds(at, x_dev), :]
    lane = lax.broadcasted_iota(jnp.int32, (BOX, LANES), 1)

    def cut_windows(step, carry):
        turned = []
        for h in range(UNROLL):
            f = fragment(UNROLL * step + h, device[0])
            x, y = corners[1, f], corners[2, f]
            tile = y // LANES
            over = y - tile * LANES
            near = wide[pl.ds(tile * tall + x, BOX), :]
            far = wide[pl.ds(lax.rem(tile + 1, tiles) * tall + x, BOX), :]
            turn = lax.rem(LANES - over, LANES)
            turned.append(pltpu.roll(jnp.where(lane < over, far, near), turn, 1))
        for h in range(UNROLL):
            at = pl.multiple_of((UNROLL * step + h) * BOX, 8)
            cut[pl.ds(at, BOX), :] = turned[h]
        return carry

    lax.fori_loop(0, slots // UNROLL, cut_windows, 0)
    count = slots * GROUPS
    flat = jnp.concatenate(
        [cut[pl.ds(r, count, stride=8), :][:, 0:BOX] for r in range(8)], axis=1
    )
    for k in range(slots):
        for g in range(GROUPS):
            out[k, :, g * WIDE : (g + 1) * WIDE] = flat[k * GROUPS + g : k * GROUPS + g + 1, :]


def plane_windows(
    device, corners, spectrum, exchange, table_x, table_y, blocks, slots, fragment
):
    count_x, count_y = spectrum.shape
    block = kept((count_x // blocks, count_y))
    return small_call(
        lambda *refs: window_kernel(fragment, *refs),
        "plane_windows",
        12,
        out_shape=[block] * blocks + [kept((slots, 1, PLANE))],
        in_specs=in_smem(2) + in_vmem(4),
        out_specs=in_vmem(blocks + 1),
        scratch_shapes=[
            pltpu.VMEM((count_y // LANES * (count_x + BOX), LANES), jnp.float32),
            pltpu.VMEM((slots * BOX, LANES), jnp.float32),
        ],
    )(device, corners, spectrum, exchange, table_x, table_y)


def output_kernel(base, device, corners, windows, *refs):
    *blocks, box, potential, copied = refs
    depth = windows.shape[0]
    first = corners[0, device[0]] - base(device[0])
    sub = lax.rem(device[0], len(blocks))
    copies = [
        pltpu.make_async_copy(block, potential.at[sub ^ d], copied.at[BOX + d])
        for d, block in enumerate(blocks)
    ]
    for i in range(BOX):
        z = lax.rem(first + i, depth)
        copies.append(pltpu.make_async_copy(windows.at[z], box.at[i], copied.at[i]))
    for copy in copies:
        copy.start()
    for copy in copies:
        copy.wait()


def outputs(device, corners, windows, blocks, base):
    count = len(blocks)
    return small_call(
        lambda *refs: output_kernel(base, *refs),
        "outputs",
        4,
        out_shape=(
            jax.ShapeDtypeStruct((BOX, 1, PLANE), jnp.float32),
            jax.ShapeDtypeStruct((count,) + blocks[0].shape, jnp.float32),
        ),
        in_specs=in_smem(2) + anywhere(1 + count),
        out_specs=tuple(anywhere(2)),
        scratch_shapes=[pltpu.SemaphoreType.DMA((BOX + count,))],
    )(device, corners, windows, *blocks)


def body(orbitals, occupations, patch_sign, corners, core_span, outer_density):
    slab_count = lax.axis_size("slab")
    sub_count = lax.axis_size("sub")
    devices = slab_count * sub_count
    z_dev, x_dev, count_y = outer_density.shape
    count_x = x_dev * sub_count
    count_z = z_dev * slab_count
    device = lax.axis_index("slab") * sub_count + lax.axis_index("sub")
    table_x = hartley(count_x)
    table_y = hartley(count_y)
    per_device = count_x * count_y // devices
    deep = max(1, per_device // count_y)
    table_z = hartley(count_z, deep)

    device = jnp.reshape(device, (1,))
    assert z_dev == sub_count
    reach = (BOX + z_dev - 2) // z_dev + 1
    if slab_count <= reach:
        slots, group = devices, KINDS

        def base(own):
            return 0

        def fragment(slot, own):
            return slot

        def spread(pieces):
            return lax.all_to_all(pieces, AXES, 0, 0, tiled=True)

        collect = spread
    else:
        slots, group = reach * sub_count, sub_count

        def base(own):
            return own - lax.rem(own, sub_count)

        def fragment(slot, own):
            away = slot // sub_count * sub_count
            return lax.rem(base(own) - away + devices, devices) + lax.rem(slot, sub_count)

        def passed(pieces, sign):
            pieces = pieces.reshape((reach, sub_count) + pieces.shape[1:])
            pieces = lax.all_to_all(pieces, "sub", 1, 1, tiled=True)
            moved = [pieces[0]]
            for d in range(1, reach):
                ring = [(i, (i + sign * d) % slab_count) for i in range(slab_count)]
                moved.append(lax.ppermute(pieces[d], "slab", ring))
            return jnp.concatenate(moved, axis=0)

        def spread(pieces):
            return passed(pieces, 1)

        def collect(pieces):
            return passed(pieces, -1)

    span, occupations, orbitals, outer_density = (
        pltpu.with_memory_space_constraint(argument, pltpu.HBM)
        for argument in (core_span, occupations, orbitals, outer_density)
    )
    corners = pltpu.with_memory_space_constraint(corners.T, CORNERS)
    counts = (count_z, count_x, count_y)

    def swapped(blocks):
        return [
            lax.ppermute(block, "sub", [(i, i ^ d) for i in range(sub_count)]) if d else block
            for d, block in enumerate(blocks)
        ]

    pieces, *blocks = core_pieces(
        device, corners, span, occupations, patch_sign, orbitals, outer_density, slots, base, counts
    )
    blocks = swapped(blocks)
    pieces = spread(pieces)
    spectrum, density = plane_spectrum(device, pieces, group, table_x, table_y, blocks)
    chunk = (devices, deep, per_device // deep)
    spectrum = lax.all_to_all(spectrum.reshape(chunk), AXES, 0, 0, tiled=True)
    exchange = exchange_correlation(density)
    spectrum = column_hartree(
        spectrum.reshape(devices * deep, per_device // deep), table_z, device, counts
    )
    spectrum = lax.all_to_all(spectrum.reshape(chunk), AXES, 0, 0, tiled=True)
    *blocks, windows = plane_windows(
        device,
        corners,
        spectrum.reshape(count_x, count_y),
        exchange,
        table_x,
        table_y,
        sub_count,
        slots,
        fragment,
    )
    blocks = swapped(blocks)
    windows = collect(windows)
    box, potential = outputs(device, corners, windows, blocks, base)
    return (box.reshape(1, BOX * PLANE), potential)


def solution(mesh):
    placed = (
        P(("slab", "sub"), None, None),
        P(("slab", "sub"), None),
        P(("slab", "sub")),
        P(),
        P(("slab", "sub"), None),
        P("slab", "sub", None),
    )
    return jax.shard_map(
        body,
        mesh=mesh,
        in_specs=placed,
        out_specs=(P(("slab", "sub"), None), P("slab", "sub", None)),
        check_vma=False,
    )
```

```python
import math

import jax
import jax.numpy as jnp
import numpy as np
from jax import lax
from jax.experimental import pallas as pl
from jax.experimental.pallas import tpu as pltpu
from jax.sharding import PartitionSpec as P

BOX = 48
CORE = 32
PLANE = BOX * BOX
GROUPS = 6
WIDE = PLANE // GROUPS
PACK = CORE * CORE
LANES = 128
PIECE = PACK + LANES
KINDS = 8

spacing = 0.35
floor_density = 0.001

AXES = ("slab", "sub")


def exchange_correlation(density):
    clipped = jnp.maximum(density, floor_density)
    radius = jnp.cbrt(3.0 / (4.0 * math.pi * clipped))
    exchange = -jnp.cbrt(3.0 * clipped / math.pi)
    correlation = -0.44 / (radius + 7.8) - 0.44 * radius / (3.0 * (radius + 7.8) ** 2)
    return exchange + correlation


def split_table(table):
    high = table.astype(np.float32).astype(jnp.bfloat16)
    low = (table - high.astype(np.float64)).astype(np.float32).astype(jnp.bfloat16)
    return np.stack([high, low])


def hartley(count, repeat=1):
    index = np.arange(count)
    angle = 2.0 * np.pi / count * (np.outer(index, index) % count)
    return split_table(np.kron(np.cos(angle) + np.sin(angle), np.eye(repeat)))


def parts(values):
    high = values.astype(jnp.bfloat16)
    low = (values - high.astype(jnp.float32)).astype(jnp.bfloat16)
    return high, low


def product(a, b):
    return jnp.dot(a, b, preferred_element_type=jnp.float32)


def table_times(table, values):
    high, low = parts(values)
    return product(table[0], high) + (product(table[0], low) + product(table[1], high))


def times_table(values, table):
    high, low = parts(values)
    return product(high, table[0]) + (product(high, table[1]) + product(low, table[0]))


def small_call(kernel, megabytes, **kwargs):
    limit = pltpu.CompilerParams(vmem_limit_bytes=megabytes * 2**20)
    return pl.pallas_call(kernel, compiler_params=limit, **kwargs)


def in_vmem(count):
    return [pl.BlockSpec(memory_space=pltpu.VMEM)] * count


def in_smem(count):
    return [pl.BlockSpec(memory_space=pltpu.SMEM)] * count


def anywhere(count):
    return [pl.BlockSpec(memory_space=pl.ANY)] * count


def kept(shape):
    return pltpu.VMEM(shape, jnp.float32)


def row_sums(tiles):
    row = lax.broadcasted_iota(jnp.int32, (8, LANES), 0)
    top = row < 4
    fours = [
        jnp.where(top, tiles[i], tiles[i + 4])
        + pltpu.roll(jnp.where(top, tiles[i + 4], tiles[i]), 4, 0)
        for i in range(4)
    ]
    for step in (2, 1):
        early = (row % (2 * step)) < step
        fours = [
            jnp.where(
                early,
                fours[i] + pltpu.roll(fours[i], 8 - step, 0),
                fours[i + step] + pltpu.roll(fours[i + step], step, 0),
            )
            for i in range(step)
        ]
    return fours[0]


CHUNK = 8
UNROLL = 4


def core_kernel(
    base, depth, count_x, count_y, device, corners, span, occupations, sign, orbitals, outer, out,
    *refs,
):
    *blocks, buffer, sums, rows, arrived, filled = refs
    own, slots, orbital_count = device[0], out.shape[0], orbitals.shape[1]
    first_z, first_x, first_y = span[0, 0], span[0, 1], span[0, 2]
    len_z, len_x, len_y = span[0, 3], span[0, 4], span[0, 5]
    begin = jnp.minimum(first_z, BOX - CORE)
    chunks = CORE // CHUNK
    copies = [
        pltpu.make_async_copy(
            orbitals.at[0, :, pl.ds(pl.multiple_of((begin + c * CHUNK) * PLANE, LANES), CHUNK * PLANE)],
            buffer.at[c],
            arrived.at[c],
        )
        for c in range(chunks)
    ]
    for copy in copies:
        copy.start()
    sub = lax.rem(own, len(blocks))
    fills = [
        pltpu.make_async_copy(outer.at[sub ^ d], block, filled.at[d])
        for d, block in enumerate(blocks)
    ]
    for fill in fills:
        fill.start()
    orbital = lax.broadcasted_iota(jnp.int32, (orbital_count, LANES), 0)
    weight = jnp.zeros((orbital_count, LANES), jnp.int32)
    for o in range(orbital_count):
        weight = jnp.where(orbital == o, occupations[0, o], weight)
    weight = (weight * sign[0]).astype(jnp.float32)
    groups = CHUNK * GROUPS // 8
    tiles = WIDE // LANES
    for c in range(chunks):
        copies[c].wait()

        def add_rows(b, carry, c=c):
            for q in range(tiles):
                cells = []
                for s in range(8):
                    lane = pl.multiple_of((8 * b + s) * WIDE + q * LANES, LANES)
                    values = buffer[c, :, pl.ds(lane, LANES)].astype(jnp.float32)
                    values = values * values * weight
                    cells.append(sum(values[8 * h : 8 * h + 8] for h in range(orbital_count // 8)))
                at = pl.multiple_of((c * groups + b) * 8, 8)
                sums[pl.ds(at, 8), q * LANES : (q + 1) * LANES] = row_sums(cells)
            return carry

        lax.fori_loop(0, groups, add_rows, 0, unroll=2)
    count = CORE * GROUPS
    for r in range(8):
        rows[pl.ds(r, count, stride=8), 0:BOX] = sums[:, r * BOX : (r + 1) * BOX]

    start_z = lax.rem(corners[0, own] + first_z, depth) - base(own)
    start_x = lax.rem(corners[1, own] + first_x, count_x)
    start_y = lax.rem(corners[2, own] + first_y, count_y)
    row = lax.broadcasted_iota(jnp.int32, (8, LANES), 0)
    lane = lax.broadcasted_iota(jnp.int32, (8, LANES), 1)
    first = jnp.where(lane[0:1] == 0, start_x, start_y).astype(jnp.float32)

    def pack(step, carry):
        turned = []
        for h in range(UNROLL):
            p = lax.rem(UNROLL * step + h - start_z + depth, depth)
            local = jnp.minimum(p + first_z - begin, CORE - 1)
            cells = rows[pl.ds(local * BOX + first_x, CORE), :]
            for q in range(4):
                turn = lax.rem(32 * q - first_y + LANES, LANES)
                turned.append(pltpu.roll(cells[8 * q : 8 * q + 8], turn, 1))
        for h in range(UNROLL):
            k = UNROLL * step + h
            held = lax.rem(k - start_z + depth, depth) < len_z
            packed = jnp.zeros((8, LANES), jnp.float32)
            for q in range(4):
                keep = (row + 8 * q < len_x) & (lane >= 32 * q) & (lane < 32 * q + len_y) & held
                packed = jnp.where(keep, turned[4 * h + q], packed)
            for s in range(8):
                out[k, :, s * LANES : (s + 1) * LANES] = packed[s : s + 1]
            out[k, :, PACK:PIECE] = first
        return carry

    lax.fori_loop(0, slots // UNROLL, pack, 0)
    for fill in fills:
        fill.wait()


def core_pieces(device, corners, span, occupations, sign, orbitals, outer, slots, base, counts):
    orbital_count = orbitals.shape[1]
    blocks = outer.shape[0]
    return small_call(
        lambda *refs: core_kernel(base, *counts, *refs),
        8,
        out_shape=[kept((slots, 1, PIECE))] + [kept(outer.shape[1:])] * blocks,
        in_specs=in_smem(5) + anywhere(2),
        out_specs=in_vmem(1 + blocks),
        scratch_shapes=[
            pltpu.VMEM((CORE // CHUNK, orbital_count, CHUNK * PLANE), orbitals.dtype),
            pltpu.VMEM((CORE * GROUPS, WIDE), jnp.float32),
            pltpu.VMEM((CORE * BOX + CORE, LANES), jnp.float32),
            pltpu.SemaphoreType.DMA((CORE // CHUNK,)),
            pltpu.SemaphoreType.DMA((blocks,)),
        ],
        cost_estimate=pl.CostEstimate(flops=40_000_000, bytes_accessed=4_000_000, transcendentals=0),
    )(device, corners, span, occupations, sign, orbitals, outer)


def plane_kernel(group, device, pieces, table_x, table_y, *refs):
    *blocks, spectrum, density, packed = refs
    slots = pieces.shape[0]
    count_x, count_y = density.shape
    sub = lax.rem(device[0], len(blocks))
    x_dev = count_x // len(blocks)
    for d, block in enumerate(blocks):
        density[pl.ds(pl.multiple_of((sub ^ d) * x_dev, 8), x_dev), :] = block[...]
    groups = slots // group
    column = lax.broadcasted_iota(jnp.int32, (count_x, CORE), 1)
    cell_x = lax.broadcasted_iota(jnp.int32, (count_x, CORE), 0)
    row = lax.broadcasted_iota(jnp.int32, (CORE, count_y), 0)
    cell_y = lax.broadcasted_iota(jnp.int32, (CORE, count_y), 1)
    lefts, rights = [], []
    for j in range(groups):
        total = pieces[j * group, :, 0:PACK]
        for m in range(1, group):
            total = total + pieces[j * group + m, :, 0:PACK]
        for s in range(8):
            packed[8 * j + s : 8 * j + s + 1, :] = total[:, s * LANES : (s + 1) * LANES]
        tile = packed[8 * j : 8 * j + 8, :]
        square = jnp.concatenate([tile[:, 32 * q : 32 * q + 32] for q in range(4)], axis=0)
        first = pieces[j * group, :, PACK : PACK + LANES].astype(jnp.int32)
        away_x = cell_x - first[:, 0:1]
        away_y = cell_y - first[:, 1:2]
        left = jnp.where(away_x < 0, away_x + count_x, away_x) == column
        right = jnp.where(away_y < 0, away_y + count_y, away_y) == row
        right = jnp.where(right, 1.0, 0.0).astype(jnp.bfloat16)
        high = square.astype(jnp.bfloat16)
        rest = square - high.astype(jnp.float32)
        middle = rest.astype(jnp.bfloat16)
        low = (rest - middle.astype(jnp.float32)).astype(jnp.bfloat16)
        lefts.append(jnp.where(left, 1.0, 0.0).astype(jnp.bfloat16))
        rights.append([product(part, right).astype(jnp.bfloat16) for part in (high, middle, low)])
    left = jnp.concatenate(lefts, axis=1)
    placed = density[...]
    for part in range(2, -1, -1):
        placed = placed + product(left, jnp.concatenate([r[part] for r in rights], axis=0))
    density[...] = placed
    spectrum[...] = times_table(table_times(table_x, placed), table_y)


def plane_spectrum(device, pieces, group, table_x, table_y, blocks):
    shape = (blocks[0].shape[0] * len(blocks), blocks[0].shape[1])
    return small_call(
        lambda *refs: plane_kernel(group, *refs),
        12,
        out_shape=(kept(shape), kept(shape)),
        in_specs=in_smem(1) + in_vmem(3 + len(blocks)),
        out_specs=in_vmem(2),
        scratch_shapes=[pltpu.VMEM((8 * (pieces.shape[0] // group), LANES), jnp.float32)],
    )(device, pieces, table_x, table_y, *blocks)


def wave_squares(index, count):
    folded = jnp.where(index > count // 2, index - count, index)
    wave = 2.0 * math.pi / (count * spacing) * folded.astype(jnp.float32)
    return wave * wave


def column_kernel(count_z, count_x, count_y, device, values, table, out):
    rows, lanes = values.shape
    deep = rows // count_z
    transformed = table_times(table, values[...])
    row = lax.broadcasted_iota(jnp.int32, (rows, lanes), 0)
    lane = lax.broadcasted_iota(jnp.int32, (rows, lanes), 1)
    cell = (device[0] * deep + row % deep) * lanes + lane
    square = (
        wave_squares(row // deep, count_z)
        + wave_squares(cell // count_y, count_x)
        + wave_squares(cell % count_y, count_y)
    )
    scale = 4.0 * math.pi / float(count_z * count_x * count_y)
    kernel = jnp.where(square > 0, scale / jnp.where(square > 0, square, 1.0), 0.0)
    out[...] = table_times(table, transformed * kernel)


def column_hartree(values, table, device, counts):
    return small_call(
        lambda *refs: column_kernel(*counts, *refs),
        12,
        out_shape=kept(values.shape),
        in_specs=in_smem(1) + in_vmem(2),
        out_specs=in_vmem(1)[0],
    )(device, values, table)


def window_kernel(fragment, device, corners, spectrum, exchange, table_x, table_y, *refs):
    *blocks, out, wide, cut = refs
    slots = out.shape[0]
    count_x, count_y = spectrum.shape
    x_dev = count_x // len(blocks)
    plane = times_table(table_times(table_x, spectrum[...]), table_y) + exchange[...]
    tall = count_x + BOX
    tiles = count_y // LANES
    for t in range(tiles):
        part = plane[:, t * LANES : (t + 1) * LANES]
        wide[t * tall : t * tall + count_x, :] = part
        wide[t * tall + count_x : (t + 1) * tall, :] = part[0:BOX]
    sub = lax.rem(device[0], len(blocks))
    for d, block in enumerate(blocks):
        for t in range(tiles):
            at = pl.multiple_of(t * tall + (sub ^ d) * x_dev, 8)
            block[:, t * LANES : (t + 1) * LANES] = wide[pl.ds(at, x_dev), :]
    lane = lax.broadcasted_iota(jnp.int32, (BOX, LANES), 1)

    def cut_windows(step, carry):
        turned = []
        for h in range(UNROLL):
            f = fragment(UNROLL * step + h, device[0])
            x, y = corners[1, f], corners[2, f]
            tile = y // LANES
            over = y - tile * LANES
            near = wide[pl.ds(tile * tall + x, BOX), :]
            far = wide[pl.ds(lax.rem(tile + 1, tiles) * tall + x, BOX), :]
            turn = lax.rem(LANES - over, LANES)
            turned.append(pltpu.roll(jnp.where(lane < over, far, near), turn, 1))
        for h in range(UNROLL):
            at = pl.multiple_of((UNROLL * step + h) * BOX, 8)
            cut[pl.ds(at, BOX), :] = turned[h]
        return carry

    lax.fori_loop(0, slots // UNROLL, cut_windows, 0)
    count = slots * GROUPS
    flat = jnp.concatenate(
        [cut[pl.ds(r, count, stride=8), :][:, 0:BOX] for r in range(8)], axis=1
    )
    for k in range(slots):
        for g in range(GROUPS):
            out[k, :, g * WIDE : (g + 1) * WIDE] = flat[k * GROUPS + g : k * GROUPS + g + 1, :]


def plane_windows(
    device, corners, spectrum, exchange, table_x, table_y, blocks, slots, fragment
):
    count_x, count_y = spectrum.shape
    block = kept((count_x // blocks, count_y))
    return small_call(
        lambda *refs: window_kernel(fragment, *refs),
        12,
        out_shape=[block] * blocks + [kept((slots, 1, PLANE))],
        in_specs=in_smem(2) + in_vmem(4),
        out_specs=in_vmem(blocks + 1),
        scratch_shapes=[
            pltpu.VMEM((count_y // LANES * (count_x + BOX), LANES), jnp.float32),
            pltpu.VMEM((slots * BOX, LANES), jnp.float32),
        ],
    )(device, corners, spectrum, exchange, table_x, table_y)


def output_kernel(base, device, corners, windows, *refs):
    *blocks, box, potential, copied = refs
    depth = windows.shape[0]
    first = corners[0, device[0]] - base(device[0])
    sub = lax.rem(device[0], len(blocks))
    copies = [
        pltpu.make_async_copy(block, potential.at[sub ^ d], copied.at[BOX + d])
        for d, block in enumerate(blocks)
    ]
    for i in range(BOX):
        z = lax.rem(first + i, depth)
        copies.append(pltpu.make_async_copy(windows.at[z], box.at[i], copied.at[i]))
    for copy in copies:
        copy.start()
    for copy in copies:
        copy.wait()


def outputs(device, corners, windows, blocks, base):
    count = len(blocks)
    return small_call(
        lambda *refs: output_kernel(base, *refs),
        4,
        out_shape=(
            jax.ShapeDtypeStruct((BOX, 1, PLANE), jnp.float32),
            jax.ShapeDtypeStruct((count,) + blocks[0].shape, jnp.float32),
        ),
        in_specs=in_smem(2) + anywhere(1 + count),
        out_specs=tuple(anywhere(2)),
        scratch_shapes=[pltpu.SemaphoreType.DMA((BOX + count,))],
    )(device, corners, windows, *blocks)


def body(orbitals, occupations, patch_sign, corners, core_span, outer_density):
    slab_count = lax.axis_size("slab")
    sub_count = lax.axis_size("sub")
    devices = slab_count * sub_count
    z_dev, x_dev, count_y = outer_density.shape
    count_x = x_dev * sub_count
    count_z = z_dev * slab_count
    device = lax.axis_index("slab") * sub_count + lax.axis_index("sub")
    table_x = hartley(count_x)
    table_y = hartley(count_y)
    per_device = count_x * count_y // devices
    deep = max(1, per_device // count_y)
    table_z = hartley(count_z, deep)

    device = jnp.reshape(device, (1,))
    assert z_dev == sub_count
    reach = (BOX + z_dev - 2) // z_dev + 1
    if slab_count <= reach:
        slots, group = devices, KINDS

        def base(own):
            return 0

        def fragment(slot, own):
            return slot

        def spread(pieces):
            return lax.all_to_all(pieces, AXES, 0, 0, tiled=True)

        collect = spread
    else:
        slots, group = reach * sub_count, sub_count

        def base(own):
            return own - lax.rem(own, sub_count)

        def fragment(slot, own):
            away = slot // sub_count * sub_count
            return lax.rem(base(own) - away + devices, devices) + lax.rem(slot, sub_count)

        def passed(pieces, sign):
            pieces = pieces.reshape((reach, sub_count) + pieces.shape[1:])
            pieces = lax.all_to_all(pieces, "sub", 1, 1, tiled=True)
            moved = [pieces[0]]
            for d in range(1, reach):
                ring = [(i, (i + sign * d) % slab_count) for i in range(slab_count)]
                moved.append(lax.ppermute(pieces[d], "slab", ring))
            return jnp.concatenate(moved, axis=0)

        def spread(pieces):
            return passed(pieces, 1)

        def collect(pieces):
            return passed(pieces, -1)

    corners = corners.T
    arguments = [
        pltpu.with_memory_space_constraint(argument, pltpu.HBM)
        for argument in (corners, core_span, occupations, patch_sign, orbitals, outer_density)
    ]
    arguments[3] = patch_sign
    counts = (count_z, count_x, count_y)

    def swapped(blocks):
        return [
            lax.ppermute(block, "sub", [(i, i ^ d) for i in range(sub_count)]) if d else block
            for d, block in enumerate(blocks)
        ]

    pieces, *blocks = core_pieces(device, *arguments, slots, base, counts)
    blocks = swapped(blocks)
    pieces = spread(pieces)
    spectrum, density = plane_spectrum(device, pieces, group, table_x, table_y, blocks)
    chunk = (devices, deep, per_device // deep)
    exchange = exchange_correlation(density)
    spectrum, exchange = lax.optimization_barrier((spectrum, exchange))
    spectrum = lax.all_to_all(spectrum.reshape(chunk), AXES, 0, 0, tiled=True)
    spectrum = column_hartree(
        spectrum.reshape(devices * deep, per_device // deep), table_z, device, counts
    )
    spectrum = lax.all_to_all(spectrum.reshape(chunk), AXES, 0, 0, tiled=True)
    *blocks, windows = plane_windows(
        device,
        corners,
        spectrum.reshape(count_x, count_y),
        exchange,
        table_x,
        table_y,
        sub_count,
        slots,
        fragment,
    )
    blocks = swapped(blocks)
    windows = collect(windows)
    box, potential = outputs(device, corners, windows, blocks, base)
    return (box.reshape(1, BOX * PLANE), potential)


def solution(mesh):
    placed = (
        P(("slab", "sub"), None, None),
        P(("slab", "sub"), None),
        P(("slab", "sub")),
        P(),
        P(("slab", "sub"), None),
        P("slab", "sub", None),
    )
    return jax.shard_map(
        body,
        mesh=mesh,
        in_specs=placed,
        out_specs=(P(("slab", "sub"), None), P("slab", "sub", None)),
        check_vma=False,
    )
```

```python
import math

import jax
import jax.numpy as jnp
import numpy as np
from jax import lax
from jax.experimental import pallas as pl
from jax.experimental.pallas import tpu as pltpu
from jax.sharding import PartitionSpec as P

BOX = 48
CORE = 32
PLANE = BOX * BOX
GROUPS = 6
WIDE = PLANE // GROUPS
PACK = CORE * CORE
LANES = 128
PIECE = PACK + LANES
KINDS = 8

spacing = 0.35
floor_density = 0.001

AXES = ("slab", "sub")


def exchange_correlation(density):
    clipped = jnp.maximum(density, floor_density)
    radius = jnp.cbrt(3.0 / (4.0 * math.pi * clipped))
    exchange = -jnp.cbrt(3.0 * clipped / math.pi)
    correlation = -0.44 / (radius + 7.8) - 0.44 * radius / (3.0 * (radius + 7.8) ** 2)
    return exchange + correlation


def split_table(table):
    high = table.astype(np.float32).astype(jnp.bfloat16)
    low = (table - high.astype(np.float64)).astype(np.float32).astype(jnp.bfloat16)
    return np.stack([high, low])


def hartley(count, repeat=1):
    index = np.arange(count)
    angle = 2.0 * np.pi / count * (np.outer(index, index) % count)
    return split_table(np.kron(np.cos(angle) + np.sin(angle), np.eye(repeat)))


def parts(values):
    high = values.astype(jnp.bfloat16)
    low = (values - high.astype(jnp.float32)).astype(jnp.bfloat16)
    return high, low


def product(a, b):
    return jnp.dot(a, b, preferred_element_type=jnp.float32)


def table_times(table, values):
    high, low = parts(values)
    return product(table[0], high) + (product(table[0], low) + product(table[1], high))


def times_table(values, table):
    high, low = parts(values)
    return product(high, table[0]) + (product(high, table[1]) + product(low, table[0]))


def small_call(kernel, megabytes, **kwargs):
    limit = pltpu.CompilerParams(vmem_limit_bytes=megabytes * 2**20)
    return pl.pallas_call(kernel, compiler_params=limit, **kwargs)


def in_vmem(count):
    return [pl.BlockSpec(memory_space=pltpu.VMEM)] * count


def in_smem(count):
    return [pl.BlockSpec(memory_space=pltpu.SMEM)] * count


def anywhere(count):
    return [pl.BlockSpec(memory_space=pl.ANY)] * count


def kept(shape):
    return pltpu.VMEM(shape, jnp.float32)


def row_sums(tiles):
    row = lax.broadcasted_iota(jnp.int32, (8, LANES), 0)
    top = row < 4
    fours = [
        jnp.where(top, tiles[i], tiles[i + 4])
        + pltpu.roll(jnp.where(top, tiles[i + 4], tiles[i]), 4, 0)
        for i in range(4)
    ]
    for step in (2, 1):
        early = (row % (2 * step)) < step
        fours = [
            jnp.where(
                early,
                fours[i] + pltpu.roll(fours[i], 8 - step, 0),
                fours[i + step] + pltpu.roll(fours[i + step], step, 0),
            )
            for i in range(step)
        ]
    return fours[0]


def block_kernel(device, outer, *refs):
    *blocks, filled = refs
    sub = lax.rem(device[0], len(blocks))
    fills = [
        pltpu.make_async_copy(outer.at[sub ^ d], block, filled.at[d])
        for d, block in enumerate(blocks)
    ]
    for fill in fills:
        fill.start()
    for fill in fills:
        fill.wait()


def outer_blocks(device, outer):
    count = outer.shape[0]
    return small_call(
        block_kernel,
        4,
        out_shape=[kept(outer.shape[1:])] * count,
        in_specs=in_smem(1) + anywhere(1),
        out_specs=in_vmem(count),
        scratch_shapes=[pltpu.SemaphoreType.DMA((count,))],
    )(device, outer)


CHUNK = 8
UNROLL = 4


def core_kernel(
    base, depth, count_x, count_y, device, sign, corner_table, span_row, occupation_row, orbitals,
    out, buffer, sums, rows, corners, span, occupations, arrived, staged,
):
    own, slots, orbital_count = device[0], out.shape[0], orbitals.shape[1]
    scalars = [
        pltpu.make_async_copy(source, target, staged.at[n])
        for n, (source, target) in enumerate(
            [(span_row, span), (occupation_row, occupations), (corner_table, corners)]
        )
    ]
    for copy in scalars:
        copy.start()
    chunks = BOX // CHUNK
    copies = []
    for c in range(chunks):
        part = pl.ds(c * CHUNK * PLANE, CHUNK * PLANE)
        copies.append(
            pltpu.make_async_copy(orbitals.at[0, :, part], buffer.at[:, part], arrived.at[c])
        )
        copies[c].start()
    for copy in scalars:
        copy.wait()
    first_z, first_x, first_y = span[0, 0], span[0, 1], span[0, 2]
    len_z, len_x, len_y = span[0, 3], span[0, 4], span[0, 5]
    begin = jnp.minimum(first_z, BOX - CORE)
    orbital = lax.broadcasted_iota(jnp.int32, (orbital_count, LANES), 0)
    weight = jnp.zeros((orbital_count, LANES), jnp.int32)
    for o in range(orbital_count):
        weight = jnp.where(orbital == o, occupations[0, o], weight)
    weight = (weight * sign[0]).astype(jnp.float32)
    groups = CHUNK * GROUPS // 8
    tiles = WIDE // LANES
    ahead = chunks - CORE // CHUNK
    for c in range(ahead):
        copies[c].wait()
    for c in range(CORE // CHUNK):
        copies[c + ahead].wait()

        def add_rows(b, carry, c=c):
            for q in range(tiles):
                cells = []
                for s in range(8):
                    line = begin * GROUPS + (c * groups + b) * 8 + s
                    lane = pl.multiple_of(line * WIDE + q * LANES, LANES)
                    values = buffer[:, pl.ds(lane, LANES)].astype(jnp.float32)
                    values = values * values * weight
                    cells.append(sum(values[8 * h : 8 * h + 8] for h in range(orbital_count // 8)))
                at = pl.multiple_of((c * groups + b) * 8, 8)
                sums[pl.ds(at, 8), q * LANES : (q + 1) * LANES] = row_sums(cells)
            return carry

        lax.fori_loop(0, groups, add_rows, 0, unroll=2)
    count = CORE * GROUPS
    for r in range(8):
        rows[pl.ds(r, count, stride=8), 0:BOX] = sums[:, r * BOX : (r + 1) * BOX]

    start_z = lax.rem(corners[0, own] + first_z, depth) - base(own)
    start_x = lax.rem(corners[1, own] + first_x, count_x)
    start_y = lax.rem(corners[2, own] + first_y, count_y)
    row = lax.broadcasted_iota(jnp.int32, (8, LANES), 0)
    lane = lax.broadcasted_iota(jnp.int32, (8, LANES), 1)
    first = jnp.where(lane[0:1] == 0, start_x, start_y).astype(jnp.float32)

    def pack(step, carry):
        turned = []
        for h in range(UNROLL):
            p = lax.rem(UNROLL * step + h - start_z + depth, depth)
            local = jnp.minimum(p + first_z - begin, CORE - 1)
            cells = rows[pl.ds(local * BOX + first_x, CORE), :]
            for q in range(4):
                turn = lax.rem(32 * q - first_y + LANES, LANES)
                turned.append(pltpu.roll(cells[8 * q : 8 * q + 8], turn, 1))
        for h in range(UNROLL):
            k = UNROLL * step + h
            held = lax.rem(k - start_z + depth, depth) < len_z
            packed = jnp.zeros((8, LANES), jnp.float32)
            for q in range(4):
                keep = (row + 8 * q < len_x) & (lane >= 32 * q) & (lane < 32 * q + len_y) & held
                packed = jnp.where(keep, turned[4 * h + q], packed)
            for s in range(8):
                out[k, :, s * LANES : (s + 1) * LANES] = packed[s : s + 1]
            out[k, :, PACK:PIECE] = first
        return carry

    lax.fori_loop(0, slots // UNROLL, pack, 0)


def core_pieces(device, sign, corners, span, occupations, orbitals, slots, base, counts):
    orbital_count = orbitals.shape[1]
    return small_call(
        lambda *refs: core_kernel(base, *counts, *refs),
        8,
        out_shape=kept((slots, 1, PIECE)),
        in_specs=in_smem(2) + anywhere(4),
        out_specs=in_vmem(1)[0],
        scratch_shapes=[
            pltpu.VMEM((orbital_count, BOX * PLANE), orbitals.dtype),
            pltpu.VMEM((CORE * GROUPS, WIDE), jnp.float32),
            pltpu.VMEM((CORE * BOX + CORE, LANES), jnp.float32),
            pltpu.SMEM(corners.shape, jnp.int32),
            pltpu.SMEM(span.shape, jnp.int32),
            pltpu.SMEM(occupations.shape, jnp.int32),
            pltpu.SemaphoreType.DMA((BOX // CHUNK,)),
            pltpu.SemaphoreType.DMA((3,)),
        ],
        cost_estimate=pl.CostEstimate(flops=40_000_000, bytes_accessed=4_000_000, transcendentals=0),
    )(device, sign, corners, span, occupations, orbitals)


def plane_kernel(group, device, pieces, table_x, table_y, *refs):
    *blocks, spectrum, density, packed = refs
    slots = pieces.shape[0]
    count_x, count_y = density.shape
    sub = lax.rem(device[0], len(blocks))
    x_dev = count_x // len(blocks)
    for d, block in enumerate(blocks):
        density[pl.ds(pl.multiple_of((sub ^ d) * x_dev, 8), x_dev), :] = block[...]
    groups = slots // group
    column = lax.broadcasted_iota(jnp.int32, (count_x, CORE), 1)
    cell_x = lax.broadcasted_iota(jnp.int32, (count_x, CORE), 0)
    row = lax.broadcasted_iota(jnp.int32, (CORE, count_y), 0)
    cell_y = lax.broadcasted_iota(jnp.int32, (CORE, count_y), 1)
    lefts, rights = [], []
    for j in range(groups):
        total = pieces[j * group, :, 0:PACK]
        for m in range(1, group):
            total = total + pieces[j * group + m, :, 0:PACK]
        for s in range(8):
            packed[8 * j + s : 8 * j + s + 1, :] = total[:, s * LANES : (s + 1) * LANES]
        tile = packed[8 * j : 8 * j + 8, :]
        square = jnp.concatenate([tile[:, 32 * q : 32 * q + 32] for q in range(4)], axis=0)
        first = pieces[j * group, :, PACK : PACK + LANES].astype(jnp.int32)
        away_x = cell_x - first[:, 0:1]
        away_y = cell_y - first[:, 1:2]
        left = jnp.where(away_x < 0, away_x + count_x, away_x) == column
        right = jnp.where(away_y < 0, away_y + count_y, away_y) == row
        right = jnp.where(right, 1.0, 0.0).astype(jnp.bfloat16)
        high = square.astype(jnp.bfloat16)
        rest = square - high.astype(jnp.float32)
        middle = rest.astype(jnp.bfloat16)
        low = (rest - middle.astype(jnp.float32)).astype(jnp.bfloat16)
        lefts.append(jnp.where(left, 1.0, 0.0).astype(jnp.bfloat16))
        rights.append([product(part, right).astype(jnp.bfloat16) for part in (high, middle, low)])
    left = jnp.concatenate(lefts, axis=1)
    placed = density[...]
    for part in range(2, -1, -1):
        placed = placed + product(left, jnp.concatenate([r[part] for r in rights], axis=0))
    density[...] = placed
    spectrum[...] = times_table(table_times(table_x, placed), table_y)


def plane_spectrum(device, pieces, group, table_x, table_y, blocks):
    shape = (blocks[0].shape[0] * len(blocks), blocks[0].shape[1])
    return small_call(
        lambda *refs: plane_kernel(group, *refs),
        12,
        out_shape=(kept(shape), kept(shape)),
        in_specs=in_smem(1) + in_vmem(3 + len(blocks)),
        out_specs=in_vmem(2),
        scratch_shapes=[pltpu.VMEM((8 * (pieces.shape[0] // group), LANES), jnp.float32)],
    )(device, pieces, table_x, table_y, *blocks)


def wave_squares(index, count):
    folded = jnp.where(index > count // 2, index - count, index)
    wave = 2.0 * math.pi / (count * spacing) * folded.astype(jnp.float32)
    return wave * wave


def column_kernel(count_z, count_x, count_y, device, values, table, out):
    rows, lanes = values.shape
    deep = rows // count_z
    transformed = table_times(table, values[...])
    row = lax.broadcasted_iota(jnp.int32, (rows, lanes), 0)
    lane = lax.broadcasted_iota(jnp.int32, (rows, lanes), 1)
    cell = (device[0] * deep + row % deep) * lanes + lane
    square = (
        wave_squares(row // deep, count_z)
        + wave_squares(cell // count_y, count_x)
        + wave_squares(cell % count_y, count_y)
    )
    scale = 4.0 * math.pi / float(count_z * count_x * count_y)
    kernel = jnp.where(square > 0, scale / jnp.where(square > 0, square, 1.0), 0.0)
    out[...] = table_times(table, transformed * kernel)


def column_hartree(values, table, device, counts):
    return small_call(
        lambda *refs: column_kernel(*counts, *refs),
        12,
        out_shape=kept(values.shape),
        in_specs=in_smem(1) + in_vmem(2),
        out_specs=in_vmem(1)[0],
    )(device, values, table)


def window_kernel(fragment, device, corner_table, spectrum, exchange, table_x, table_y, *refs):
    *blocks, out, wide, cut, corners, staged = refs
    scalars = pltpu.make_async_copy(corner_table, corners, staged)
    scalars.start()
    slots = out.shape[0]
    count_x, count_y = spectrum.shape
    x_dev = count_x // len(blocks)
    plane = times_table(table_times(table_x, spectrum[...]), table_y) + exchange[...]
    tall = count_x + BOX
    tiles = count_y // LANES
    for t in range(tiles):
        part = plane[:, t * LANES : (t + 1) * LANES]
        wide[t * tall : t * tall + count_x, :] = part
        wide[t * tall + count_x : (t + 1) * tall, :] = part[0:BOX]
    sub = lax.rem(device[0], len(blocks))
    for d, block in enumerate(blocks):
        for t in range(tiles):
            at = pl.multiple_of(t * tall + (sub ^ d) * x_dev, 8)
            block[:, t * LANES : (t + 1) * LANES] = wide[pl.ds(at, x_dev), :]
    lane = lax.broadcasted_iota(jnp.int32, (BOX, LANES), 1)
    scalars.wait()

    def cut_windows(step, carry):
        turned = []
        for h in range(UNROLL):
            f = fragment(UNROLL * step + h, device[0])
            x, y = corners[1, f], corners[2, f]
            tile = y // LANES
            over = y - tile * LANES
            near = wide[pl.ds(tile * tall + x, BOX), :]
            far = wide[pl.ds(lax.rem(tile + 1, tiles) * tall + x, BOX), :]
            turn = lax.rem(LANES - over, LANES)
            turned.append(pltpu.roll(jnp.where(lane < over, far, near), turn, 1))
        for h in range(UNROLL):
            at = pl.multiple_of((UNROLL * step + h) * BOX, 8)
            cut[pl.ds(at, BOX), :] = turned[h]
        return carry

    lax.fori_loop(0, slots // UNROLL, cut_windows, 0)
    count = slots * GROUPS
    flat = jnp.concatenate(
        [cut[pl.ds(r, count, stride=8), :][:, 0:BOX] for r in range(8)], axis=1
    )
    for k in range(slots):
        for g in range(GROUPS):
            out[k, :, g * WIDE : (g + 1) * WIDE] = flat[k * GROUPS + g : k * GROUPS + g + 1, :]


def plane_windows(
    device, corners, spectrum, exchange, table_x, table_y, blocks, slots, fragment
):
    count_x, count_y = spectrum.shape
    block = kept((count_x // blocks, count_y))
    return small_call(
        lambda *refs: window_kernel(fragment, *refs),
        12,
        out_shape=[block] * blocks + [kept((slots, 1, PLANE))],
        in_specs=in_smem(1) + anywhere(1) + in_vmem(4),
        out_specs=in_vmem(blocks + 1),
        scratch_shapes=[
            pltpu.VMEM((count_y // LANES * (count_x + BOX), LANES), jnp.float32),
            pltpu.VMEM((slots * BOX, LANES), jnp.float32),
            pltpu.SMEM(corners.shape, jnp.int32),
            pltpu.SemaphoreType.DMA,
        ],
    )(device, corners, spectrum, exchange, table_x, table_y)


def output_kernel(base, device, corners, windows, *refs):
    *blocks, box, potential, copied = refs
    depth = windows.shape[0]
    row = corners[0:1, :]
    own = lax.broadcasted_iota(jnp.int32, row.shape, 1) == device[0]
    first = jnp.sum(jnp.where(own, row, 0)) - base(device[0])
    sub = lax.rem(device[0], len(blocks))
    copies = [
        pltpu.make_async_copy(block, potential.at[sub ^ d], copied.at[BOX + d])
        for d, block in enumerate(blocks)
    ]
    for i in range(BOX):
        z = lax.rem(first + i, depth)
        copies.append(pltpu.make_async_copy(windows.at[z], box.at[i], copied.at[i]))
    for copy in copies:
        copy.start()
    for copy in copies:
        copy.wait()


def outputs(device, corners, windows, blocks, base):
    count = len(blocks)
    return small_call(
        lambda *refs: output_kernel(base, *refs),
        4,
        out_shape=(
            jax.ShapeDtypeStruct((BOX, 1, PLANE), jnp.float32),
            jax.ShapeDtypeStruct((count,) + blocks[0].shape, jnp.float32),
        ),
        in_specs=in_smem(1) + in_vmem(1) + anywhere(1 + count),
        out_specs=tuple(anywhere(2)),
        scratch_shapes=[pltpu.SemaphoreType.DMA((BOX + count,))],
    )(device, corners, windows, *blocks)


def body(orbitals, occupations, patch_sign, corners, core_span, outer_density):
    slab_count = lax.axis_size("slab")
    sub_count = lax.axis_size("sub")
    devices = slab_count * sub_count
    z_dev, x_dev, count_y = outer_density.shape
    count_x = x_dev * sub_count
    count_z = z_dev * slab_count
    device = lax.axis_index("slab") * sub_count + lax.axis_index("sub")
    table_x = hartley(count_x)
    table_y = hartley(count_y)
    per_device = count_x * count_y // devices
    deep = max(1, per_device // count_y)
    table_z = hartley(count_z, deep)

    device = jnp.reshape(device, (1,))
    assert z_dev == sub_count
    reach = (BOX + z_dev - 2) // z_dev + 1
    if slab_count <= reach:
        slots, group = devices, KINDS

        def base(own):
            return 0

        def fragment(slot, own):
            return slot

        def spread(pieces):
            return lax.all_to_all(pieces, AXES, 0, 0, tiled=True)

        collect = spread
    else:
        slots, group = reach * sub_count, sub_count

        def base(own):
            return own - lax.rem(own, sub_count)

        def fragment(slot, own):
            away = slot // sub_count * sub_count
            return lax.rem(base(own) - away + devices, devices) + lax.rem(slot, sub_count)

        def passed(pieces, sign):
            pieces = pieces.reshape((reach, sub_count) + pieces.shape[1:])
            pieces = lax.all_to_all(pieces, "sub", 1, 1, tiled=True)
            moved = [pieces[0]]
            for d in range(1, reach):
                ring = [(i, (i + sign * d) % slab_count) for i in range(slab_count)]
                moved.append(lax.ppermute(pieces[d], "slab", ring))
            return jnp.concatenate(moved, axis=0)

        def spread(pieces):
            return passed(pieces, 1)

        def collect(pieces):
            return passed(pieces, -1)

    counts = (count_z, count_x, count_y)
    corners = corners.T
    arguments = [
        pltpu.with_memory_space_constraint(argument, pltpu.HBM)
        for argument in (corners, core_span, occupations, orbitals, outer_density)
    ]

    def swapped(blocks):
        return [
            lax.ppermute(block, "sub", [(i, i ^ d) for i in range(sub_count)]) if d else block
            for d, block in enumerate(blocks)
        ]

    blocks = outer_blocks(device, arguments.pop())
    blocks = swapped(blocks)
    pieces = core_pieces(device, patch_sign, *arguments, slots, base, counts)
    pieces, blocks = lax.optimization_barrier((pieces, blocks))
    pieces = spread(pieces)
    spectrum, density = plane_spectrum(device, pieces, group, table_x, table_y, blocks)
    chunk = (devices, deep, per_device // deep)
    exchange = exchange_correlation(density)
    spectrum, exchange = lax.optimization_barrier((spectrum, exchange))
    spectrum = lax.all_to_all(spectrum.reshape(chunk), AXES, 0, 0, tiled=True)
    spectrum = column_hartree(
        spectrum.reshape(devices * deep, per_device // deep), table_z, device, counts
    )
    spectrum = lax.all_to_all(spectrum.reshape(chunk), AXES, 0, 0, tiled=True)
    *blocks, windows = plane_windows(
        device,
        corners,
        spectrum.reshape(count_x, count_y),
        exchange,
        table_x,
        table_y,
        sub_count,
        slots,
        fragment,
    )
    blocks = swapped(blocks)
    windows = collect(windows)
    box, potential = outputs(device, corners, windows, blocks, base)
    return (box.reshape(1, BOX * PLANE), potential)


def solution(mesh):
    placed = (
        P(("slab", "sub"), None, None),
        P(("slab", "sub"), None),
        P(("slab", "sub")),
        P(),
        P(("slab", "sub"), None),
        P("slab", "sub", None),
    )
    return jax.shard_map(
        body,
        mesh=mesh,
        in_specs=placed,
        out_specs=(P(("slab", "sub"), None), P("slab", "sub", None)),
        check_vma=False,
    )
```

```python
import math

import jax
import jax.numpy as jnp
import numpy as np
from jax import lax
from jax.experimental import pallas as pl
from jax.experimental.pallas import tpu as pltpu
from jax.sharding import PartitionSpec as P

BOX = 48
CORE = 32
PLANE = BOX * BOX
GROUPS = 6
WIDE = PLANE // GROUPS
PACK = CORE * CORE
LANES = 128
PIECE = PACK + LANES
KINDS = 8

spacing = 0.35
floor_density = 0.001

AXES = ("slab", "sub")


def exchange_correlation(density):
    clipped = jnp.maximum(density, floor_density)
    root = jnp.exp(jnp.log(clipped) * (1.0 / 3.0))
    radius = (0.75 / math.pi) ** (1.0 / 3.0) / root
    exchange = -((3.0 / math.pi) ** (1.0 / 3.0)) * root
    inverse = 1.0 / (radius + 7.8)
    return exchange - 0.44 * inverse - (0.44 / 3.0) * radius * inverse * inverse


def split_table(table):
    high = table.astype(np.float32).astype(jnp.bfloat16)
    low = (table - high.astype(np.float64)).astype(np.float32).astype(jnp.bfloat16)
    return np.stack([high, low])


def hartley(count, repeat=1):
    index = np.arange(count)
    angle = 2.0 * np.pi / count * (np.outer(index, index) % count)
    return split_table(np.kron(np.cos(angle) + np.sin(angle), np.eye(repeat)))


def parts(values):
    high = values.astype(jnp.bfloat16)
    low = (values - high.astype(jnp.float32)).astype(jnp.bfloat16)
    return high, low


def product(a, b):
    return jnp.dot(a, b, preferred_element_type=jnp.float32)


def table_times(table, values):
    high, low = parts(values)
    return product(table[0], high) + (product(table[0], low) + product(table[1], high))


def times_table(values, table):
    high, low = parts(values)
    return product(high, table[0]) + (product(high, table[1]) + product(low, table[0]))


def small_call(kernel, megabytes, **kwargs):
    limit = pltpu.CompilerParams(vmem_limit_bytes=megabytes * 2**20)
    return pl.pallas_call(kernel, compiler_params=limit, **kwargs)


def in_vmem(count):
    return [pl.BlockSpec(memory_space=pltpu.VMEM)] * count


def in_smem(count):
    return [pl.BlockSpec(memory_space=pltpu.SMEM)] * count


def anywhere(count):
    return [pl.BlockSpec(memory_space=pl.ANY)] * count


def kept(shape):
    return pltpu.VMEM(shape, jnp.float32)


def row_sums(tiles):
    row = lax.broadcasted_iota(jnp.int32, (8, LANES), 0)
    top = row < 4
    fours = [
        jnp.where(top, tiles[i], tiles[i + 4])
        + pltpu.roll(jnp.where(top, tiles[i + 4], tiles[i]), 4, 0)
        for i in range(4)
    ]
    for step in (2, 1):
        early = (row % (2 * step)) < step
        fours = [
            jnp.where(
                early,
                fours[i] + pltpu.roll(fours[i], 8 - step, 0),
                fours[i + step] + pltpu.roll(fours[i + step], step, 0),
            )
            for i in range(step)
        ]
    return fours[0]


def block_kernel(device, outer, *refs):
    *blocks, filled = refs
    sub = lax.rem(device[0], len(blocks))
    fills = [
        pltpu.make_async_copy(outer.at[sub ^ d], block, filled.at[d])
        for d, block in enumerate(blocks)
    ]
    for fill in fills:
        fill.start()
    for fill in fills:
        fill.wait()


def outer_blocks(device, outer):
    count = outer.shape[0]
    return small_call(
        block_kernel,
        4,
        out_shape=[kept(outer.shape[1:])] * count,
        in_specs=in_smem(1) + anywhere(1),
        out_specs=in_vmem(count),
        scratch_shapes=[pltpu.SemaphoreType.DMA((count,))],
    )(device, outer)


CHUNK = 8
UNROLL = 4


def core_kernel(
    base, depth, count_x, count_y, device, corner_table, span_row, occupation_row, orbitals,
    out, buffer, sums, rows, corners, span, occupations, arrived, staged,
):
    own, slots, orbital_count = device[0], out.shape[0], orbitals.shape[1]
    scalars = [
        pltpu.make_async_copy(source, target, staged.at[n])
        for n, (source, target) in enumerate(
            [(span_row, span), (occupation_row, occupations), (corner_table, corners)]
        )
    ]
    for copy in scalars:
        copy.start()
    chunks = BOX // CHUNK
    copies = []
    for c in range(chunks):
        part = pl.ds(c * CHUNK * PLANE, CHUNK * PLANE)
        copies.append(
            pltpu.make_async_copy(orbitals.at[0, :, part], buffer.at[:, part], arrived.at[c])
        )
        copies[c].start()
    for copy in scalars:
        copy.wait()
    first_z, first_x, first_y = span[0, 0], span[0, 1], span[0, 2]
    len_z, len_x, len_y = span[0, 3], span[0, 4], span[0, 5]
    begin = jnp.minimum(first_z, BOX - CORE)
    orbital = lax.broadcasted_iota(jnp.int32, (orbital_count, LANES), 0)
    weight = jnp.zeros((orbital_count, LANES), jnp.int32)
    for o in range(orbital_count):
        weight = jnp.where(orbital == o, occupations[0, o], weight)
    sign = 1
    for length in (len_z, len_x, len_y):
        sign = jnp.where(length == CORE, sign, -sign)
    weight = (weight * sign).astype(jnp.float32)
    groups = CHUNK * GROUPS // 8
    tiles = WIDE // LANES
    ahead = chunks - CORE // CHUNK
    for c in range(ahead):
        copies[c].wait()
    for c in range(CORE // CHUNK):
        copies[c + ahead].wait()

        def add_rows(b, carry, c=c):
            for q in range(tiles):
                cells = []
                for s in range(8):
                    line = begin * GROUPS + (c * groups + b) * 8 + s
                    lane = pl.multiple_of(line * WIDE + q * LANES, LANES)
                    values = buffer[:, pl.ds(lane, LANES)].astype(jnp.float32)
                    values = values * values * weight
                    cells.append(sum(values[8 * h : 8 * h + 8] for h in range(orbital_count // 8)))
                at = pl.multiple_of((c * groups + b) * 8, 8)
                sums[pl.ds(at, 8), q * LANES : (q + 1) * LANES] = row_sums(cells)
            return carry

        lax.fori_loop(0, groups, add_rows, 0, unroll=2)
    count = CORE * GROUPS
    for r in range(8):
        rows[pl.ds(r, count, stride=8), 0:BOX] = sums[:, r * BOX : (r + 1) * BOX]

    start_z = lax.rem(corners[0, own] + first_z, depth) - base(own)
    start_x = lax.rem(corners[1, own] + first_x, count_x)
    start_y = lax.rem(corners[2, own] + first_y, count_y)
    row = lax.broadcasted_iota(jnp.int32, (8, LANES), 0)
    lane = lax.broadcasted_iota(jnp.int32, (8, LANES), 1)
    first = jnp.where(lane[0:1] == 0, start_x, start_y).astype(jnp.float32)

    def pack(step, carry):
        turned = []
        for h in range(UNROLL):
            p = lax.rem(UNROLL * step + h - start_z + depth, depth)
            local = jnp.minimum(p + first_z - begin, CORE - 1)
            cells = rows[pl.ds(local * BOX + first_x, CORE), :]
            for q in range(4):
                turn = lax.rem(32 * q - first_y + LANES, LANES)
                turned.append(pltpu.roll(cells[8 * q : 8 * q + 8], turn, 1))
        for h in range(UNROLL):
            k = UNROLL * step + h
            held = lax.rem(k - start_z + depth, depth) < len_z
            packed = jnp.zeros((8, LANES), jnp.float32)
            for q in range(4):
                keep = (row + 8 * q < len_x) & (lane >= 32 * q) & (lane < 32 * q + len_y) & held
                packed = jnp.where(keep, turned[4 * h + q], packed)
            for s in range(8):
                out[k, :, s * LANES : (s + 1) * LANES] = packed[s : s + 1]
            out[k, :, PACK:PIECE] = first
        return carry

    lax.fori_loop(0, slots // UNROLL, pack, 0)


def core_pieces(device, corners, span, occupations, orbitals, slots, base, counts):
    orbital_count = orbitals.shape[1]
    return small_call(
        lambda *refs: core_kernel(base, *counts, *refs),
        8,
        out_shape=kept((slots, 1, PIECE)),
        in_specs=in_smem(1) + anywhere(4),
        out_specs=in_vmem(1)[0],
        scratch_shapes=[
            pltpu.VMEM((orbital_count, BOX * PLANE), orbitals.dtype),
            pltpu.VMEM((CORE * GROUPS, WIDE), jnp.float32),
            pltpu.VMEM((CORE * BOX + CORE, LANES), jnp.float32),
            pltpu.SMEM(corners.shape, jnp.int32),
            pltpu.SMEM(span.shape, jnp.int32),
            pltpu.SMEM(occupations.shape, jnp.int32),
            pltpu.SemaphoreType.DMA((BOX // CHUNK,)),
            pltpu.SemaphoreType.DMA((3,)),
        ],
        cost_estimate=pl.CostEstimate(flops=40_000_000, bytes_accessed=4_000_000, transcendentals=0),
    )(device, corners, span, occupations, orbitals)


def plane_kernel(group, device, pieces, table_x, table_y, *refs):
    *blocks, spectrum, exchange, density, packed = refs
    slots = pieces.shape[0]
    count_x, count_y = density.shape
    sub = lax.rem(device[0], len(blocks))
    x_dev = count_x // len(blocks)
    for d, block in enumerate(blocks):
        density[pl.ds(pl.multiple_of((sub ^ d) * x_dev, 8), x_dev), :] = block[...]
    groups = slots // group
    column = lax.broadcasted_iota(jnp.int32, (count_x, CORE), 1)
    cell_x = lax.broadcasted_iota(jnp.int32, (count_x, CORE), 0)
    row = lax.broadcasted_iota(jnp.int32, (CORE, count_y), 0)
    cell_y = lax.broadcasted_iota(jnp.int32, (CORE, count_y), 1)
    lefts, rights = [], []
    for j in range(groups):
        total = pieces[j * group, :, 0:PACK]
        for m in range(1, group):
            total = total + pieces[j * group + m, :, 0:PACK]
        for s in range(8):
            packed[8 * j + s : 8 * j + s + 1, :] = total[:, s * LANES : (s + 1) * LANES]
        tile = packed[8 * j : 8 * j + 8, :]
        square = jnp.concatenate([tile[:, 32 * q : 32 * q + 32] for q in range(4)], axis=0)
        first = pieces[j * group, :, PACK : PACK + LANES].astype(jnp.int32)
        away_x = cell_x - first[:, 0:1]
        away_y = cell_y - first[:, 1:2]
        left = jnp.where(away_x < 0, away_x + count_x, away_x) == column
        right = jnp.where(away_y < 0, away_y + count_y, away_y) == row
        right = jnp.where(right, 1.0, 0.0).astype(jnp.bfloat16)
        high = square.astype(jnp.bfloat16)
        rest = square - high.astype(jnp.float32)
        middle = rest.astype(jnp.bfloat16)
        low = (rest - middle.astype(jnp.float32)).astype(jnp.bfloat16)
        lefts.append(jnp.where(left, 1.0, 0.0).astype(jnp.bfloat16))
        rights.append([product(part, right).astype(jnp.bfloat16) for part in (high, middle, low)])
    left = jnp.concatenate(lefts, axis=1)
    placed = density[...]
    for part in range(2, -1, -1):
        placed = placed + product(left, jnp.concatenate([r[part] for r in rights], axis=0))
    exchange[...] = exchange_correlation(placed)
    spectrum[...] = times_table(table_times(table_x, placed), table_y)


def plane_spectrum(device, pieces, group, table_x, table_y, blocks):
    shape = (blocks[0].shape[0] * len(blocks), blocks[0].shape[1])
    return small_call(
        lambda *refs: plane_kernel(group, *refs),
        12,
        out_shape=(kept(shape), kept(shape)),
        in_specs=in_smem(1) + in_vmem(3 + len(blocks)),
        out_specs=in_vmem(2),
        scratch_shapes=[
            pltpu.VMEM(shape, jnp.float32),
            pltpu.VMEM((8 * (pieces.shape[0] // group), LANES), jnp.float32),
        ],
    )(device, pieces, table_x, table_y, *blocks)


def wave_squares(index, count):
    folded = jnp.where(index > count // 2, index - count, index)
    wave = 2.0 * math.pi / (count * spacing) * folded.astype(jnp.float32)
    return wave * wave


def column_kernel(count_z, count_x, count_y, device, values, table, out):
    rows, lanes = values.shape
    deep = rows // count_z
    transformed = table_times(table, values[...])
    row = lax.broadcasted_iota(jnp.int32, (rows, lanes), 0)
    lane = lax.broadcasted_iota(jnp.int32, (rows, lanes), 1)
    cell = (device[0] * deep + row % deep) * lanes + lane
    square = (
        wave_squares(row // deep, count_z)
        + wave_squares(cell // count_y, count_x)
        + wave_squares(cell % count_y, count_y)
    )
    scale = 4.0 * math.pi / float(count_z * count_x * count_y)
    kernel = jnp.where(square > 0, scale / jnp.where(square > 0, square, 1.0), 0.0)
    out[...] = table_times(table, transformed * kernel)


def column_hartree(values, table, device, counts):
    return small_call(
        lambda *refs: column_kernel(*counts, *refs),
        12,
        out_shape=kept(values.shape),
        in_specs=in_smem(1) + in_vmem(2),
        out_specs=in_vmem(1)[0],
    )(device, values, table)


def window_kernel(fragment, device, corner_table, spectrum, exchange, table_x, table_y, *refs):
    *blocks, out, wide, cut, corners, staged = refs
    scalars = pltpu.make_async_copy(corner_table, corners, staged)
    scalars.start()
    slots = out.shape[0]
    count_x, count_y = spectrum.shape
    x_dev = count_x // len(blocks)
    plane = times_table(table_times(table_x, spectrum[...]), table_y) + exchange[...]
    tall = count_x + BOX
    tiles = count_y // LANES
    for t in range(tiles):
        part = plane[:, t * LANES : (t + 1) * LANES]
        wide[t * tall : t * tall + count_x, :] = part
        wide[t * tall + count_x : (t + 1) * tall, :] = part[0:BOX]
    sub = lax.rem(device[0], len(blocks))
    for d, block in enumerate(blocks):
        for t in range(tiles):
            at = pl.multiple_of(t * tall + (sub ^ d) * x_dev, 8)
            block[:, t * LANES : (t + 1) * LANES] = wide[pl.ds(at, x_dev), :]
    lane = lax.broadcasted_iota(jnp.int32, (BOX, LANES), 1)
    scalars.wait()

    def cut_windows(step, carry):
        turned = []
        for h in range(UNROLL):
            f = fragment(UNROLL * step + h, device[0])
            x, y = corners[1, f], corners[2, f]
            tile = y // LANES
            over = y - tile * LANES
            near = wide[pl.ds(tile * tall + x, BOX), :]
            far = wide[pl.ds(lax.rem(tile + 1, tiles) * tall + x, BOX), :]
            turn = lax.rem(LANES - over, LANES)
            turned.append(pltpu.roll(jnp.where(lane < over, far, near), turn, 1))
        for h in range(UNROLL):
            at = pl.multiple_of((UNROLL * step + h) * BOX, 8)
            cut[pl.ds(at, BOX), :] = turned[h]
        return carry

    lax.fori_loop(0, slots // UNROLL, cut_windows, 0)
    count = slots * GROUPS
    flat = jnp.concatenate(
        [cut[pl.ds(r, count, stride=8), :][:, 0:BOX] for r in range(8)], axis=1
    )
    for k in range(slots):
        for g in range(GROUPS):
            out[k, :, g * WIDE : (g + 1) * WIDE] = flat[k * GROUPS + g : k * GROUPS + g + 1, :]


def plane_windows(
    device, corners, spectrum, exchange, table_x, table_y, blocks, slots, fragment
):
    count_x, count_y = spectrum.shape
    block = kept((count_x // blocks, count_y))
    return small_call(
        lambda *refs: window_kernel(fragment, *refs),
        12,
        out_shape=[block] * blocks + [kept((slots, 1, PLANE))],
        in_specs=in_smem(1) + anywhere(1) + in_vmem(4),
        out_specs=in_vmem(blocks + 1),
        scratch_shapes=[
            pltpu.VMEM((count_y // LANES * (count_x + BOX), LANES), jnp.float32),
            pltpu.VMEM((slots * BOX, LANES), jnp.float32),
            pltpu.SMEM(corners.shape, jnp.int32),
            pltpu.SemaphoreType.DMA,
        ],
    )(device, corners, spectrum, exchange, table_x, table_y)


def output_kernel(base, device, corners, windows, *refs):
    *blocks, box, potential, copied = refs
    depth = windows.shape[0]
    row = corners[0:1, :]
    own = lax.broadcasted_iota(jnp.int32, row.shape, 1) == device[0]
    first = jnp.sum(jnp.where(own, row, 0)) - base(device[0])
    sub = lax.rem(device[0], len(blocks))
    copies = [
        pltpu.make_async_copy(block, potential.at[sub ^ d], copied.at[BOX + d])
        for d, block in enumerate(blocks)
    ]
    for i in range(BOX):
        z = lax.rem(first + i, depth)
        copies.append(pltpu.make_async_copy(windows.at[z], box.at[i], copied.at[i]))
    for copy in copies:
        copy.start()
    for copy in copies:
        copy.wait()


def outputs(device, corners, windows, blocks, base):
    count = len(blocks)
    return small_call(
        lambda *refs: output_kernel(base, *refs),
        4,
        out_shape=(
            jax.ShapeDtypeStruct((BOX, 1, PLANE), jnp.float32),
            jax.ShapeDtypeStruct((count,) + blocks[0].shape, jnp.float32),
        ),
        in_specs=in_smem(1) + in_vmem(1) + anywhere(1 + count),
        out_specs=tuple(anywhere(2)),
        scratch_shapes=[pltpu.SemaphoreType.DMA((BOX + count,))],
    )(device, corners, windows, *blocks)


def body(orbitals, occupations, patch_sign, corners, core_span, outer_density):
    slab_count = lax.axis_size("slab")
    sub_count = lax.axis_size("sub")
    devices = slab_count * sub_count
    z_dev, x_dev, count_y = outer_density.shape
    count_x = x_dev * sub_count
    count_z = z_dev * slab_count
    device = lax.axis_index("slab") * sub_count + lax.axis_index("sub")
    table_x = hartley(count_x)
    table_y = hartley(count_y)
    per_device = count_x * count_y // devices
    deep = max(1, per_device // count_y)
    table_z = hartley(count_z, deep)

    device = jnp.reshape(device, (1,))
    assert z_dev == sub_count
    reach = (BOX + z_dev - 2) // z_dev + 1
    if slab_count <= reach:
        slots, group = devices, KINDS

        def base(own):
            return 0

        def fragment(slot, own):
            return slot

        def spread(pieces):
            return lax.all_to_all(pieces, AXES, 0, 0, tiled=True)

        collect = spread
    else:
        slots, group = reach * sub_count, sub_count

        def base(own):
            return own - lax.rem(own, sub_count)

        def fragment(slot, own):
            away = slot // sub_count * sub_count
            return lax.rem(base(own) - away + devices, devices) + lax.rem(slot, sub_count)

        def passed(pieces, sign):
            pieces = pieces.reshape((reach, sub_count) + pieces.shape[1:])
            pieces = lax.all_to_all(pieces, "sub", 1, 1, tiled=True)
            moved = [pieces[0]]
            for d in range(1, reach):
                ring = [(i, (i + sign * d) % slab_count) for i in range(slab_count)]
                moved.append(lax.ppermute(pieces[d], "slab", ring))
            return jnp.concatenate(moved, axis=0)

        def spread(pieces):
            return passed(pieces, 1)

        def collect(pieces):
            return passed(pieces, -1)

    counts = (count_z, count_x, count_y)
    corners = corners.T
    arguments = [
        pltpu.with_memory_space_constraint(argument, pltpu.HBM)
        for argument in (corners, core_span, occupations, orbitals, outer_density)
    ]

    def swapped(blocks):
        return [
            lax.ppermute(block, "sub", [(i, i ^ d) for i in range(sub_count)]) if d else block
            for d, block in enumerate(blocks)
        ]

    blocks = outer_blocks(device, arguments.pop())
    blocks = swapped(blocks)
    pieces = core_pieces(device, *arguments, slots, base, counts)
    pieces, blocks = lax.optimization_barrier((pieces, blocks))
    pieces = spread(pieces)
    spectrum, exchange = plane_spectrum(device, pieces, group, table_x, table_y, blocks)
    chunk = (devices, deep, per_device // deep)
    spectrum = lax.all_to_all(spectrum.reshape(chunk), AXES, 0, 0, tiled=True)
    spectrum = column_hartree(
        spectrum.reshape(devices * deep, per_device // deep), table_z, device, counts
    )
    spectrum = lax.all_to_all(spectrum.reshape(chunk), AXES, 0, 0, tiled=True)
    *blocks, windows = plane_windows(
        device,
        corners,
        spectrum.reshape(count_x, count_y),
        exchange,
        table_x,
        table_y,
        sub_count,
        slots,
        fragment,
    )
    blocks = swapped(blocks)
    windows = collect(windows)
    box, potential = outputs(device, corners, windows, blocks, base)
    return (box.reshape(1, BOX * PLANE), potential)


def solution(mesh):
    placed = (
        P(("slab", "sub"), None, None),
        P(("slab", "sub"), None),
        P(("slab", "sub")),
        P(),
        P(("slab", "sub"), None),
        P("slab", "sub", None),
    )
    return jax.shard_map(
        body,
        mesh=mesh,
        in_specs=placed,
        out_specs=(P(("slab", "sub"), None), P("slab", "sub", None)),
        check_vma=False,
    )
```

```python
import math

import jax
import jax.numpy as jnp
import numpy as np
from jax import lax
from jax.experimental import pallas as pl
from jax.experimental.pallas import tpu as pltpu
from jax.sharding import PartitionSpec as P

BOX = 48
CORE = 32
PLANE = BOX * BOX
GROUPS = 6
WIDE = PLANE // GROUPS
PACK = CORE * CORE
LANES = 128
PIECE = PACK + LANES
KINDS = 8

spacing = 0.35
floor_density = 0.001

AXES = ("slab", "sub")


def exchange_correlation(density):
    clipped = jnp.maximum(density, floor_density)
    root = jnp.exp(jnp.log(clipped) * (1.0 / 3.0))
    radius = (0.75 / math.pi) ** (1.0 / 3.0) / root
    exchange = -((3.0 / math.pi) ** (1.0 / 3.0)) * root
    inverse = 1.0 / (radius + 7.8)
    return exchange - 0.44 * inverse - (0.44 / 3.0) * radius * inverse * inverse


def split_table(table):
    high = table.astype(np.float32).astype(jnp.bfloat16)
    low = (table - high.astype(np.float64)).astype(np.float32).astype(jnp.bfloat16)
    return np.stack([high, low])


def hartley(count, repeat=1):
    index = np.arange(count)
    angle = 2.0 * np.pi / count * (np.outer(index, index) % count)
    return split_table(np.kron(np.cos(angle) + np.sin(angle), np.eye(repeat)))


def parts(values):
    high = values.astype(jnp.bfloat16)
    low = (values - high.astype(jnp.float32)).astype(jnp.bfloat16)
    return high, low


def product(a, b):
    return jnp.dot(a, b, preferred_element_type=jnp.float32)


def table_times(table, values):
    high, low = parts(values)
    return product(table[0], high) + (product(table[0], low) + product(table[1], high))


def times_table(values, table):
    high, low = parts(values)
    return product(high, table[0]) + (product(high, table[1]) + product(low, table[0]))


def small_call(kernel, megabytes, **kwargs):
    limit = pltpu.CompilerParams(vmem_limit_bytes=megabytes * 2**20)
    return pl.pallas_call(kernel, compiler_params=limit, **kwargs)


def in_vmem(count):
    return [pl.BlockSpec(memory_space=pltpu.VMEM)] * count


def in_smem(count):
    return [pl.BlockSpec(memory_space=pltpu.SMEM)] * count


def anywhere(count):
    return [pl.BlockSpec(memory_space=pl.ANY)] * count


def kept(shape):
    return pltpu.VMEM(shape, jnp.float32)


def row_sums(tiles):
    row = lax.broadcasted_iota(jnp.int32, (8, LANES), 0)
    top = row < 4
    fours = [
        jnp.where(top, tiles[i], tiles[i + 4])
        + pltpu.roll(jnp.where(top, tiles[i + 4], tiles[i]), 4, 0)
        for i in range(4)
    ]
    for step in (2, 1):
        early = (row % (2 * step)) < step
        fours = [
            jnp.where(
                early,
                fours[i] + pltpu.roll(fours[i], 8 - step, 0),
                fours[i + step] + pltpu.roll(fours[i + step], step, 0),
            )
            for i in range(step)
        ]
    return fours[0]


def block_kernel(device, outer, *refs):
    *blocks, filled = refs
    sub = lax.rem(device[0], len(blocks))
    fills = [
        pltpu.make_async_copy(outer.at[sub ^ d], block, filled.at[d])
        for d, block in enumerate(blocks)
    ]
    for fill in fills:
        fill.start()
    for fill in fills:
        fill.wait()


def outer_blocks(device, outer):
    count = outer.shape[0]
    return small_call(
        block_kernel,
        4,
        out_shape=[kept(outer.shape[1:])] * count,
        in_specs=in_smem(1) + anywhere(1),
        out_specs=in_vmem(count),
        scratch_shapes=[pltpu.SemaphoreType.DMA((count,))],
    )(device, outer)


CHUNK = 8
UNROLL = 4


def core_kernel(
    base, depth, count_x, count_y, device, corner_table, span_row, occupation_row, orbitals,
    out, buffer, sums, rows, corners, span, occupations, arrived, filled,
    staged,
):
    own, slots, orbital_count = device[0], out.shape[0], orbitals.shape[1]
    scalars = [
        pltpu.make_async_copy(source, target, staged.at[n])
        for n, (source, target) in enumerate(
            [(span_row, span), (occupation_row, occupations), (corner_table, corners)]
        )
    ]
    for copy in scalars:
        copy.start()
    loose = BOX - CORE
    early = []
    for c in range(loose // CHUNK, CORE // CHUNK):
        part = pl.ds(c * CHUNK * PLANE, CHUNK * PLANE)
        copy = pltpu.make_async_copy(orbitals.at[0, :, part], buffer.at[:, part], arrived.at[c])
        copy.start()
        early.append(copy)
    for copy in scalars:
        copy.wait()
    first_z, first_x, first_y = span[0, 0], span[0, 1], span[0, 2]
    len_z, len_x, len_y = span[0, 3], span[0, 4], span[0, 5]
    begin = jnp.minimum(first_z, loose)
    late = []
    for p in range(loose):
        i = jnp.where(p < begin, p + CORE, p)
        part = pl.ds(pl.multiple_of(i * PLANE, LANES), PLANE)
        late.append(
            pltpu.make_async_copy(
                orbitals.at[0, :, part], buffer.at[:, p * PLANE : (p + 1) * PLANE], filled.at[p]
            )
        )
        late[p].start()
    orbital = lax.broadcasted_iota(jnp.int32, (orbital_count, LANES), 0)
    weight = jnp.zeros((orbital_count, LANES), jnp.int32)
    for o in range(orbital_count):
        weight = jnp.where(orbital == o, occupations[0, o], weight)
    sign = 1
    for length in (len_z, len_x, len_y):
        sign = jnp.where(length == CORE, sign, -sign)
    weight = (weight * sign).astype(jnp.float32)
    groups = CHUNK * GROUPS // 8
    tiles = WIDE // LANES
    order = list(range(loose // CHUNK, CORE // CHUNK)) + list(range(loose // CHUNK))
    for n, c in enumerate(order):
        for copy in early[n : n + 1] or late[c * CHUNK : (c + 1) * CHUNK]:
            copy.wait()

        def add_rows(b, carry, c=c):
            for q in range(tiles):
                cells = []
                for s in range(8):
                    line = (c * groups + b) * 8 + s
                    lane = pl.multiple_of(line * WIDE + q * LANES, LANES)
                    values = buffer[:, pl.ds(lane, LANES)].astype(jnp.float32)
                    values = values * values * weight
                    cells.append(sum(values[8 * h : 8 * h + 8] for h in range(orbital_count // 8)))
                at = pl.multiple_of((c * groups + b) * 8, 8)
                sums[pl.ds(at, 8), q * LANES : (q + 1) * LANES] = row_sums(cells)
            return carry

        lax.fori_loop(0, groups, add_rows, 0, unroll=2)
    count = CORE * GROUPS
    for r in range(8):
        rows[pl.ds(r, count, stride=8), 0:BOX] = sums[:, r * BOX : (r + 1) * BOX]

    start_z = lax.rem(corners[0, own] + first_z, depth) - base(own)
    start_x = lax.rem(corners[1, own] + first_x, count_x)
    start_y = lax.rem(corners[2, own] + first_y, count_y)
    row = lax.broadcasted_iota(jnp.int32, (8, LANES), 0)
    lane = lax.broadcasted_iota(jnp.int32, (8, LANES), 1)
    first = jnp.where(lane[0:1] == 0, start_x, start_y).astype(jnp.float32)

    def pack(step, carry):
        turned = []
        for h in range(UNROLL):
            p = lax.rem(UNROLL * step + h - start_z + depth, depth)
            local = lax.rem(p + first_z, CORE)
            cells = rows[pl.ds(local * BOX + first_x, CORE), :]
            for q in range(4):
                turn = lax.rem(32 * q - first_y + LANES, LANES)
                turned.append(pltpu.roll(cells[8 * q : 8 * q + 8], turn, 1))
        for h in range(UNROLL):
            k = UNROLL * step + h
            held = lax.rem(k - start_z + depth, depth) < len_z
            packed = jnp.zeros((8, LANES), jnp.float32)
            for q in range(4):
                keep = (row + 8 * q < len_x) & (lane >= 32 * q) & (lane < 32 * q + len_y) & held
                packed = jnp.where(keep, turned[4 * h + q], packed)
            for s in range(8):
                out[k, :, s * LANES : (s + 1) * LANES] = packed[s : s + 1]
            out[k, :, PACK:PIECE] = first
        return carry

    lax.fori_loop(0, slots // UNROLL, pack, 0)


def core_pieces(device, corners, span, occupations, orbitals, slots, base, counts):
    orbital_count = orbitals.shape[1]
    return small_call(
        lambda *refs: core_kernel(base, *counts, *refs),
        8,
        out_shape=kept((slots, 1, PIECE)),
        in_specs=in_smem(1) + anywhere(4),
        out_specs=in_vmem(1)[0],
        scratch_shapes=[
            pltpu.VMEM((orbital_count, CORE * PLANE), orbitals.dtype),
            pltpu.VMEM((CORE * GROUPS, WIDE), jnp.float32),
            pltpu.VMEM((CORE * BOX + CORE, LANES), jnp.float32),
            pltpu.SMEM(corners.shape, jnp.int32),
            pltpu.SMEM(span.shape, jnp.int32),
            pltpu.SMEM(occupations.shape, jnp.int32),
            pltpu.SemaphoreType.DMA((CORE // CHUNK,)),
            pltpu.SemaphoreType.DMA((BOX - CORE,)),
            pltpu.SemaphoreType.DMA((3,)),
        ],
        cost_estimate=pl.CostEstimate(flops=40_000_000, bytes_accessed=4_000_000, transcendentals=0),
    )(device, corners, span, occupations, orbitals)


def plane_kernel(group, device, pieces, table_x, table_y, *refs):
    *blocks, spectrum, exchange, density, packed = refs
    slots = pieces.shape[0]
    count_x, count_y = density.shape
    sub = lax.rem(device[0], len(blocks))
    x_dev = count_x // len(blocks)
    for d, block in enumerate(blocks):
        density[pl.ds(pl.multiple_of((sub ^ d) * x_dev, 8), x_dev), :] = block[...]
    groups = slots // group
    column = lax.broadcasted_iota(jnp.int32, (count_x, CORE), 1)
    cell_x = lax.broadcasted_iota(jnp.int32, (count_x, CORE), 0)
    row = lax.broadcasted_iota(jnp.int32, (CORE, count_y), 0)
    cell_y = lax.broadcasted_iota(jnp.int32, (CORE, count_y), 1)
    lefts, rights = [], []
    for j in range(groups):
        total = pieces[j * group, :, 0:PACK]
        for m in range(1, group):
            total = total + pieces[j * group + m, :, 0:PACK]
        for s in range(8):
            packed[8 * j + s : 8 * j + s + 1, :] = total[:, s * LANES : (s + 1) * LANES]
        tile = packed[8 * j : 8 * j + 8, :]
        square = jnp.concatenate([tile[:, 32 * q : 32 * q + 32] for q in range(4)], axis=0)
        first = pieces[j * group, :, PACK : PACK + LANES].astype(jnp.int32)
        away_x = cell_x - first[:, 0:1]
        away_y = cell_y - first[:, 1:2]
        left = jnp.where(away_x < 0, away_x + count_x, away_x) == column
        right = jnp.where(away_y < 0, away_y + count_y, away_y) == row
        right = jnp.where(right, 1.0, 0.0).astype(jnp.bfloat16)
        high = square.astype(jnp.bfloat16)
        rest = square - high.astype(jnp.float32)
        middle = rest.astype(jnp.bfloat16)
        low = (rest - middle.astype(jnp.float32)).astype(jnp.bfloat16)
        lefts.append(jnp.where(left, 1.0, 0.0).astype(jnp.bfloat16))
        rights.append([product(part, right).astype(jnp.bfloat16) for part in (high, middle, low)])
    left = jnp.concatenate(lefts, axis=1)
    placed = density[...]
    for part in range(2, -1, -1):
        placed = placed + product(left, jnp.concatenate([r[part] for r in rights], axis=0))
    exchange[...] = exchange_correlation(placed)
    spectrum[...] = times_table(table_times(table_x, placed), table_y)


def plane_spectrum(device, pieces, group, table_x, table_y, blocks):
    shape = (blocks[0].shape[0] * len(blocks), blocks[0].shape[1])
    return small_call(
        lambda *refs: plane_kernel(group, *refs),
        12,
        out_shape=(kept(shape), kept(shape)),
        in_specs=in_smem(1) + in_vmem(3 + len(blocks)),
        out_specs=in_vmem(2),
        scratch_shapes=[
            pltpu.VMEM(shape, jnp.float32),
            pltpu.VMEM((8 * (pieces.shape[0] // group), LANES), jnp.float32),
        ],
    )(device, pieces, table_x, table_y, *blocks)


def wave_squares(index, count):
    folded = jnp.where(index > count // 2, index - count, index)
    wave = 2.0 * math.pi / (count * spacing) * folded.astype(jnp.float32)
    return wave * wave


def column_kernel(count_z, count_x, count_y, device, values, table, out):
    rows, lanes = values.shape
    deep = rows // count_z
    transformed = table_times(table, values[...])
    row = lax.broadcasted_iota(jnp.int32, (rows, lanes), 0)
    lane = lax.broadcasted_iota(jnp.int32, (rows, lanes), 1)
    cell = (device[0] * deep + row % deep) * lanes + lane
    square = (
        wave_squares(row // deep, count_z)
        + wave_squares(cell // count_y, count_x)
        + wave_squares(cell % count_y, count_y)
    )
    scale = 4.0 * math.pi / float(count_z * count_x * count_y)
    kernel = jnp.where(square > 0, scale / jnp.where(square > 0, square, 1.0), 0.0)
    out[...] = table_times(table, transformed * kernel)


def column_hartree(values, table, device, counts):
    return small_call(
        lambda *refs: column_kernel(*counts, *refs),
        12,
        out_shape=kept(values.shape),
        in_specs=in_smem(1) + in_vmem(2),
        out_specs=in_vmem(1)[0],
    )(device, values, table)


def window_kernel(fragment, device, corner_table, spectrum, exchange, table_x, table_y, *refs):
    *blocks, out, wide, cut, ready, corners, staged, sent = refs
    scalars = pltpu.make_async_copy(corner_table, corners, staged)
    scalars.start()
    slots = out.shape[0]
    count_x, count_y = spectrum.shape
    x_dev = count_x // len(blocks)
    plane = times_table(table_times(table_x, spectrum[...]), table_y) + exchange[...]
    tall = count_x + BOX
    tiles = count_y // LANES
    for t in range(tiles):
        part = plane[:, t * LANES : (t + 1) * LANES]
        wide[t * tall : t * tall + count_x, :] = part
        wide[t * tall + count_x : (t + 1) * tall, :] = part[0:BOX]
    sub = lax.rem(device[0], len(blocks))
    for d, block in enumerate(blocks):
        for t in range(tiles):
            at = pl.multiple_of(t * tall + (sub ^ d) * x_dev, 8)
            block[:, t * LANES : (t + 1) * LANES] = wide[pl.ds(at, x_dev), :]
    lane = lax.broadcasted_iota(jnp.int32, (BOX, LANES), 1)
    scalars.wait()

    def cut_windows(step, carry):
        turned = []
        for h in range(UNROLL):
            f = fragment(UNROLL * step + h, device[0])
            x, y = corners[1, f], corners[2, f]
            tile = y // LANES
            over = y - tile * LANES
            near = wide[pl.ds(tile * tall + x, BOX), :]
            far = wide[pl.ds(lax.rem(tile + 1, tiles) * tall + x, BOX), :]
            turn = lax.rem(LANES - over, LANES)
            turned.append(pltpu.roll(jnp.where(lane < over, far, near), turn, 1))
        for h in range(UNROLL):
            at = pl.multiple_of((UNROLL * step + h) * BOX, 8)
            cut[pl.ds(at, BOX), :] = turned[h]
        return carry

    parts = len(range(0, slots, slots // 4))
    many = slots // parts
    copies = []
    for n in range(parts):
        lax.fori_loop(-(-n * many // UNROLL), -(-(n + 1) * many // UNROLL), cut_windows, 0)
        at = n * many * BOX
        lines = [cut[pl.ds(at + r, many * GROUPS, stride=8), :][:, 0:BOX] for r in range(8)]
        flat = jnp.concatenate(lines, axis=1)
        for k in range(many):
            for g in range(GROUPS):
                line = flat[k * GROUPS + g : k * GROUPS + g + 1, :]
                ready[n * many + k, :, g * WIDE : (g + 1) * WIDE] = line
        some = pl.ds(n * many, many)
        copies.append(pltpu.make_async_copy(ready.at[some], out.at[some], sent.at[n]))
        copies[n].start()
    for copy in copies:
        copy.wait()


def plane_windows(
    device, corners, spectrum, exchange, table_x, table_y, blocks, slots, fragment
):
    count_x, count_y = spectrum.shape
    block = kept((count_x // blocks, count_y))
    return small_call(
        lambda *refs: window_kernel(fragment, *refs),
        12,
        out_shape=[block] * blocks + [jax.ShapeDtypeStruct((slots, 1, PLANE), jnp.float32)],
        in_specs=in_smem(1) + anywhere(1) + in_vmem(4),
        out_specs=in_vmem(blocks) + anywhere(1),
        scratch_shapes=[
            pltpu.VMEM((count_y // LANES * (count_x + BOX), LANES), jnp.float32),
            pltpu.VMEM((slots * BOX, LANES), jnp.float32),
            pltpu.VMEM((slots, 1, PLANE), jnp.float32),
            pltpu.SMEM(corners.shape, jnp.int32),
            pltpu.SemaphoreType.DMA,
            pltpu.SemaphoreType.DMA((4,)),
        ],
    )(device, corners, spectrum, exchange, table_x, table_y)


def output_kernel(base, device, corners, windows, *refs):
    *blocks, box, potential, copied = refs
    depth = windows.shape[0]
    row = corners[0:1, :]
    own = lax.broadcasted_iota(jnp.int32, row.shape, 1) == device[0]
    first = jnp.sum(jnp.where(own, row, 0)) - base(device[0])
    sub = lax.rem(device[0], len(blocks))
    copies = [
        pltpu.make_async_copy(block, potential.at[sub ^ d], copied.at[BOX + d])
        for d, block in enumerate(blocks)
    ]
    for i in range(BOX):
        z = lax.rem(first + i, depth)
        copies.append(pltpu.make_async_copy(windows.at[z], box.at[i], copied.at[i]))
    for copy in copies:
        copy.start()
    for copy in copies:
        copy.wait()


def outputs(device, corners, windows, blocks, base):
    count = len(blocks)
    return small_call(
        lambda *refs: output_kernel(base, *refs),
        4,
        out_shape=(
            jax.ShapeDtypeStruct((BOX, 1, PLANE), jnp.float32),
            jax.ShapeDtypeStruct((count,) + blocks[0].shape, jnp.float32),
        ),
        in_specs=in_smem(1) + in_vmem(1) + anywhere(1 + count),
        out_specs=tuple(anywhere(2)),
        scratch_shapes=[pltpu.SemaphoreType.DMA((BOX + count,))],
    )(device, corners, windows, *blocks)


def body(orbitals, occupations, patch_sign, corners, core_span, outer_density):
    slab_count = lax.axis_size("slab")
    sub_count = lax.axis_size("sub")
    devices = slab_count * sub_count
    z_dev, x_dev, count_y = outer_density.shape
    count_x = x_dev * sub_count
    count_z = z_dev * slab_count
    device = lax.axis_index("slab") * sub_count + lax.axis_index("sub")
    table_x = hartley(count_x)
    table_y = hartley(count_y)
    per_device = count_x * count_y // devices
    deep = max(1, per_device // count_y)
    table_z = hartley(count_z, deep)

    device = jnp.reshape(device, (1,))
    assert z_dev == sub_count
    reach = (BOX + z_dev - 2) // z_dev + 1
    if slab_count <= reach:
        slots, group = devices, KINDS

        def base(own):
            return 0

        def fragment(slot, own):
            return slot

        def spread(pieces):
            return lax.all_to_all(pieces, AXES, 0, 0, tiled=True)

        collect = spread
    else:
        slots, group = reach * sub_count, sub_count

        def base(own):
            return own - lax.rem(own, sub_count)

        def fragment(slot, own):
            away = slot // sub_count * sub_count
            return lax.rem(base(own) - away + devices, devices) + lax.rem(slot, sub_count)

        def passed(pieces, sign):
            pieces = pieces.reshape((reach, sub_count) + pieces.shape[1:])
            pieces = lax.all_to_all(pieces, "sub", 1, 1, tiled=True)
            moved = [pieces[0]]
            for d in range(1, reach):
                ring = [(i, (i + sign * d) % slab_count) for i in range(slab_count)]
                moved.append(lax.ppermute(pieces[d], "slab", ring))
            return jnp.concatenate(moved, axis=0)

        def spread(pieces):
            return passed(pieces, 1)

        def collect(pieces):
            return passed(pieces, -1)

    counts = (count_z, count_x, count_y)
    corners = corners.T
    arguments = [
        pltpu.with_memory_space_constraint(argument, pltpu.HBM)
        for argument in (corners, core_span, occupations, orbitals, outer_density)
    ]

    def swapped(blocks):
        return [
            lax.ppermute(block, "sub", [(i, i ^ d) for i in range(sub_count)]) if d else block
            for d, block in enumerate(blocks)
        ]

    blocks = outer_blocks(device, arguments.pop())
    blocks = swapped(blocks)
    pieces = core_pieces(device, *arguments, slots, base, counts)
    pieces, blocks = lax.optimization_barrier((pieces, blocks))
    pieces = spread(pieces)
    spectrum, exchange = plane_spectrum(device, pieces, group, table_x, table_y, blocks)
    chunk = (devices, deep, per_device // deep)
    spectrum = lax.all_to_all(spectrum.reshape(chunk), AXES, 0, 0, tiled=True)
    spectrum = column_hartree(
        spectrum.reshape(devices * deep, per_device // deep), table_z, device, counts
    )
    spectrum = lax.all_to_all(spectrum.reshape(chunk), AXES, 0, 0, tiled=True)
    *blocks, windows = plane_windows(
        device,
        corners,
        spectrum.reshape(count_x, count_y),
        exchange,
        table_x,
        table_y,
        sub_count,
        slots,
        fragment,
    )
    blocks = swapped(blocks)
    windows = collect(windows)
    box, potential = outputs(device, corners, windows, blocks, base)
    return (box.reshape(1, BOX * PLANE), potential)


def solution(mesh):
    placed = (
        P(("slab", "sub"), None, None),
        P(("slab", "sub"), None),
        P(("slab", "sub")),
        P(),
        P(("slab", "sub"), None),
        P("slab", "sub", None),
    )
    return jax.shard_map(
        body,
        mesh=mesh,
        in_specs=placed,
        out_specs=(P(("slab", "sub"), None), P("slab", "sub", None)),
        check_vma=False,
    )
```

```python
import math

import jax
import jax.numpy as jnp
import numpy as np
from jax import lax
from jax.experimental import pallas as pl
from jax.experimental.pallas import tpu as pltpu
from jax.sharding import PartitionSpec as P

BOX = 48
CORE = 32
PLANE = BOX * BOX
GROUPS = 6
WIDE = PLANE // GROUPS
PACK = CORE * CORE
LANES = 128
PIECE = PACK + LANES
KINDS = 8

spacing = 0.35
floor_density = 0.001

AXES = ("slab", "sub")


def exchange_correlation(density):
    clipped = jnp.maximum(density, floor_density)
    root = jnp.exp(jnp.log(clipped) * (1.0 / 3.0))
    radius = (0.75 / math.pi) ** (1.0 / 3.0) / root
    exchange = -((3.0 / math.pi) ** (1.0 / 3.0)) * root
    inverse = 1.0 / (radius + 7.8)
    return exchange - 0.44 * inverse - (0.44 / 3.0) * radius * inverse * inverse


def split_table(table):
    high = table.astype(np.float32).astype(jnp.bfloat16)
    low = (table - high.astype(np.float64)).astype(np.float32).astype(jnp.bfloat16)
    return np.stack([high, low])


def hartley(count, repeat=1):
    index = np.arange(count)
    angle = 2.0 * np.pi / count * (np.outer(index, index) % count)
    return split_table(np.kron(np.cos(angle) + np.sin(angle), np.eye(repeat)))


def parts(values):
    high = values.astype(jnp.bfloat16)
    low = (values - high.astype(jnp.float32)).astype(jnp.bfloat16)
    return high, low


def product(a, b):
    return jnp.dot(a, b, preferred_element_type=jnp.float32)


def table_times(table, values):
    high, low = parts(values)
    return product(table[0], high) + (product(table[0], low) + product(table[1], high))


def times_table(values, table):
    high, low = parts(values)
    return product(high, table[0]) + (product(high, table[1]) + product(low, table[0]))


def small_call(kernel, megabytes, **kwargs):
    limit = pltpu.CompilerParams(vmem_limit_bytes=megabytes * 2**20)
    return pl.pallas_call(kernel, compiler_params=limit, **kwargs)


def in_vmem(count):
    return [pl.BlockSpec(memory_space=pltpu.VMEM)] * count


def in_smem(count):
    return [pl.BlockSpec(memory_space=pltpu.SMEM)] * count


def anywhere(count):
    return [pl.BlockSpec(memory_space=pl.ANY)] * count


def at_once(slots):
    return next(n for n in (8, 4, 2, 1) if slots % n == 0)


def repeated(steps, step):
    together = next(n for n in (4, 3, 2, 1) if steps % n == 0)
    lax.fori_loop(0, steps, step, 0, unroll=together)


def kept(shape):
    return pltpu.VMEM(shape, jnp.float32)


def row_sums(tiles):
    row = lax.broadcasted_iota(jnp.int32, (8, LANES), 0)
    top = row < 4
    fours = [
        jnp.where(top, tiles[i], tiles[i + 4])
        + pltpu.roll(jnp.where(top, tiles[i + 4], tiles[i]), 4, 0)
        for i in range(4)
    ]
    for step in (2, 1):
        early = (row % (2 * step)) < step
        fours = [
            jnp.where(
                early,
                fours[i] + pltpu.roll(fours[i], 8 - step, 0),
                fours[i + step] + pltpu.roll(fours[i + step], step, 0),
            )
            for i in range(step)
        ]
    return fours[0]


def block_kernel(device, outer, *refs):
    *blocks, filled = refs
    sub = lax.rem(device[0], len(blocks))
    fills = [
        pltpu.make_async_copy(outer.at[sub ^ d], block, filled.at[d])
        for d, block in enumerate(blocks)
    ]
    for fill in fills:
        fill.start()
    for fill in fills:
        fill.wait()


def outer_blocks(device, outer):
    count = outer.shape[0]
    return small_call(
        block_kernel,
        4,
        out_shape=[kept(outer.shape[1:])] * count,
        in_specs=in_smem(1) + anywhere(1),
        out_specs=in_vmem(count),
        scratch_shapes=[pltpu.SemaphoreType.DMA((count,))],
    )(device, outer)


CHUNK = 8


def core_kernel(
    base, depth, count_x, count_y, device, corner_table, span_row, occupation_row, orbitals,
    out, buffer, sums, rows, corners, span, occupations, arrived, staged,
):
    own, slots, orbital_count = device[0], out.shape[0], orbitals.shape[1]
    scalars = [
        pltpu.make_async_copy(source, target, staged.at[n])
        for n, (source, target) in enumerate(
            [(span_row, span), (occupation_row, occupations), (corner_table, corners)]
        )
    ]
    for copy in scalars:
        copy.start()
    chunks = BOX // CHUNK
    copies = []
    for c in range(chunks):
        part = pl.ds(c * CHUNK * PLANE, CHUNK * PLANE)
        copies.append(
            pltpu.make_async_copy(orbitals.at[0, :, part], buffer.at[:, part], arrived.at[c])
        )
        copies[c].start()
    for copy in scalars:
        copy.wait()
    first_z, first_x, first_y = span[0, 0], span[0, 1], span[0, 2]
    len_z, len_x, len_y = span[0, 3], span[0, 4], span[0, 5]
    begin = jnp.minimum(first_z, BOX - CORE)
    orbital = lax.broadcasted_iota(jnp.int32, (orbital_count, LANES), 0)
    weight = jnp.zeros((orbital_count, LANES), jnp.int32)
    for o in range(orbital_count):
        weight = jnp.where(orbital == o, occupations[0, o], weight)
    sign = 1
    for length in (len_z, len_x, len_y):
        sign = jnp.where(length == CORE, sign, -sign)
    weight = (weight * sign).astype(jnp.float32)
    groups = CHUNK * GROUPS // 8
    tiles = WIDE // LANES
    ahead = chunks - CORE // CHUNK
    for c in range(ahead):
        copies[c].wait()
    for c in range(CORE // CHUNK):
        copies[c + ahead].wait()

        def add_rows(b, carry, c=c):
            for q in range(tiles):
                cells = []
                for s in range(8):
                    line = begin * GROUPS + (c * groups + b) * 8 + s
                    lane = pl.multiple_of(line * WIDE + q * LANES, LANES)
                    values = buffer[:, pl.ds(lane, LANES)].astype(jnp.float32)
                    values = values * values * weight
                    cells.append(sum(values[8 * h : 8 * h + 8] for h in range(orbital_count // 8)))
                at = pl.multiple_of((c * groups + b) * 8, 8)
                sums[pl.ds(at, 8), q * LANES : (q + 1) * LANES] = row_sums(cells)
            return carry

        lax.fori_loop(0, groups, add_rows, 0, unroll=True)
        count = 8 * groups
        for r in range(8):
            line = sums[c * count : (c + 1) * count, r * BOX : (r + 1) * BOX]
            rows[pl.ds(8 * c * count + r, count, stride=8), 0:BOX] = line

    start_z = lax.rem(corners[0, own] + first_z, depth) - base(own)
    start_x = lax.rem(corners[1, own] + first_x, count_x)
    start_y = lax.rem(corners[2, own] + first_y, count_y)
    row = lax.broadcasted_iota(jnp.int32, (8, LANES), 0)
    lane = lax.broadcasted_iota(jnp.int32, (8, LANES), 1)
    first = jnp.where(lane[0:1] == 0, start_x, start_y).astype(jnp.float32)

    many = at_once(slots)

    def pack(step, carry):
        turned = []
        for h in range(many):
            p = lax.rem(many * step + h - start_z + depth, depth)
            local = jnp.minimum(p + first_z - begin, CORE - 1)
            cells = rows[pl.ds(local * BOX + first_x, CORE), :]
            for q in range(4):
                turn = lax.rem(32 * q - first_y + LANES, LANES)
                turned.append(pltpu.roll(cells[8 * q : 8 * q + 8], turn, 1))
        for h in range(many):
            k = many * step + h
            held = lax.rem(k - start_z + depth, depth) < len_z
            packed = jnp.zeros((8, LANES), jnp.float32)
            for q in range(4):
                keep = (row + 8 * q < len_x) & (lane >= 32 * q) & (lane < 32 * q + len_y) & held
                packed = jnp.where(keep, turned[4 * h + q], packed)
            for s in range(8):
                out[k, :, s * LANES : (s + 1) * LANES] = packed[s : s + 1]
            out[k, :, PACK:PIECE] = first
        return carry

    repeated(slots // many, pack)


def core_pieces(device, corners, span, occupations, orbitals, slots, base, counts):
    orbital_count = orbitals.shape[1]
    return small_call(
        lambda *refs: core_kernel(base, *counts, *refs),
        8,
        out_shape=kept((slots, 1, PIECE)),
        in_specs=in_smem(1) + anywhere(4),
        out_specs=in_vmem(1)[0],
        scratch_shapes=[
            pltpu.VMEM((orbital_count, BOX * PLANE), orbitals.dtype),
            pltpu.VMEM((CORE * GROUPS, WIDE), jnp.float32),
            pltpu.VMEM((CORE * BOX + CORE, LANES), jnp.float32),
            pltpu.SMEM(corners.shape, jnp.int32),
            pltpu.SMEM(span.shape, jnp.int32),
            pltpu.SMEM(occupations.shape, jnp.int32),
            pltpu.SemaphoreType.DMA((BOX // CHUNK,)),
            pltpu.SemaphoreType.DMA((3,)),
        ],
        cost_estimate=pl.CostEstimate(flops=40_000_000, bytes_accessed=4_000_000, transcendentals=0),
    )(device, corners, span, occupations, orbitals)


def plane_kernel(group, device, pieces, table_x, table_y, *refs):
    *blocks, spectrum, exchange, density, packed = refs
    slots = pieces.shape[0]
    count_x, count_y = density.shape
    sub = lax.rem(device[0], len(blocks))
    x_dev = count_x // len(blocks)
    for d, block in enumerate(blocks):
        density[pl.ds(pl.multiple_of((sub ^ d) * x_dev, 8), x_dev), :] = block[...]
    groups = slots // group
    column = lax.broadcasted_iota(jnp.int32, (count_x, CORE), 1)
    cell_x = lax.broadcasted_iota(jnp.int32, (count_x, CORE), 0)
    row = lax.broadcasted_iota(jnp.int32, (CORE, count_y), 0)
    cell_y = lax.broadcasted_iota(jnp.int32, (CORE, count_y), 1)
    lefts, rights = [], []
    for j in range(groups):
        total = pieces[j * group, :, 0:PACK]
        for m in range(1, group):
            total = total + pieces[j * group + m, :, 0:PACK]
        for s in range(8):
            packed[8 * j + s : 8 * j + s + 1, :] = total[:, s * LANES : (s + 1) * LANES]
        tile = packed[8 * j : 8 * j + 8, :]
        square = jnp.concatenate([tile[:, 32 * q : 32 * q + 32] for q in range(4)], axis=0)
        first = pieces[j * group, :, PACK : PACK + LANES].astype(jnp.int32)
        away_x = cell_x - first[:, 0:1]
        away_y = cell_y - first[:, 1:2]
        left = jnp.where(away_x < 0, away_x + count_x, away_x) == column
        right = jnp.where(away_y < 0, away_y + count_y, away_y) == row
        right = jnp.where(right, 1.0, 0.0).astype(jnp.bfloat16)
        high = square.astype(jnp.bfloat16)
        rest = square - high.astype(jnp.float32)
        middle = rest.astype(jnp.bfloat16)
        low = (rest - middle.astype(jnp.float32)).astype(jnp.bfloat16)
        lefts.append(jnp.where(left, 1.0, 0.0).astype(jnp.bfloat16))
        rights.append([product(part, right).astype(jnp.bfloat16) for part in (high, middle, low)])
    left = jnp.concatenate(lefts, axis=1)
    placed = density[...]
    for part in range(2, -1, -1):
        placed = placed + product(left, jnp.concatenate([r[part] for r in rights], axis=0))
    exchange[...] = exchange_correlation(placed)
    spectrum[...] = times_table(table_times(table_x, placed), table_y)


def plane_spectrum(device, pieces, group, table_x, table_y, blocks):
    shape = (blocks[0].shape[0] * len(blocks), blocks[0].shape[1])
    return small_call(
        lambda *refs: plane_kernel(group, *refs),
        12,
        out_shape=(kept(shape), kept(shape)),
        in_specs=in_smem(1) + in_vmem(3 + len(blocks)),
        out_specs=in_vmem(2),
        scratch_shapes=[
            pltpu.VMEM(shape, jnp.float32),
            pltpu.VMEM((8 * (pieces.shape[0] // group), LANES), jnp.float32),
        ],
    )(device, pieces, table_x, table_y, *blocks)


def wave_squares(index, count):
    folded = jnp.where(index > count // 2, index - count, index)
    wave = 2.0 * math.pi / (count * spacing) * folded.astype(jnp.float32)
    return wave * wave


def column_kernel(count_z, count_x, count_y, device, values, table, out):
    rows, lanes = values.shape
    deep = rows // count_z
    transformed = table_times(table, values[...])
    row = lax.broadcasted_iota(jnp.int32, (rows, lanes), 0)
    lane = lax.broadcasted_iota(jnp.int32, (rows, lanes), 1)
    cell = (device[0] * deep + row % deep) * lanes + lane
    square = (
        wave_squares(row // deep, count_z)
        + wave_squares(cell // count_y, count_x)
        + wave_squares(cell % count_y, count_y)
    )
    scale = 4.0 * math.pi / float(count_z * count_x * count_y)
    kernel = jnp.where(square > 0, scale / jnp.where(square > 0, square, 1.0), 0.0)
    out[...] = table_times(table, transformed * kernel)


def column_hartree(values, table, device, counts):
    return small_call(
        lambda *refs: column_kernel(*counts, *refs),
        12,
        out_shape=kept(values.shape),
        in_specs=in_smem(1) + in_vmem(2),
        out_specs=in_vmem(1)[0],
    )(device, values, table)


def window_kernel(fragment, device, corner_table, spectrum, exchange, table_x, table_y, *refs):
    *blocks, out, wide, cut, corners, staged = refs
    scalars = pltpu.make_async_copy(corner_table, corners, staged)
    scalars.start()
    slots = out.shape[0]
    count_x, count_y = spectrum.shape
    x_dev = count_x // len(blocks)
    plane = times_table(table_times(table_x, spectrum[...]), table_y) + exchange[...]
    tall = count_x + BOX
    tiles = count_y // LANES
    for t in range(tiles):
        part = plane[:, t * LANES : (t + 1) * LANES]
        wide[t * tall : t * tall + count_x, :] = part
        wide[t * tall + count_x : (t + 1) * tall, :] = part[0:BOX]
    sub = lax.rem(device[0], len(blocks))
    for d, block in enumerate(blocks):
        for t in range(tiles):
            at = pl.multiple_of(t * tall + (sub ^ d) * x_dev, 8)
            block[:, t * LANES : (t + 1) * LANES] = wide[pl.ds(at, x_dev), :]
    lane = lax.broadcasted_iota(jnp.int32, (BOX, LANES), 1)
    scalars.wait()

    many = at_once(slots)

    def cut_windows(step, carry):
        turned = []
        for h in range(many):
            f = fragment(many * step + h, device[0])
            x, y = corners[1, f], corners[2, f]
            tile = y // LANES
            over = y - tile * LANES
            near = wide[pl.ds(tile * tall + x, BOX), :]
            far = wide[pl.ds(lax.rem(tile + 1, tiles) * tall + x, BOX), :]
            turn = lax.rem(LANES - over, LANES)
            turned.append(pltpu.roll(jnp.where(lane < over, far, near), turn, 1))
        for h in range(many):
            at = pl.multiple_of((many * step + h) * BOX, 8)
            cut[pl.ds(at, BOX), :] = turned[h]
        return carry

    repeated(slots // many, cut_windows)
    count = slots * GROUPS
    flat = jnp.concatenate(
        [cut[pl.ds(r, count, stride=8), :][:, 0:BOX] for r in range(8)], axis=1
    )
    for k in range(slots):
        for g in range(GROUPS):
            out[k, :, g * WIDE : (g + 1) * WIDE] = flat[k * GROUPS + g : k * GROUPS + g + 1, :]


def plane_windows(
    device, corners, spectrum, exchange, table_x, table_y, blocks, slots, fragment
):
    count_x, count_y = spectrum.shape
    block = kept((count_x // blocks, count_y))
    return small_call(
        lambda *refs: window_kernel(fragment, *refs),
        12,
        out_shape=[block] * blocks + [kept((slots, 1, PLANE))],
        in_specs=in_smem(1) + anywhere(1) + in_vmem(4),
        out_specs=in_vmem(blocks + 1),
        scratch_shapes=[
            pltpu.VMEM((count_y // LANES * (count_x + BOX), LANES), jnp.float32),
            pltpu.VMEM((slots * BOX, LANES), jnp.float32),
            pltpu.SMEM(corners.shape, jnp.int32),
            pltpu.SemaphoreType.DMA,
        ],
    )(device, corners, spectrum, exchange, table_x, table_y)


def output_kernel(base, device, corners, windows, *refs):
    *blocks, box, potential, copied = refs
    depth = windows.shape[0]
    row = corners[0:1, :]
    own = lax.broadcasted_iota(jnp.int32, row.shape, 1) == device[0]
    first = jnp.sum(jnp.where(own, row, 0)) - base(device[0])
    sub = lax.rem(device[0], len(blocks))
    copies = [
        pltpu.make_async_copy(block, potential.at[sub ^ d], copied.at[BOX + d])
        for d, block in enumerate(blocks)
    ]
    tall = len(blocks)
    over = lax.rem(first, tall)
    for t in range(1, BOX // tall):
        z = pl.ds(lax.rem(first - over + t * tall, depth), tall)
        i = pl.ds(t * tall - over, tall)
        copies.append(pltpu.make_async_copy(windows.at[z], box.at[i], copied.at[t]))
    for q in range(tall):
        z = jnp.where(q < over, lax.rem(first - over + BOX, depth), first - over) + q
        i = jnp.where(q < over, BOX, 0) + q - over
        copies.append(pltpu.make_async_copy(windows.at[z], box.at[i], copied.at[BOX + tall + q]))
    for copy in copies:
        copy.start()
    for copy in copies:
        copy.wait()


def outputs(device, corners, windows, blocks, base):
    count = len(blocks)
    return small_call(
        lambda *refs: output_kernel(base, *refs),
        4,
        out_shape=(
            jax.ShapeDtypeStruct((BOX, 1, PLANE), jnp.float32),
            jax.ShapeDtypeStruct((count,) + blocks[0].shape, jnp.float32),
        ),
        in_specs=in_smem(1) + in_vmem(1) + anywhere(1 + count),
        out_specs=tuple(anywhere(2)),
        scratch_shapes=[pltpu.SemaphoreType.DMA((BOX + 2 * count,))],
    )(device, corners, windows, *blocks)


def body(orbitals, occupations, patch_sign, corners, core_span, outer_density):
    slab_count = lax.axis_size("slab")
    sub_count = lax.axis_size("sub")
    devices = slab_count * sub_count
    z_dev, x_dev, count_y = outer_density.shape
    count_x = x_dev * sub_count
    count_z = z_dev * slab_count
    device = lax.axis_index("slab") * sub_count + lax.axis_index("sub")
    table_x = hartley(count_x)
    table_y = hartley(count_y)
    per_device = count_x * count_y // devices
    deep = max(1, per_device // count_y)
    table_z = hartley(count_z, deep)

    device = jnp.reshape(device, (1,))
    assert z_dev == sub_count
    reach = (BOX + z_dev - 2) // z_dev + 1
    if slab_count <= reach:
        slots, group = devices, KINDS

        def base(own):
            return 0

        def fragment(slot, own):
            return slot

        def spread(pieces):
            return lax.all_to_all(pieces, AXES, 0, 0, tiled=True)

        collect = spread
    else:
        slots, group = reach * sub_count, sub_count

        def base(own):
            return own - lax.rem(own, sub_count)

        def fragment(slot, own):
            away = slot // sub_count * sub_count
            return lax.rem(base(own) - away + devices, devices) + lax.rem(slot, sub_count)

        def passed(pieces, sign):
            pieces = pieces.reshape((reach, sub_count) + pieces.shape[1:])
            pieces = lax.all_to_all(pieces, "sub", 1, 1, tiled=True)
            moved = [pieces[0]]
            for d in range(1, reach):
                ring = [(i, (i + sign * d) % slab_count) for i in range(slab_count)]
                moved.append(lax.ppermute(pieces[d], "slab", ring))
            return jnp.concatenate(moved, axis=0)

        def spread(pieces):
            return passed(pieces, 1)

        def collect(pieces):
            return passed(pieces, -1)

    counts = (count_z, count_x, count_y)
    corners = corners.T
    arguments = [
        pltpu.with_memory_space_constraint(argument, pltpu.HBM)
        for argument in (corners, core_span, occupations, orbitals, outer_density)
    ]

    def swapped(blocks):
        return [
            lax.ppermute(block, "sub", [(i, i ^ d) for i in range(sub_count)]) if d else block
            for d, block in enumerate(blocks)
        ]

    blocks = outer_blocks(device, arguments.pop())
    blocks = swapped(blocks)
    pieces = core_pieces(device, *arguments, slots, base, counts)
    pieces, blocks = lax.optimization_barrier((pieces, blocks))
    pieces = spread(pieces)
    spectrum, exchange = plane_spectrum(device, pieces, group, table_x, table_y, blocks)
    chunk = (devices, deep, per_device // deep)
    spectrum = lax.all_to_all(spectrum.reshape(chunk), AXES, 0, 0, tiled=True)
    spectrum = column_hartree(
        spectrum.reshape(devices * deep, per_device // deep), table_z, device, counts
    )
    spectrum = lax.all_to_all(spectrum.reshape(chunk), AXES, 0, 0, tiled=True)
    *blocks, windows = plane_windows(
        device,
        corners,
        spectrum.reshape(count_x, count_y),
        exchange,
        table_x,
        table_y,
        sub_count,
        slots,
        fragment,
    )
    blocks = swapped(blocks)
    windows = collect(windows)
    box, potential = outputs(device, corners, windows, blocks, base)
    return (box.reshape(1, BOX * PLANE), potential)


def solution(mesh):
    placed = (
        P(("slab", "sub"), None, None),
        P(("slab", "sub"), None),
        P(("slab", "sub")),
        P(),
        P(("slab", "sub"), None),
        P("slab", "sub", None),
    )
    return jax.shard_map(
        body,
        mesh=mesh,
        in_specs=placed,
        out_specs=(P(("slab", "sub"), None), P("slab", "sub", None)),
        check_vma=False,
    )
```

```python
import math

import jax
import jax.numpy as jnp
import numpy as np
from jax import lax
from jax.experimental import pallas as pl
from jax.experimental.pallas import tpu as pltpu
from jax.sharding import PartitionSpec as P

BOX = 48
CORE = 32
PLANE = BOX * BOX
GROUPS = 6
WIDE = PLANE // GROUPS
PACK = CORE * CORE
LANES = 128
PIECE = PACK + LANES
KINDS = 8

spacing = 0.35
floor_density = 0.001

AXES = ("slab", "sub")


def exchange_correlation(density):
    clipped = jnp.maximum(density, floor_density)
    root = jnp.exp(jnp.log(clipped) * (1.0 / 3.0))
    radius = (0.75 / math.pi) ** (1.0 / 3.0) / root
    exchange = -((3.0 / math.pi) ** (1.0 / 3.0)) * root
    inverse = 1.0 / (radius + 7.8)
    return exchange - 0.44 * inverse - (0.44 / 3.0) * radius * inverse * inverse


def split_table(table):
    high = table.astype(np.float32).astype(jnp.bfloat16)
    low = (table - high.astype(np.float64)).astype(np.float32).astype(jnp.bfloat16)
    return np.stack([high, low])


def hartley(count, repeat=1):
    index = np.arange(count)
    angle = 2.0 * np.pi / count * (np.outer(index, index) % count)
    return split_table(np.kron(np.cos(angle) + np.sin(angle), np.eye(repeat)))


def parts(values):
    high = values.astype(jnp.bfloat16)
    low = (values - high.astype(jnp.float32)).astype(jnp.bfloat16)
    return high, low


def product(a, b):
    return jnp.dot(a, b, preferred_element_type=jnp.float32)


def table_times(table, values):
    high, low = parts(values)
    return product(table[0], high) + (product(table[0], low) + product(table[1], high))


def times_table(values, table):
    high, low = parts(values)
    return product(high, table[0]) + (product(high, table[1]) + product(low, table[0]))


def small_call(kernel, megabytes, **kwargs):
    limit = pltpu.CompilerParams(vmem_limit_bytes=megabytes * 2**20)
    return pl.pallas_call(kernel, compiler_params=limit, **kwargs)


def in_vmem(count):
    return [pl.BlockSpec(memory_space=pltpu.VMEM)] * count


def in_smem(count):
    return [pl.BlockSpec(memory_space=pltpu.SMEM)] * count


def anywhere(count):
    return [pl.BlockSpec(memory_space=pl.ANY)] * count


def at_once(slots):
    return next(n for n in (8, 4, 2, 1) if slots % n == 0)


def repeated(steps, step):
    together = next(n for n in (4, 3, 2, 1) if steps % n == 0)
    lax.fori_loop(0, steps, step, 0, unroll=together)


def kept(shape):
    return pltpu.VMEM(shape, jnp.float32)


def row_sums(tiles):
    row = lax.broadcasted_iota(jnp.int32, (8, LANES), 0)
    top = row < 4
    fours = [
        jnp.where(top, tiles[i], tiles[i + 4])
        + pltpu.roll(jnp.where(top, tiles[i + 4], tiles[i]), 4, 0)
        for i in range(4)
    ]
    for step in (2, 1):
        early = (row % (2 * step)) < step
        fours = [
            jnp.where(
                early,
                fours[i] + pltpu.roll(fours[i], 8 - step, 0),
                fours[i + step] + pltpu.roll(fours[i + step], step, 0),
            )
            for i in range(step)
        ]
    return fours[0]


def block_kernel(device, outer, *refs):
    *blocks, filled = refs
    sub = lax.rem(device[0], len(blocks))
    fills = [
        pltpu.make_async_copy(outer.at[sub ^ d], block, filled.at[d])
        for d, block in enumerate(blocks)
    ]
    for fill in fills:
        fill.start()
    for fill in fills:
        fill.wait()


def outer_blocks(device, outer):
    count = outer.shape[0]
    return small_call(
        block_kernel,
        4,
        out_shape=[kept(outer.shape[1:])] * count,
        in_specs=in_smem(1) + anywhere(1),
        out_specs=in_vmem(count),
        scratch_shapes=[pltpu.SemaphoreType.DMA((count,))],
    )(device, outer)


CHUNK = 8


def core_kernel(
    base, depth, count_x, count_y, device, corner_table, span_row, occupation_row, orbitals,
    out, buffer, sums, rows, corners, span, occupations, arrived, staged,
):
    own, slots, orbital_count = device[0], out.shape[0], orbitals.shape[1]
    scalars = [
        pltpu.make_async_copy(source, target, staged.at[n])
        for n, (source, target) in enumerate(
            [(span_row, span), (occupation_row, occupations), (corner_table, corners)]
        )
    ]
    for copy in scalars:
        copy.start()
    chunks = BOX // CHUNK
    copies = []
    for c in range(chunks):
        part = pl.ds(c * CHUNK * PLANE, CHUNK * PLANE)
        copies.append(
            pltpu.make_async_copy(orbitals.at[0, :, part], buffer.at[:, part], arrived.at[c])
        )
        copies[c].start()
    for copy in scalars:
        copy.wait()
    first_z, first_x, first_y = span[0, 0], span[0, 1], span[0, 2]
    len_z, len_x, len_y = span[0, 3], span[0, 4], span[0, 5]
    begin = jnp.minimum(first_z, BOX - CORE)
    orbital = lax.broadcasted_iota(jnp.int32, (orbital_count, LANES), 0)
    weight = jnp.zeros((orbital_count, LANES), jnp.int32)
    for o in range(orbital_count):
        weight = jnp.where(orbital == o, occupations[0, o], weight)
    sign = 1
    for length in (len_z, len_x, len_y):
        sign = jnp.where(length == CORE, sign, -sign)
    weight = (weight * sign).astype(jnp.float32)
    groups = CHUNK * GROUPS // 8
    tiles = WIDE // LANES
    ahead = chunks - CORE // CHUNK
    for c in range(ahead):
        copies[c].wait()
    for c in range(CORE // CHUNK):
        copies[c + ahead].wait()

        def add_rows(b, carry, c=c):
            for q in range(tiles):
                cells = []
                for s in range(8):
                    line = begin * GROUPS + (c * groups + b) * 8 + s
                    lane = pl.multiple_of(line * WIDE + q * LANES, LANES)
                    values = buffer[:, pl.ds(lane, LANES)].astype(jnp.float32)
                    values = values * values * weight
                    cells.append(sum(values[8 * h : 8 * h + 8] for h in range(orbital_count // 8)))
                at = pl.multiple_of((c * groups + b) * 8, 8)
                sums[pl.ds(at, 8), q * LANES : (q + 1) * LANES] = row_sums(cells)
            return carry

        lax.fori_loop(0, groups, add_rows, 0, unroll=True)
        count = 8 * groups
        for r in range(8):
            line = sums[c * count : (c + 1) * count, r * BOX : (r + 1) * BOX]
            rows[pl.ds(8 * c * count + r, count, stride=8), 0:BOX] = line

    start_z = lax.rem(corners[0, own] + first_z, depth) - base(own)
    start_x = lax.rem(corners[1, own] + first_x, count_x)
    start_y = lax.rem(corners[2, own] + first_y, count_y)
    row = lax.broadcasted_iota(jnp.int32, (8, LANES), 0)
    lane = lax.broadcasted_iota(jnp.int32, (8, LANES), 1)
    first = jnp.where(lane[0:1] == 0, start_x, start_y).astype(jnp.float32)

    many = at_once(slots)

    def pack(step, carry):
        turned = []
        for h in range(many):
            p = lax.rem(many * step + h - start_z + depth, depth)
            local = jnp.minimum(p + first_z - begin, CORE - 1)
            cells = rows[pl.ds(local * BOX + first_x, CORE), :]
            for q in range(4):
                turn = lax.rem(32 * q - first_y + LANES, LANES)
                turned.append(pltpu.roll(cells[8 * q : 8 * q + 8], turn, 1))
        for h in range(many):
            k = many * step + h
            held = lax.rem(k - start_z + depth, depth) < len_z
            packed = jnp.zeros((8, LANES), jnp.float32)
            for q in range(4):
                keep = (row + 8 * q < len_x) & (lane >= 32 * q) & (lane < 32 * q + len_y) & held
                packed = jnp.where(keep, turned[4 * h + q], packed)
            for s in range(8):
                out[k, :, s * LANES : (s + 1) * LANES] = packed[s : s + 1]
            out[k, :, PACK:PIECE] = first
        return carry

    repeated(slots // many, pack)


def core_pieces(device, corners, span, occupations, orbitals, slots, base, counts):
    orbital_count = orbitals.shape[1]
    return small_call(
        lambda *refs: core_kernel(base, *counts, *refs),
        8,
        out_shape=kept((slots, 1, PIECE)),
        in_specs=in_smem(1) + anywhere(4),
        out_specs=in_vmem(1)[0],
        scratch_shapes=[
            pltpu.VMEM((orbital_count, BOX * PLANE), orbitals.dtype),
            pltpu.VMEM((CORE * GROUPS, WIDE), jnp.float32),
            pltpu.VMEM((CORE * BOX + CORE, LANES), jnp.float32),
            pltpu.SMEM(corners.shape, jnp.int32),
            pltpu.SMEM(span.shape, jnp.int32),
            pltpu.SMEM(occupations.shape, jnp.int32),
            pltpu.SemaphoreType.DMA((BOX // CHUNK,)),
            pltpu.SemaphoreType.DMA((3,)),
        ],
        cost_estimate=pl.CostEstimate(flops=40_000_000, bytes_accessed=4_000_000, transcendentals=0),
    )(device, corners, span, occupations, orbitals)


def place_kernel(group, pieces, placed, packed):
    count_x, count_y = placed.shape
    groups = pieces.shape[0] // group
    column = lax.broadcasted_iota(jnp.int32, (count_x, CORE), 1)
    cell_x = lax.broadcasted_iota(jnp.int32, (count_x, CORE), 0)
    row = lax.broadcasted_iota(jnp.int32, (CORE, count_y), 0)
    cell_y = lax.broadcasted_iota(jnp.int32, (CORE, count_y), 1)
    lefts, rights = [], []
    for j in range(groups):
        total = pieces[j * group, :, 0:PACK]
        for m in range(1, group):
            total = total + pieces[j * group + m, :, 0:PACK]
        for s in range(8):
            packed[8 * j + s : 8 * j + s + 1, :] = total[:, s * LANES : (s + 1) * LANES]
        tile = packed[8 * j : 8 * j + 8, :]
        square = jnp.concatenate([tile[:, 32 * q : 32 * q + 32] for q in range(4)], axis=0)
        first = pieces[j * group, :, PACK : PACK + LANES].astype(jnp.int32)
        away_x = cell_x - first[:, 0:1]
        away_y = cell_y - first[:, 1:2]
        left = jnp.where(away_x < 0, away_x + count_x, away_x) == column
        right = jnp.where(away_y < 0, away_y + count_y, away_y) == row
        right = jnp.where(right, 1.0, 0.0).astype(jnp.bfloat16)
        high = square.astype(jnp.bfloat16)
        rest = square - high.astype(jnp.float32)
        middle = rest.astype(jnp.bfloat16)
        low = (rest - middle.astype(jnp.float32)).astype(jnp.bfloat16)
        lefts.append(jnp.where(left, 1.0, 0.0).astype(jnp.bfloat16))
        rights.append([product(part, right).astype(jnp.bfloat16) for part in (high, middle, low)])
    left = jnp.concatenate(lefts, axis=1)
    total = product(left, jnp.concatenate([r[2] for r in rights], axis=0))
    for part in (1, 0):
        total = total + product(left, jnp.concatenate([r[part] for r in rights], axis=0))
    placed[...] = total


def placed_cores(pieces, group, count_x, count_y):
    return small_call(
        lambda *refs: place_kernel(group, *refs),
        12,
        out_shape=kept((count_x, count_y)),
        in_specs=in_vmem(1),
        out_specs=in_vmem(1)[0],
        scratch_shapes=[pltpu.VMEM((8 * (pieces.shape[0] // group), LANES), jnp.float32)],
    )(pieces)


def plane_kernel(device, placed, table_x, table_y, *refs):
    *blocks, spectrum, exchange, outer = refs
    sub = lax.rem(device[0], len(blocks))
    x_dev = placed.shape[0] // len(blocks)
    for d, block in enumerate(blocks):
        outer[pl.ds(pl.multiple_of((sub ^ d) * x_dev, 8), x_dev), :] = block[...]
    density = outer[...] + placed[...]
    exchange[...] = exchange_correlation(density)
    spectrum[...] = times_table(table_times(table_x, density), table_y)


def plane_spectrum(device, placed, table_x, table_y, blocks):
    return small_call(
        plane_kernel,
        12,
        out_shape=(kept(placed.shape), kept(placed.shape)),
        in_specs=in_smem(1) + in_vmem(3 + len(blocks)),
        out_specs=in_vmem(2),
        scratch_shapes=[pltpu.VMEM(placed.shape, jnp.float32)],
    )(device, placed, table_x, table_y, *blocks)


def wave_squares(index, count):
    folded = jnp.where(index > count // 2, index - count, index)
    wave = 2.0 * math.pi / (count * spacing) * folded.astype(jnp.float32)
    return wave * wave


def column_kernel(count_z, count_x, count_y, device, values, table, out):
    rows, lanes = values.shape
    deep = rows // count_z
    transformed = table_times(table, values[...])
    row = lax.broadcasted_iota(jnp.int32, (rows, 1), 0)
    lane = lax.broadcasted_iota(jnp.int32, (1, lanes), 1)
    assert deep == 1 or lanes == count_y
    cell = (device[0] * deep + row % deep) * lanes
    square = (
        wave_squares(row // deep, count_z) + wave_squares(cell // count_y, count_x)
    ) + wave_squares(device[0] * deep * lanes % count_y + lane, count_y)
    scale = 4.0 * math.pi / float(count_z * count_x * count_y)
    kernel = jnp.where(square > 0, scale / jnp.where(square > 0, square, 1.0), 0.0)
    out[...] = table_times(table, transformed * kernel)


def column_hartree(values, table, device, counts):
    return small_call(
        lambda *refs: column_kernel(*counts, *refs),
        12,
        out_shape=kept(values.shape),
        in_specs=in_smem(1) + in_vmem(2),
        out_specs=in_vmem(1)[0],
    )(device, values, table)


def window_kernel(fragment, device, corner_table, spectrum, exchange, table_x, table_y, *refs):
    *blocks, out, wide, cut, corners, staged = refs
    scalars = pltpu.make_async_copy(corner_table, corners, staged)
    scalars.start()
    slots = out.shape[0]
    count_x, count_y = spectrum.shape
    x_dev = count_x // len(blocks)
    plane = times_table(table_times(table_x, spectrum[...]), table_y) + exchange[...]
    tall = count_x + BOX
    tiles = count_y // LANES
    for t in range(tiles):
        part = plane[:, t * LANES : (t + 1) * LANES]
        wide[t * tall : t * tall + count_x, :] = part
        wide[t * tall + count_x : (t + 1) * tall, :] = part[0:BOX]
    sub = lax.rem(device[0], len(blocks))
    for d, block in enumerate(blocks):
        for t in range(tiles):
            at = pl.multiple_of(t * tall + (sub ^ d) * x_dev, 8)
            block[:, t * LANES : (t + 1) * LANES] = wide[pl.ds(at, x_dev), :]
    lane = lax.broadcasted_iota(jnp.int32, (BOX, LANES), 1)
    scalars.wait()

    many = at_once(slots)

    def cut_windows(step, carry):
        turned = []
        for h in range(many):
            f = fragment(many * step + h, device[0])
            x, y = corners[1, f], corners[2, f]
            tile = y // LANES
            over = y - tile * LANES
            near = wide[pl.ds(tile * tall + x, BOX), :]
            far = wide[pl.ds(lax.rem(tile + 1, tiles) * tall + x, BOX), :]
            turn = lax.rem(LANES - over, LANES)
            turned.append(pltpu.roll(jnp.where(lane < over, far, near), turn, 1))
        for h in range(many):
            at = pl.multiple_of((many * step + h) * BOX, 8)
            cut[pl.ds(at, BOX), :] = turned[h]
        return carry

    repeated(slots // many, cut_windows)
    count = slots * GROUPS
    flat = jnp.concatenate(
        [cut[pl.ds(r, count, stride=8), :][:, 0:BOX] for r in range(8)], axis=1
    )
    for k in range(slots):
        for g in range(GROUPS):
            out[k, :, g * WIDE : (g + 1) * WIDE] = flat[k * GROUPS + g : k * GROUPS + g + 1, :]


def plane_windows(
    device, corners, spectrum, exchange, table_x, table_y, blocks, slots, fragment
):
    count_x, count_y = spectrum.shape
    block = kept((count_x // blocks, count_y))
    return small_call(
        lambda *refs: window_kernel(fragment, *refs),
        12,
        out_shape=[block] * blocks + [kept((slots, 1, PLANE))],
        in_specs=in_smem(1) + anywhere(1) + in_vmem(4),
        out_specs=in_vmem(blocks + 1),
        scratch_shapes=[
            pltpu.VMEM((count_y // LANES * (count_x + BOX), LANES), jnp.float32),
            pltpu.VMEM((slots * BOX, LANES), jnp.float32),
            pltpu.SMEM(corners.shape, jnp.int32),
            pltpu.SemaphoreType.DMA,
        ],
    )(device, corners, spectrum, exchange, table_x, table_y)


def output_kernel(base, device, corners, windows, *refs):
    *blocks, box, potential, copied = refs
    depth = windows.shape[0]
    row = corners[0:1, :]
    own = lax.broadcasted_iota(jnp.int32, row.shape, 1) == device[0]
    first = jnp.sum(jnp.where(own, row, 0)) - base(device[0])
    sub = lax.rem(device[0], len(blocks))
    copies = [
        pltpu.make_async_copy(block, potential.at[sub ^ d], copied.at[BOX + d])
        for d, block in enumerate(blocks)
    ]
    tall = len(blocks)
    over = lax.rem(first, tall)
    for t in range(1, BOX // tall):
        z = pl.ds(lax.rem(first - over + t * tall, depth), tall)
        i = pl.ds(t * tall - over, tall)
        copies.append(pltpu.make_async_copy(windows.at[z], box.at[i], copied.at[t]))
    for q in range(tall):
        z = jnp.where(q < over, lax.rem(first - over + BOX, depth), first - over) + q
        i = jnp.where(q < over, BOX, 0) + q - over
        copies.append(pltpu.make_async_copy(windows.at[z], box.at[i], copied.at[BOX + tall + q]))
    for copy in copies:
        copy.start()
    for copy in copies:
        copy.wait()


def outputs(device, corners, windows, blocks, base):
    count = len(blocks)
    return small_call(
        lambda *refs: output_kernel(base, *refs),
        4,
        out_shape=(
            jax.ShapeDtypeStruct((BOX, 1, PLANE), jnp.float32),
            jax.ShapeDtypeStruct((count,) + blocks[0].shape, jnp.float32),
        ),
        in_specs=in_smem(1) + in_vmem(1) + anywhere(1 + count),
        out_specs=tuple(anywhere(2)),
        scratch_shapes=[pltpu.SemaphoreType.DMA((BOX + 2 * count,))],
    )(device, corners, windows, *blocks)


def body(orbitals, occupations, patch_sign, corners, core_span, outer_density):
    slab_count = lax.axis_size("slab")
    sub_count = lax.axis_size("sub")
    devices = slab_count * sub_count
    z_dev, x_dev, count_y = outer_density.shape
    count_x = x_dev * sub_count
    count_z = z_dev * slab_count
    device = lax.axis_index("slab") * sub_count + lax.axis_index("sub")
    table_x = hartley(count_x)
    table_y = hartley(count_y)
    per_device = count_x * count_y // devices
    deep = max(1, per_device // count_y)
    table_z = hartley(count_z, deep)

    device = jnp.reshape(device, (1,))
    assert z_dev == sub_count
    reach = (BOX + z_dev - 2) // z_dev + 1
    if slab_count <= reach:
        slots, group = devices, KINDS

        def base(own):
            return 0

        def fragment(slot, own):
            return slot

        def spread(pieces):
            return lax.all_to_all(pieces, AXES, 0, 0, tiled=True)

        collect = spread
    else:
        slots, group = reach * sub_count, sub_count

        def base(own):
            return own - lax.rem(own, sub_count)

        def fragment(slot, own):
            away = slot // sub_count * sub_count
            return lax.rem(base(own) - away + devices, devices) + lax.rem(slot, sub_count)

        def passed(pieces, sign):
            pieces = pieces.reshape((reach, sub_count) + pieces.shape[1:])
            pieces = lax.all_to_all(pieces, "sub", 1, 1, tiled=True)
            moved = [pieces[0]]
            for d in range(1, reach):
                ring = [(i, (i + sign * d) % slab_count) for i in range(slab_count)]
                moved.append(lax.ppermute(pieces[d], "slab", ring))
            return jnp.concatenate(moved, axis=0)

        def spread(pieces):
            return passed(pieces, 1)

        def collect(pieces):
            return passed(pieces, -1)

    counts = (count_z, count_x, count_y)
    corners = corners.T
    arguments = [
        pltpu.with_memory_space_constraint(argument, pltpu.HBM)
        for argument in (corners, core_span, occupations, orbitals, outer_density)
    ]

    def swapped(blocks):
        return [
            lax.ppermute(block, "sub", [(i, i ^ d) for i in range(sub_count)]) if d else block
            for d, block in enumerate(blocks)
        ]

    blocks = outer_blocks(device, arguments.pop())
    blocks = swapped(blocks)
    pieces = spread(core_pieces(device, *arguments, slots, base, counts))
    placed = placed_cores(pieces, group, count_x, count_y)
    spectrum, exchange = plane_spectrum(device, placed, table_x, table_y, blocks)
    chunk = (devices, deep, per_device // deep)
    spectrum = lax.all_to_all(spectrum.reshape(chunk), AXES, 0, 0, tiled=True)
    spectrum = column_hartree(
        spectrum.reshape(devices * deep, per_device // deep), table_z, device, counts
    )
    spectrum = lax.all_to_all(spectrum.reshape(chunk), AXES, 0, 0, tiled=True)
    *blocks, windows = plane_windows(
        device,
        corners,
        spectrum.reshape(count_x, count_y),
        exchange,
        table_x,
        table_y,
        sub_count,
        slots,
        fragment,
    )
    blocks = swapped(blocks)
    windows = collect(windows)
    box, potential = outputs(device, corners, windows, blocks, base)
    return (box.reshape(1, BOX * PLANE), potential)


def solution(mesh):
    placed = (
        P(("slab", "sub"), None, None),
        P(("slab", "sub"), None),
        P(("slab", "sub")),
        P(),
        P(("slab", "sub"), None),
        P("slab", "sub", None),
    )
    return jax.shard_map(
        body,
        mesh=mesh,
        in_specs=placed,
        out_specs=(P(("slab", "sub"), None), P("slab", "sub", None)),
        check_vma=False,
    )
```

```python
import math

import jax
import jax.numpy as jnp
import numpy as np
from jax import lax
from jax.experimental import pallas as pl
from jax.experimental.pallas import tpu as pltpu
from jax.sharding import PartitionSpec as P

BOX = 48
CORE = 32
PLANE = BOX * BOX
GROUPS = 6
WIDE = PLANE // GROUPS
PACK = CORE * CORE
LANES = 128
PIECE = PACK + LANES
KINDS = 8

spacing = 0.35
floor_density = 0.001

AXES = ("slab", "sub")


def exchange_correlation(density):
    clipped = jnp.maximum(density, floor_density)
    root = jnp.exp(jnp.log(clipped) * (1.0 / 3.0))
    radius = (0.75 / math.pi) ** (1.0 / 3.0) / root
    exchange = -((3.0 / math.pi) ** (1.0 / 3.0)) * root
    inverse = 1.0 / (radius + 7.8)
    return exchange - 0.44 * inverse - (0.44 / 3.0) * radius * inverse * inverse


def split_table(table):
    high = table.astype(np.float32).astype(jnp.bfloat16)
    low = (table - high.astype(np.float64)).astype(np.float32).astype(jnp.bfloat16)
    return np.stack([high, low])


def hartley(count, repeat=1):
    index = np.arange(count)
    angle = 2.0 * np.pi / count * (np.outer(index, index) % count)
    return split_table(np.kron(np.cos(angle) + np.sin(angle), np.eye(repeat)))


def parts(values):
    high = values.astype(jnp.bfloat16)
    low = (values - high.astype(jnp.float32)).astype(jnp.bfloat16)
    return high, low


def product(a, b):
    return jnp.dot(a, b, preferred_element_type=jnp.float32)


def table_times(table, values):
    high, low = parts(values)
    return product(table[0], high) + (product(table[0], low) + product(table[1], high))


def times_table(values, table):
    high, low = parts(values)
    return product(high, table[0]) + (product(high, table[1]) + product(low, table[0]))


def small_call(kernel, megabytes, **kwargs):
    limit = pltpu.CompilerParams(vmem_limit_bytes=megabytes * 2**20)
    return pl.pallas_call(kernel, compiler_params=limit, **kwargs)


def in_vmem(count):
    return [pl.BlockSpec(memory_space=pltpu.VMEM)] * count


def in_smem(count):
    return [pl.BlockSpec(memory_space=pltpu.SMEM)] * count


def anywhere(count):
    return [pl.BlockSpec(memory_space=pl.ANY)] * count


def at_once(slots):
    return next(n for n in (8, 4, 2, 1) if slots % n == 0)


def repeated(steps, step):
    together = next(n for n in (4, 3, 2, 1) if steps % n == 0)
    lax.fori_loop(0, steps, step, 0, unroll=together)


def kept(shape):
    return pltpu.VMEM(shape, jnp.float32)


def row_sums(tiles):
    row = lax.broadcasted_iota(jnp.int32, (8, LANES), 0)
    top = row < 4
    fours = [
        jnp.where(top, tiles[i], tiles[i + 4])
        + pltpu.roll(jnp.where(top, tiles[i + 4], tiles[i]), 4, 0)
        for i in range(4)
    ]
    for step in (2, 1):
        early = (row % (2 * step)) < step
        fours = [
            jnp.where(
                early,
                fours[i] + pltpu.roll(fours[i], 8 - step, 0),
                fours[i + step] + pltpu.roll(fours[i + step], step, 0),
            )
            for i in range(step)
        ]
    return fours[0]


CHUNK = 8


def core_kernel(
    base, depth, count_x, count_y, device, corner_table, span_row, occupation_row, orbitals,
    outer, out, *refs,
):
    *blocks, buffer, sums, rows, corners, span, occupations, arrived, staged, filled = refs
    own, slots, orbital_count = device[0], out.shape[0], orbitals.shape[1]
    scalars = [
        pltpu.make_async_copy(source, target, staged.at[n])
        for n, (source, target) in enumerate(
            [(span_row, span), (occupation_row, occupations), (corner_table, corners)]
        )
    ]
    for copy in scalars:
        copy.start()
    chunks = BOX // CHUNK
    copies = []
    for c in range(chunks):
        part = pl.ds(c * CHUNK * PLANE, CHUNK * PLANE)
        copies.append(
            pltpu.make_async_copy(orbitals.at[0, :, part], buffer.at[:, part], arrived.at[c])
        )
        copies[c].start()
    sub = lax.rem(own, len(blocks))
    fills = [
        pltpu.make_async_copy(outer.at[sub ^ d], block, filled.at[d])
        for d, block in enumerate(blocks)
    ]
    for fill in fills:
        fill.start()
    for copy in scalars:
        copy.wait()
    first_z, first_x, first_y = span[0, 0], span[0, 1], span[0, 2]
    len_z, len_x, len_y = span[0, 3], span[0, 4], span[0, 5]
    begin = jnp.minimum(first_z, BOX - CORE)
    orbital = lax.broadcasted_iota(jnp.int32, (orbital_count, LANES), 0)
    weight = jnp.zeros((orbital_count, LANES), jnp.int32)
    for o in range(orbital_count):
        weight = jnp.where(orbital == o, occupations[0, o], weight)
    sign = 1
    for length in (len_z, len_x, len_y):
        sign = jnp.where(length == CORE, sign, -sign)
    weight = (weight * sign).astype(jnp.float32)
    groups = CHUNK * GROUPS // 8
    tiles = WIDE // LANES
    ahead = chunks - CORE // CHUNK
    for c in range(ahead):
        copies[c].wait()
    for c in range(CORE // CHUNK):
        copies[c + ahead].wait()

        def add_rows(b, carry, c=c):
            for q in range(tiles):
                cells = []
                for s in range(8):
                    line = begin * GROUPS + (c * groups + b) * 8 + s
                    lane = pl.multiple_of(line * WIDE + q * LANES, LANES)
                    values = buffer[:, pl.ds(lane, LANES)].astype(jnp.float32)
                    values = values * values * weight
                    cells.append(sum(values[8 * h : 8 * h + 8] for h in range(orbital_count // 8)))
                at = pl.multiple_of((c * groups + b) * 8, 8)
                sums[pl.ds(at, 8), q * LANES : (q + 1) * LANES] = row_sums(cells)
            return carry

        lax.fori_loop(0, groups, add_rows, 0, unroll=True)
        count = 8 * groups
        for r in range(8):
            line = sums[c * count : (c + 1) * count, r * BOX : (r + 1) * BOX]
            rows[pl.ds(8 * c * count + r, count, stride=8), 0:BOX] = line

    start_z = lax.rem(corners[0, own] + first_z, depth) - base(own)
    start_x = lax.rem(corners[1, own] + first_x, count_x)
    start_y = lax.rem(corners[2, own] + first_y, count_y)
    row = lax.broadcasted_iota(jnp.int32, (8, LANES), 0)
    lane = lax.broadcasted_iota(jnp.int32, (8, LANES), 1)
    first = jnp.where(lane[0:1] == 0, start_x, start_y).astype(jnp.float32)

    many = at_once(slots)

    def pack(step, carry):
        turned = []
        for h in range(many):
            p = lax.rem(many * step + h - start_z + depth, depth)
            local = jnp.minimum(p + first_z - begin, CORE - 1)
            cells = rows[pl.ds(local * BOX + first_x, CORE), :]
            for q in range(4):
                turn = lax.rem(32 * q - first_y + LANES, LANES)
                turned.append(pltpu.roll(cells[8 * q : 8 * q + 8], turn, 1))
        for h in range(many):
            k = many * step + h
            held = lax.rem(k - start_z + depth, depth) < len_z
            packed = jnp.zeros((8, LANES), jnp.float32)
            for q in range(4):
                keep = (row + 8 * q < len_x) & (lane >= 32 * q) & (lane < 32 * q + len_y) & held
                packed = jnp.where(keep, turned[4 * h + q], packed)
            for s in range(8):
                out[k, :, s * LANES : (s + 1) * LANES] = packed[s : s + 1]
            out[k, :, PACK:PIECE] = first
        return carry

    repeated(slots // many, pack)
    for fill in fills:
        fill.wait()


def core_pieces(device, corners, span, occupations, orbitals, outer, slots, base, counts):
    orbital_count = orbitals.shape[1]
    return small_call(
        lambda *refs: core_kernel(base, *counts, *refs),
        8,
        out_shape=[kept((slots, 1, PIECE))] + [kept(outer.shape[1:])] * outer.shape[0],
        in_specs=in_smem(1) + anywhere(5),
        out_specs=in_vmem(1 + outer.shape[0]),
        scratch_shapes=[
            pltpu.VMEM((orbital_count, BOX * PLANE), orbitals.dtype),
            pltpu.VMEM((CORE * GROUPS, WIDE), jnp.float32),
            pltpu.VMEM((CORE * BOX + CORE, LANES), jnp.float32),
            pltpu.SMEM(corners.shape, jnp.int32),
            pltpu.SMEM(span.shape, jnp.int32),
            pltpu.SMEM(occupations.shape, jnp.int32),
            pltpu.SemaphoreType.DMA((BOX // CHUNK,)),
            pltpu.SemaphoreType.DMA((3,)),
            pltpu.SemaphoreType.DMA((outer.shape[0],)),
        ],
        cost_estimate=pl.CostEstimate(flops=40_000_000, bytes_accessed=4_000_000, transcendentals=0),
    )(device, corners, span, occupations, orbitals, outer)


def place_kernel(group, pieces, placed, packed):
    count_x, count_y = placed.shape
    groups = pieces.shape[0] // group
    column = lax.broadcasted_iota(jnp.int32, (count_x, CORE), 1)
    cell_x = lax.broadcasted_iota(jnp.int32, (count_x, CORE), 0)
    row = lax.broadcasted_iota(jnp.int32, (CORE, count_y), 0)
    cell_y = lax.broadcasted_iota(jnp.int32, (CORE, count_y), 1)
    lefts, rights = [], []
    for j in range(groups):
        total = pieces[j * group, :, 0:PACK]
        for m in range(1, group):
            total = total + pieces[j * group + m, :, 0:PACK]
        for s in range(8):
            packed[8 * j + s : 8 * j + s + 1, :] = total[:, s * LANES : (s + 1) * LANES]
        tile = packed[8 * j : 8 * j + 8, :]
        square = jnp.concatenate([tile[:, 32 * q : 32 * q + 32] for q in range(4)], axis=0)
        first = pieces[j * group, :, PACK : PACK + LANES].astype(jnp.int32)
        away_x = cell_x - first[:, 0:1]
        away_y = cell_y - first[:, 1:2]
        left = jnp.where(away_x < 0, away_x + count_x, away_x) == column
        right = jnp.where(away_y < 0, away_y + count_y, away_y) == row
        right = jnp.where(right, 1.0, 0.0).astype(jnp.bfloat16)
        high = square.astype(jnp.bfloat16)
        rest = square - high.astype(jnp.float32)
        middle = rest.astype(jnp.bfloat16)
        low = (rest - middle.astype(jnp.float32)).astype(jnp.bfloat16)
        lefts.append(jnp.where(left, 1.0, 0.0).astype(jnp.bfloat16))
        rights.append([product(part, right).astype(jnp.bfloat16) for part in (high, middle, low)])
    left = jnp.concatenate(lefts, axis=1)
    total = product(left, jnp.concatenate([r[2] for r in rights], axis=0))
    for part in (1, 0):
        total = total + product(left, jnp.concatenate([r[part] for r in rights], axis=0))
    placed[...] = total


def placed_cores(pieces, group, count_x, count_y):
    return small_call(
        lambda *refs: place_kernel(group, *refs),
        12,
        out_shape=kept((count_x, count_y)),
        in_specs=in_vmem(1),
        out_specs=in_vmem(1)[0],
        scratch_shapes=[pltpu.VMEM((8 * (pieces.shape[0] // group), LANES), jnp.float32)],
    )(pieces)


def plane_kernel(device, placed, table_x, table_y, *refs):
    *blocks, spectrum, exchange, outer = refs
    sub = lax.rem(device[0], len(blocks))
    x_dev = placed.shape[0] // len(blocks)
    for d, block in enumerate(blocks):
        outer[pl.ds(pl.multiple_of((sub ^ d) * x_dev, 8), x_dev), :] = block[...]
    density = outer[...] + placed[...]
    exchange[...] = exchange_correlation(density)
    spectrum[...] = times_table(table_times(table_x, density), table_y)


def plane_spectrum(device, placed, table_x, table_y, blocks):
    return small_call(
        plane_kernel,
        12,
        out_shape=(kept(placed.shape), kept(placed.shape)),
        in_specs=in_smem(1) + in_vmem(3 + len(blocks)),
        out_specs=in_vmem(2),
        scratch_shapes=[pltpu.VMEM(placed.shape, jnp.float32)],
    )(device, placed, table_x, table_y, *blocks)


def wave_squares(index, count):
    folded = jnp.where(index > count // 2, index - count, index)
    wave = 2.0 * math.pi / (count * spacing) * folded.astype(jnp.float32)
    return wave * wave


def column_kernel(count_z, count_x, count_y, device, values, table, out):
    rows, lanes = values.shape
    deep = rows // count_z
    transformed = table_times(table, values[...])
    row = lax.broadcasted_iota(jnp.int32, (rows, 1), 0)
    lane = lax.broadcasted_iota(jnp.int32, (1, lanes), 1)
    assert deep == 1 or lanes == count_y
    cell = (device[0] * deep + row % deep) * lanes
    square = (
        wave_squares(row // deep, count_z) + wave_squares(cell // count_y, count_x)
    ) + wave_squares(device[0] * deep * lanes % count_y + lane, count_y)
    scale = 4.0 * math.pi / float(count_z * count_x * count_y)
    kernel = jnp.where(square > 0, scale / jnp.where(square > 0, square, 1.0), 0.0)
    out[...] = table_times(table, transformed * kernel)


def column_hartree(values, table, device, counts):
    return small_call(
        lambda *refs: column_kernel(*counts, *refs),
        12,
        out_shape=kept(values.shape),
        in_specs=in_smem(1) + in_vmem(2),
        out_specs=in_vmem(1)[0],
    )(device, values, table)


def window_kernel(fragment, device, corner_table, spectrum, exchange, table_x, table_y, *refs):
    *blocks, out, wide, cut, corners, staged = refs
    scalars = pltpu.make_async_copy(corner_table, corners, staged)
    scalars.start()
    slots = out.shape[0]
    count_x, count_y = spectrum.shape
    x_dev = count_x // len(blocks)
    plane = times_table(table_times(table_x, spectrum[...]), table_y) + exchange[...]
    tall = count_x + BOX
    tiles = count_y // LANES
    for t in range(tiles):
        part = plane[:, t * LANES : (t + 1) * LANES]
        wide[t * tall : t * tall + count_x, :] = part
        wide[t * tall + count_x : (t + 1) * tall, :] = part[0:BOX]
    sub = lax.rem(device[0], len(blocks))
    for d, block in enumerate(blocks):
        for t in range(tiles):
            at = pl.multiple_of(t * tall + (sub ^ d) * x_dev, 8)
            block[:, t * LANES : (t + 1) * LANES] = wide[pl.ds(at, x_dev), :]
    lane = lax.broadcasted_iota(jnp.int32, (BOX, LANES), 1)
    scalars.wait()

    many = at_once(slots)

    def cut_windows(step, carry):
        turned = []
        for h in range(many):
            f = fragment(many * step + h, device[0])
            x, y = corners[1, f], corners[2, f]
            tile = y // LANES
            over = y - tile * LANES
            near = wide[pl.ds(tile * tall + x, BOX), :]
            far = wide[pl.ds(lax.rem(tile + 1, tiles) * tall + x, BOX), :]
            turn = lax.rem(LANES - over, LANES)
            turned.append(pltpu.roll(jnp.where(lane < over, far, near), turn, 1))
        for h in range(many):
            at = pl.multiple_of((many * step + h) * BOX, 8)
            cut[pl.ds(at, BOX), :] = turned[h]
        return carry

    repeated(slots // many, cut_windows)
    count = slots * GROUPS
    flat = jnp.concatenate(
        [cut[pl.ds(r, count, stride=8), :][:, 0:BOX] for r in range(8)], axis=1
    )
    for k in range(slots):
        for g in range(GROUPS):
            out[k, :, g * WIDE : (g + 1) * WIDE] = flat[k * GROUPS + g : k * GROUPS + g + 1, :]


def plane_windows(
    device, corners, spectrum, exchange, table_x, table_y, blocks, slots, fragment
):
    count_x, count_y = spectrum.shape
    block = kept((count_x // blocks, count_y))
    return small_call(
        lambda *refs: window_kernel(fragment, *refs),
        12,
        out_shape=[block] * blocks + [kept((slots, 1, PLANE))],
        in_specs=in_smem(1) + anywhere(1) + in_vmem(4),
        out_specs=in_vmem(blocks + 1),
        scratch_shapes=[
            pltpu.VMEM((count_y // LANES * (count_x + BOX), LANES), jnp.float32),
            pltpu.VMEM((slots * BOX, LANES), jnp.float32),
            pltpu.SMEM(corners.shape, jnp.int32),
            pltpu.SemaphoreType.DMA,
        ],
    )(device, corners, spectrum, exchange, table_x, table_y)


def output_kernel(base, device, corners, windows, *refs):
    *blocks, box, potential, copied = refs
    depth = windows.shape[0]
    row = corners[0:1, :]
    own = lax.broadcasted_iota(jnp.int32, row.shape, 1) == device[0]
    first = jnp.sum(jnp.where(own, row, 0)) - base(device[0])
    sub = lax.rem(device[0], len(blocks))
    copies = [
        pltpu.make_async_copy(block, potential.at[sub ^ d], copied.at[BOX + d])
        for d, block in enumerate(blocks)
    ]
    tall = len(blocks)
    over = lax.rem(first, tall)
    for t in range(1, BOX // tall):
        z = pl.ds(lax.rem(first - over + t * tall, depth), tall)
        i = pl.ds(t * tall - over, tall)
        copies.append(pltpu.make_async_copy(windows.at[z], box.at[i], copied.at[t]))
    for q in range(tall):
        z = jnp.where(q < over, lax.rem(first - over + BOX, depth), first - over) + q
        i = jnp.where(q < over, BOX, 0) + q - over
        copies.append(pltpu.make_async_copy(windows.at[z], box.at[i], copied.at[BOX + tall + q]))
    for copy in copies:
        copy.start()
    for copy in copies:
        copy.wait()


def outputs(device, corners, windows, blocks, base):
    count = len(blocks)
    return small_call(
        lambda *refs: output_kernel(base, *refs),
        4,
        out_shape=(
            jax.ShapeDtypeStruct((BOX, 1, PLANE), jnp.float32),
            jax.ShapeDtypeStruct((count,) + blocks[0].shape, jnp.float32),
        ),
        in_specs=in_smem(1) + in_vmem(1) + anywhere(1 + count),
        out_specs=tuple(anywhere(2)),
        scratch_shapes=[pltpu.SemaphoreType.DMA((BOX + 2 * count,))],
    )(device, corners, windows, *blocks)


def body(orbitals, occupations, patch_sign, corners, core_span, outer_density):
    slab_count = lax.axis_size("slab")
    sub_count = lax.axis_size("sub")
    devices = slab_count * sub_count
    z_dev, x_dev, count_y = outer_density.shape
    count_x = x_dev * sub_count
    count_z = z_dev * slab_count
    device = lax.axis_index("slab") * sub_count + lax.axis_index("sub")
    table_x = hartley(count_x)
    table_y = hartley(count_y)
    per_device = count_x * count_y // devices
    deep = max(1, per_device // count_y)
    table_z = hartley(count_z, deep)

    device = jnp.reshape(device, (1,))
    assert z_dev == sub_count
    reach = (BOX + z_dev - 2) // z_dev + 1
    if slab_count <= reach:
        slots, group = devices, KINDS

        def base(own):
            return 0

        def fragment(slot, own):
            return slot

        def spread(pieces):
            return lax.all_to_all(pieces, AXES, 0, 0, tiled=True)

        collect = spread
    else:
        slots, group = reach * sub_count, sub_count

        def base(own):
            return own - lax.rem(own, sub_count)

        def fragment(slot, own):
            away = slot // sub_count * sub_count
            return lax.rem(base(own) - away + devices, devices) + lax.rem(slot, sub_count)

        def passed(pieces, sign):
            pieces = pieces.reshape((reach, sub_count) + pieces.shape[1:])
            pieces = lax.all_to_all(pieces, "sub", 1, 1, tiled=True)
            moved = [pieces[0]]
            for d in range(1, reach):
                ring = [(i, (i + sign * d) % slab_count) for i in range(slab_count)]
                moved.append(lax.ppermute(pieces[d], "slab", ring))
            return jnp.concatenate(moved, axis=0)

        def spread(pieces):
            return passed(pieces, 1)

        def collect(pieces):
            return passed(pieces, -1)

    counts = (count_z, count_x, count_y)
    corners = corners.T
    arguments = [
        pltpu.with_memory_space_constraint(argument, pltpu.HBM)
        for argument in (corners, core_span, occupations, orbitals, outer_density)
    ]

    def swapped(blocks):
        return [
            lax.ppermute(block, "sub", [(i, i ^ d) for i in range(sub_count)]) if d else block
            for d, block in enumerate(blocks)
        ]

    pieces, *blocks = core_pieces(device, *arguments, slots, base, counts)
    blocks = swapped(blocks)
    pieces = spread(pieces)
    placed = placed_cores(pieces, group, count_x, count_y)
    spectrum, exchange = plane_spectrum(device, placed, table_x, table_y, blocks)
    chunk = (devices, deep, per_device // deep)
    spectrum = lax.all_to_all(spectrum.reshape(chunk), AXES, 0, 0, tiled=True)
    spectrum = column_hartree(
        spectrum.reshape(devices * deep, per_device // deep), table_z, device, counts
    )
    spectrum = lax.all_to_all(spectrum.reshape(chunk), AXES, 0, 0, tiled=True)
    *blocks, windows = plane_windows(
        device,
        corners,
        spectrum.reshape(count_x, count_y),
        exchange,
        table_x,
        table_y,
        sub_count,
        slots,
        fragment,
    )
    blocks = swapped(blocks)
    windows = collect(windows)
    box, potential = outputs(device, corners, windows, blocks, base)
    return (box.reshape(1, BOX * PLANE), potential)


def solution(mesh):
    placed = (
        P(("slab", "sub"), None, None),
        P(("slab", "sub"), None),
        P(("slab", "sub")),
        P(),
        P(("slab", "sub"), None),
        P("slab", "sub", None),
    )
    return jax.shard_map(
        body,
        mesh=mesh,
        in_specs=placed,
        out_specs=(P(("slab", "sub"), None), P("slab", "sub", None)),
        check_vma=False,
    )
```

```python
import math

import jax
import jax.numpy as jnp
import numpy as np
from jax import lax
from jax.experimental import pallas as pl
from jax.experimental.pallas import tpu as pltpu
from jax.sharding import PartitionSpec as P

BOX = 48
CORE = 32
FIRST = 8
PLANE = BOX * BOX
GROUPS = 6
WIDE = PLANE // GROUPS
PACK = CORE * CORE
LANES = 128
PIECE = PACK + LANES
KINDS = 8

spacing = 0.35
floor_density = 0.001

AXES = ("slab", "sub")


def exchange_correlation(density):
    clipped = jnp.maximum(density, floor_density)
    root = jnp.exp(jnp.log(clipped) * (1.0 / 3.0))
    radius = (0.75 / math.pi) ** (1.0 / 3.0) / root
    exchange = -((3.0 / math.pi) ** (1.0 / 3.0)) * root
    inverse = 1.0 / (radius + 7.8)
    return exchange - 0.44 * inverse - (0.44 / 3.0) * radius * inverse * inverse


def split_table(table):
    high = table.astype(np.float32).astype(jnp.bfloat16)
    low = (table - high.astype(np.float64)).astype(np.float32).astype(jnp.bfloat16)
    return np.stack([high, low])


def hartley(count, repeat=1):
    index = np.arange(count)
    angle = 2.0 * np.pi / count * (np.outer(index, index) % count)
    return split_table(np.kron(np.cos(angle) + np.sin(angle), np.eye(repeat)))


def parts(values):
    high = values.astype(jnp.bfloat16)
    low = (values - high.astype(jnp.float32)).astype(jnp.bfloat16)
    return high, low


def product(a, b):
    return jnp.dot(a, b, preferred_element_type=jnp.float32)


def table_times(table, values):
    high, low = parts(values)
    return product(table[0], high) + (product(table[0], low) + product(table[1], high))


def times_table(values, table):
    high, low = parts(values)
    return product(high, table[0]) + (product(high, table[1]) + product(low, table[0]))


def small_call(kernel, megabytes, **kwargs):
    limit = pltpu.CompilerParams(vmem_limit_bytes=megabytes * 2**20)
    return pl.pallas_call(kernel, compiler_params=limit, **kwargs)


def in_vmem(count):
    return [pl.BlockSpec(memory_space=pltpu.VMEM)] * count


def in_smem(count):
    return [pl.BlockSpec(memory_space=pltpu.SMEM)] * count


def anywhere(count):
    return [pl.BlockSpec(memory_space=pl.ANY)] * count


def by_distance(blocks):
    return [((len(blocks) - n) % len(blocks), block) for n, block in enumerate(blocks)]


def at_once(slots):
    return next(n for n in (8, 4, 2, 1) if slots % n == 0)


def repeated(steps, step):
    together = next(n for n in (4, 3, 2, 1) if steps % n == 0)
    lax.fori_loop(0, steps, step, 0, unroll=together)


def kept(shape):
    return pltpu.VMEM(shape, jnp.float32)


def row_sums(tiles):
    row = lax.broadcasted_iota(jnp.int32, (8, LANES), 0)
    top = row < 4
    fours = [
        jnp.where(top, tiles[i], tiles[i + 4])
        + pltpu.roll(jnp.where(top, tiles[i + 4], tiles[i]), 4, 0)
        for i in range(4)
    ]
    for step in (2, 1):
        early = (row % (2 * step)) < step
        fours = [
            jnp.where(
                early,
                fours[i] + pltpu.roll(fours[i], 8 - step, 0),
                fours[i + step] + pltpu.roll(fours[i + step], step, 0),
            )
            for i in range(step)
        ]
    return fours[0]


CHUNK = 8


def core_kernel(
    base, depth, count_x, count_y, device, corner_table, span_row, occupation_row, orbitals,
    outer, out, *refs,
):
    *blocks, buffer, sums, rows, corners, span, occupations, arrived, staged, filled = refs
    own, slots, orbital_count = device[0], out.shape[0], orbitals.shape[1]
    scalars = [
        pltpu.make_async_copy(source, target, staged.at[n])
        for n, (source, target) in enumerate(
            [(span_row, span), (occupation_row, occupations), (corner_table, corners)]
        )
    ]
    for copy in scalars:
        copy.start()
    chunks = (BOX - FIRST) // CHUNK
    copies = []
    for c in range(chunks):
        part = pl.ds((FIRST + c * CHUNK) * PLANE, CHUNK * PLANE)
        room = pl.ds(c * CHUNK * PLANE, CHUNK * PLANE)
        copies.append(
            pltpu.make_async_copy(orbitals.at[0, :, part], buffer.at[:, room], arrived.at[c])
        )
        copies[c].start()
    sub = lax.rem(own, len(blocks))
    fills = [
        pltpu.make_async_copy(outer.at[sub ^ d], block, filled.at[d])
        for d, block in by_distance(blocks)
    ]
    for fill in fills:
        fill.start()
    for copy in scalars:
        copy.wait()
    first_z, first_x, first_y = span[0, 0], span[0, 1], span[0, 2]
    len_z, len_x, len_y = span[0, 3], span[0, 4], span[0, 5]
    begin = jnp.minimum(first_z, BOX - CORE)
    orbital = lax.broadcasted_iota(jnp.int32, (orbital_count, LANES), 0)
    weight = jnp.zeros((orbital_count, LANES), jnp.int32)
    for o in range(orbital_count):
        weight = jnp.where(orbital == o, occupations[0, o], weight)
    sign = 1
    for length in (len_z, len_x, len_y):
        sign = jnp.where(length == CORE, sign, -sign)
    weight = (weight * sign).astype(jnp.float32)
    groups = CHUNK * GROUPS // 8
    tiles = WIDE // LANES
    ahead = chunks - CORE // CHUNK
    for c in range(ahead):
        copies[c].wait()
    for c in range(CORE // CHUNK):
        copies[c + ahead].wait()

        def add_rows(b, carry, c=c):
            for q in range(tiles):
                cells = []
                for s in range(8):
                    line = (begin - FIRST) * GROUPS + (c * groups + b) * 8 + s
                    lane = pl.multiple_of(line * WIDE + q * LANES, LANES)
                    values = buffer[:, pl.ds(lane, LANES)].astype(jnp.float32)
                    values = values * values * weight
                    cells.append(sum(values[8 * h : 8 * h + 8] for h in range(orbital_count // 8)))
                at = pl.multiple_of((c * groups + b) * 8, 8)
                sums[pl.ds(at, 8), q * LANES : (q + 1) * LANES] = row_sums(cells)
            return carry

        lax.fori_loop(0, groups, add_rows, 0, unroll=True)
        count = 8 * groups
        for r in range(8):
            line = sums[c * count : (c + 1) * count, r * BOX : (r + 1) * BOX]
            rows[pl.ds(8 * c * count + r, count, stride=8), 0:BOX] = line

    start_z = lax.rem(corners[0, own] + first_z, depth) - base(own)
    start_x = lax.rem(corners[1, own] + first_x, count_x)
    start_y = lax.rem(corners[2, own] + first_y, count_y)
    row = lax.broadcasted_iota(jnp.int32, (8, LANES), 0)
    lane = lax.broadcasted_iota(jnp.int32, (8, LANES), 1)
    first = jnp.where(lane[0:1] == 0, start_x, start_y).astype(jnp.float32)

    many = at_once(slots)

    def pack(step, carry):
        turned = []
        for h in range(many):
            p = lax.rem(many * step + h - start_z + depth, depth)
            local = jnp.minimum(p + first_z - begin, CORE - 1)
            cells = rows[pl.ds(local * BOX + first_x, CORE), :]
            for q in range(4):
                turn = lax.rem(32 * q - first_y + LANES, LANES)
                turned.append(pltpu.roll(cells[8 * q : 8 * q + 8], turn, 1))
        for h in range(many):
            k = many * step + h
            held = lax.rem(k - start_z + depth, depth) < len_z
            packed = jnp.zeros((8, LANES), jnp.float32)
            for q in range(4):
                keep = (row + 8 * q < len_x) & (lane >= 32 * q) & (lane < 32 * q + len_y) & held
                packed = jnp.where(keep, turned[4 * h + q], packed)
            for s in range(8):
                out[k, :, s * LANES : (s + 1) * LANES] = packed[s : s + 1]
            out[k, :, PACK:PIECE] = first
        return carry

    repeated(slots // many, pack)
    for fill in fills:
        fill.wait()


def core_pieces(device, corners, span, occupations, orbitals, outer, slots, base, counts):
    orbital_count = orbitals.shape[1]
    return small_call(
        lambda *refs: core_kernel(base, *counts, *refs),
        8,
        out_shape=[kept((slots, 1, PIECE))] + [kept(outer.shape[1:])] * outer.shape[0],
        in_specs=in_smem(1) + anywhere(5),
        out_specs=in_vmem(1 + outer.shape[0]),
        scratch_shapes=[
            pltpu.VMEM((orbital_count, (BOX - FIRST) * PLANE), orbitals.dtype),
            pltpu.VMEM((CORE * GROUPS, WIDE), jnp.float32),
            pltpu.VMEM((CORE * BOX + CORE, LANES), jnp.float32),
            pltpu.SMEM(corners.shape, jnp.int32),
            pltpu.SMEM(span.shape, jnp.int32),
            pltpu.SMEM(occupations.shape, jnp.int32),
            pltpu.SemaphoreType.DMA(((BOX - FIRST) // CHUNK,)),
            pltpu.SemaphoreType.DMA((3,)),
            pltpu.SemaphoreType.DMA((outer.shape[0],)),
        ],
        cost_estimate=pl.CostEstimate(flops=40_000_000, bytes_accessed=4_000_000, transcendentals=0),
    )(device, corners, span, occupations, orbitals, outer)


def place_kernel(group, pieces, placed, packed):
    count_x, count_y = placed.shape
    groups = pieces.shape[0] // group
    column = lax.broadcasted_iota(jnp.int32, (count_x, CORE), 1)
    cell_x = lax.broadcasted_iota(jnp.int32, (count_x, CORE), 0)
    row = lax.broadcasted_iota(jnp.int32, (CORE, count_y), 0)
    cell_y = lax.broadcasted_iota(jnp.int32, (CORE, count_y), 1)
    lefts, rights = [], []
    for j in range(groups):
        total = pieces[j * group, :, 0:PACK]
        for m in range(1, group):
            total = total + pieces[j * group + m, :, 0:PACK]
        for s in range(8):
            packed[8 * j + s : 8 * j + s + 1, :] = total[:, s * LANES : (s + 1) * LANES]
        tile = packed[8 * j : 8 * j + 8, :]
        square = jnp.concatenate([tile[:, 32 * q : 32 * q + 32] for q in range(4)], axis=0)
        first = pieces[j * group, :, PACK : PACK + LANES].astype(jnp.int32)
        away_x = cell_x - first[:, 0:1]
        away_y = cell_y - first[:, 1:2]
        left = jnp.where(away_x < 0, away_x + count_x, away_x) == column
        right = jnp.where(away_y < 0, away_y + count_y, away_y) == row
        right = jnp.where(right, 1.0, 0.0).astype(jnp.bfloat16)
        high = square.astype(jnp.bfloat16)
        rest = square - high.astype(jnp.float32)
        middle = rest.astype(jnp.bfloat16)
        low = (rest - middle.astype(jnp.float32)).astype(jnp.bfloat16)
        lefts.append(jnp.where(left, 1.0, 0.0).astype(jnp.bfloat16))
        rights.append([product(part, right).astype(jnp.bfloat16) for part in (high, middle, low)])
    left = jnp.concatenate(lefts, axis=1)
    total = product(left, jnp.concatenate([r[2] for r in rights], axis=0))
    for part in (1, 0):
        total = total + product(left, jnp.concatenate([r[part] for r in rights], axis=0))
    placed[...] = total


def placed_cores(pieces, group, count_x, count_y):
    return small_call(
        lambda *refs: place_kernel(group, *refs),
        12,
        out_shape=kept((count_x, count_y)),
        in_specs=in_vmem(1),
        out_specs=in_vmem(1)[0],
        scratch_shapes=[pltpu.VMEM((8 * (pieces.shape[0] // group), LANES), jnp.float32)],
    )(pieces)


def plane_kernel(device, placed, table_x, table_y, *refs):
    *blocks, spectrum, exchange, outer = refs
    sub = lax.rem(device[0], len(blocks))
    x_dev = placed.shape[0] // len(blocks)
    for d, block in by_distance(blocks):
        outer[pl.ds(pl.multiple_of((sub ^ d) * x_dev, 8), x_dev), :] = block[...]
    density = outer[...] + placed[...]
    exchange[...] = exchange_correlation(density)
    spectrum[...] = times_table(table_times(table_x, density), table_y)


def plane_spectrum(device, placed, table_x, table_y, blocks):
    return small_call(
        plane_kernel,
        12,
        out_shape=(kept(placed.shape), kept(placed.shape)),
        in_specs=in_smem(1) + in_vmem(3 + len(blocks)),
        out_specs=in_vmem(2),
        scratch_shapes=[pltpu.VMEM(placed.shape, jnp.float32)],
    )(device, placed, table_x, table_y, *blocks)


def wave_squares(index, count):
    folded = jnp.where(index > count // 2, index - count, index)
    wave = 2.0 * math.pi / (count * spacing) * folded.astype(jnp.float32)
    return wave * wave


def column_kernel(count_z, count_x, count_y, device, values, table, out):
    rows, lanes = values.shape
    deep = rows // count_z
    transformed = table_times(table, values[...])
    row = lax.broadcasted_iota(jnp.int32, (rows, 1), 0)
    lane = lax.broadcasted_iota(jnp.int32, (1, lanes), 1)
    assert deep == 1 or lanes == count_y
    cell = (device[0] * deep + row % deep) * lanes
    square = (
        wave_squares(row // deep, count_z) + wave_squares(cell // count_y, count_x)
    ) + wave_squares(device[0] * deep * lanes % count_y + lane, count_y)
    scale = 4.0 * math.pi / float(count_z * count_x * count_y)
    kernel = jnp.where(square > 0, scale / jnp.where(square > 0, square, 1.0), 0.0)
    out[...] = table_times(table, transformed * kernel)


def column_hartree(values, table, device, counts):
    return small_call(
        lambda *refs: column_kernel(*counts, *refs),
        12,
        out_shape=kept(values.shape),
        in_specs=in_smem(1) + in_vmem(2),
        out_specs=in_vmem(1)[0],
    )(device, values, table)


def window_kernel(fragment, device, corner_table, spectrum, exchange, table_x, table_y, *refs):
    *blocks, out, wide, cut, corners, staged = refs
    scalars = pltpu.make_async_copy(corner_table, corners, staged)
    scalars.start()
    slots = out.shape[0]
    count_x, count_y = spectrum.shape
    x_dev = count_x // len(blocks)
    plane = times_table(table_times(table_x, spectrum[...]), table_y) + exchange[...]
    tall = count_x + BOX
    tiles = count_y // LANES
    for t in range(tiles):
        part = plane[:, t * LANES : (t + 1) * LANES]
        wide[t * tall : t * tall + count_x, :] = part
        wide[t * tall + count_x : (t + 1) * tall, :] = part[0:BOX]
    sub = lax.rem(device[0], len(blocks))
    for d, block in by_distance(blocks):
        for t in range(tiles):
            at = pl.multiple_of(t * tall + (sub ^ d) * x_dev, 8)
            block[:, t * LANES : (t + 1) * LANES] = wide[pl.ds(at, x_dev), :]
    lane = lax.broadcasted_iota(jnp.int32, (BOX, LANES), 1)
    scalars.wait()

    many = at_once(slots)

    def cut_windows(step, carry):
        turned = []
        for h in range(many):
            f = fragment(many * step + h, device[0])
            x, y = corners[1, f], corners[2, f]
            tile = y // LANES
            over = y - tile * LANES
            near = wide[pl.ds(tile * tall + x, BOX), :]
            far = wide[pl.ds(lax.rem(tile + 1, tiles) * tall + x, BOX), :]
            turn = lax.rem(LANES - over, LANES)
            turned.append(pltpu.roll(jnp.where(lane < over, far, near), turn, 1))
        for h in range(many):
            at = pl.multiple_of((many * step + h) * BOX, 8)
            cut[pl.ds(at, BOX), :] = turned[h]
        return carry

    repeated(slots // many, cut_windows)
    count = slots * GROUPS
    flat = jnp.concatenate(
        [cut[pl.ds(r, count, stride=8), :][:, 0:BOX] for r in range(8)], axis=1
    )
    for k in range(slots):
        for g in range(GROUPS):
            out[k, :, g * WIDE : (g + 1) * WIDE] = flat[k * GROUPS + g : k * GROUPS + g + 1, :]


def plane_windows(
    device, corners, spectrum, exchange, table_x, table_y, blocks, slots, fragment
):
    count_x, count_y = spectrum.shape
    block = kept((count_x // blocks, count_y))
    return small_call(
        lambda *refs: window_kernel(fragment, *refs),
        12,
        out_shape=[block] * blocks + [kept((slots, 1, PLANE))],
        in_specs=in_smem(1) + anywhere(1) + in_vmem(4),
        out_specs=in_vmem(blocks + 1),
        scratch_shapes=[
            pltpu.VMEM((count_y // LANES * (count_x + BOX), LANES), jnp.float32),
            pltpu.VMEM((slots * BOX, LANES), jnp.float32),
            pltpu.SMEM(corners.shape, jnp.int32),
            pltpu.SemaphoreType.DMA,
        ],
    )(device, corners, spectrum, exchange, table_x, table_y)


def output_kernel(base, device, corners, windows, *refs):
    *blocks, box, potential, copied = refs
    depth = windows.shape[0]
    row = corners[0:1, :]
    own = lax.broadcasted_iota(jnp.int32, row.shape, 1) == device[0]
    first = jnp.sum(jnp.where(own, row, 0)) - base(device[0])
    sub = lax.rem(device[0], len(blocks))
    copies = [
        pltpu.make_async_copy(block, potential.at[sub ^ d], copied.at[BOX + d])
        for d, block in by_distance(blocks)
    ]
    tall = len(blocks)
    over = lax.rem(first, tall)
    for t in range(1, BOX // tall):
        z = pl.ds(lax.rem(first - over + t * tall, depth), tall)
        i = pl.ds(t * tall - over, tall)
        copies.append(pltpu.make_async_copy(windows.at[z], box.at[i], copied.at[t]))
    for q in range(tall):
        z = jnp.where(q < over, lax.rem(first - over + BOX, depth), first - over) + q
        i = jnp.where(q < over, BOX, 0) + q - over
        copies.append(pltpu.make_async_copy(windows.at[z], box.at[i], copied.at[BOX + tall + q]))
    for copy in copies:
        copy.start()
    for copy in copies:
        copy.wait()


def outputs(device, corners, windows, blocks, base):
    count = len(blocks)
    return small_call(
        lambda *refs: output_kernel(base, *refs),
        4,
        out_shape=(
            jax.ShapeDtypeStruct((BOX, 1, PLANE), jnp.float32),
            jax.ShapeDtypeStruct((count,) + blocks[0].shape, jnp.float32),
        ),
        in_specs=in_smem(1) + in_vmem(1) + anywhere(1 + count),
        out_specs=tuple(anywhere(2)),
        scratch_shapes=[pltpu.SemaphoreType.DMA((BOX + 2 * count,))],
    )(device, corners, windows, *blocks)


def body(orbitals, occupations, patch_sign, corners, core_span, outer_density):
    slab_count = lax.axis_size("slab")
    sub_count = lax.axis_size("sub")
    devices = slab_count * sub_count
    z_dev, x_dev, count_y = outer_density.shape
    count_x = x_dev * sub_count
    count_z = z_dev * slab_count
    device = lax.axis_index("slab") * sub_count + lax.axis_index("sub")
    table_x = hartley(count_x)
    table_y = hartley(count_y)
    per_device = count_x * count_y // devices
    deep = max(1, per_device // count_y)
    table_z = hartley(count_z, deep)

    device = jnp.reshape(device, (1,))
    assert z_dev == sub_count
    reach = (BOX + z_dev - 2) // z_dev + 1
    if slab_count <= reach:
        slots, group = devices, KINDS

        def base(own):
            return 0

        def fragment(slot, own):
            return slot

        def spread(pieces):
            return lax.all_to_all(pieces, AXES, 0, 0, tiled=True)

        collect = spread
    else:
        slots, group = reach * sub_count, sub_count

        def base(own):
            return own - lax.rem(own, sub_count)

        def fragment(slot, own):
            away = slot // sub_count * sub_count
            return lax.rem(base(own) - away + devices, devices) + lax.rem(slot, sub_count)

        def passed(pieces, sign):
            pieces = pieces.reshape((reach, sub_count) + pieces.shape[1:])
            pieces = lax.all_to_all(pieces, "sub", 1, 1, tiled=True)
            moved = [pieces[0]]
            for d in range(1, reach):
                ring = [(i, (i + sign * d) % slab_count) for i in range(slab_count)]
                moved.append(lax.ppermute(pieces[d], "slab", ring))
            return jnp.concatenate(moved, axis=0)

        def spread(pieces):
            return passed(pieces, 1)

        def collect(pieces):
            return passed(pieces, -1)

    counts = (count_z, count_x, count_y)
    corners = corners.T
    arguments = [
        pltpu.with_memory_space_constraint(argument, pltpu.HBM)
        for argument in (corners, core_span, occupations, orbitals, outer_density)
    ]

    def swapped(blocks):
        return [
            lax.ppermute(block, "sub", [(i, i ^ d) for i in range(sub_count)]) if d else block
            for d, block in by_distance(blocks)
        ]

    pieces, *blocks = core_pieces(device, *arguments, slots, base, counts)
    blocks = swapped(blocks)
    pieces = spread(pieces)
    placed = placed_cores(pieces, group, count_x, count_y)
    spectrum, exchange = plane_spectrum(device, placed, table_x, table_y, blocks)
    chunk = (devices, deep, per_device // deep)
    spectrum = lax.all_to_all(spectrum.reshape(chunk), AXES, 0, 0, tiled=True)
    spectrum = column_hartree(
        spectrum.reshape(devices * deep, per_device // deep), table_z, device, counts
    )
    spectrum = lax.all_to_all(spectrum.reshape(chunk), AXES, 0, 0, tiled=True)
    *blocks, windows = plane_windows(
        device,
        corners,
        spectrum.reshape(count_x, count_y),
        exchange,
        table_x,
        table_y,
        sub_count,
        slots,
        fragment,
    )
    blocks = swapped(blocks)
    windows = collect(windows)
    box, potential = outputs(device, corners, windows, blocks, base)
    return (box.reshape(1, BOX * PLANE), potential)


def solution(mesh):
    placed = (
        P(("slab", "sub"), None, None),
        P(("slab", "sub"), None),
        P(("slab", "sub")),
        P(),
        P(("slab", "sub"), None),
        P("slab", "sub", None),
    )
    return jax.shard_map(
        body,
        mesh=mesh,
        in_specs=placed,
        out_specs=(P(("slab", "sub"), None), P("slab", "sub", None)),
        check_vma=False,
    )
```

```python
import math

import jax
import jax.numpy as jnp
import numpy as np
from jax import lax
from jax.experimental import pallas as pl
from jax.experimental.pallas import tpu as pltpu
from jax.sharding import PartitionSpec as P

BOX = 48
CORE = 32
FIRST = 8
PLANE = BOX * BOX
GROUPS = 6
WIDE = PLANE // GROUPS
PACK = CORE * CORE
LANES = 128
PIECE = PACK + LANES
KINDS = 8

spacing = 0.35
floor_density = 0.001

AXES = ("slab", "sub")


def exchange_correlation(density):
    clipped = jnp.maximum(density, floor_density)
    root = jnp.exp(jnp.log(clipped) * (1.0 / 3.0))
    radius = (0.75 / math.pi) ** (1.0 / 3.0) / root
    exchange = -((3.0 / math.pi) ** (1.0 / 3.0)) * root
    inverse = 1.0 / (radius + 7.8)
    return exchange - 0.44 * inverse - (0.44 / 3.0) * radius * inverse * inverse


def split_table(table):
    high = table.astype(np.float32).astype(jnp.bfloat16)
    low = (table - high.astype(np.float64)).astype(np.float32).astype(jnp.bfloat16)
    return np.stack([high, low])


def hartley(count, repeat=1):
    index = np.arange(count)
    angle = 2.0 * np.pi / count * (np.outer(index, index) % count)
    return split_table(np.kron(np.cos(angle) + np.sin(angle), np.eye(repeat)))


def parts(values):
    high = values.astype(jnp.bfloat16)
    low = (values - high.astype(jnp.float32)).astype(jnp.bfloat16)
    return high, low


def product(a, b):
    return jnp.dot(a, b, preferred_element_type=jnp.float32)


def table_times(table, values):
    high, low = parts(values)
    return product(table[0], high) + (product(table[0], low) + product(table[1], high))


def times_table(values, table):
    high, low = parts(values)
    return product(high, table[0]) + (product(high, table[1]) + product(low, table[0]))


def small_call(kernel, megabytes, **kwargs):
    limit = pltpu.CompilerParams(vmem_limit_bytes=megabytes * 2**20)
    return pl.pallas_call(kernel, compiler_params=limit, **kwargs)


def in_vmem(count):
    return [pl.BlockSpec(memory_space=pltpu.VMEM)] * count


def in_smem(count):
    return [pl.BlockSpec(memory_space=pltpu.SMEM)] * count


def anywhere(count):
    return [pl.BlockSpec(memory_space=pl.ANY)] * count


def at_once(slots):
    return next(n for n in (8, 4, 2, 1) if slots % n == 0)


def repeated(steps, step):
    together = next(n for n in (4, 3, 2, 1) if steps % n == 0)
    lax.fori_loop(0, steps, step, 0, unroll=together)


def kept(shape):
    return pltpu.VMEM(shape, jnp.float32)


def row_sums(tiles):
    row = lax.broadcasted_iota(jnp.int32, (8, LANES), 0)
    top = row < 4
    fours = [
        jnp.where(top, tiles[i], tiles[i + 4])
        + pltpu.roll(jnp.where(top, tiles[i + 4], tiles[i]), 4, 0)
        for i in range(4)
    ]
    for step in (2, 1):
        early = (row % (2 * step)) < step
        fours = [
            jnp.where(
                early,
                fours[i] + pltpu.roll(fours[i], 8 - step, 0),
                fours[i + step] + pltpu.roll(fours[i + step], step, 0),
            )
            for i in range(step)
        ]
    return fours[0]


CHUNK = 8


def core_kernel(
    base, depth, count_x, count_y, device, corner_table, span_row, occupation_row, orbitals,
    outer, out, *refs,
):
    *blocks, buffer, sums, rows, corners, span, occupations, arrived, staged, filled = refs
    own, slots, orbital_count = device[0], out.shape[0], orbitals.shape[1]
    scalars = [
        pltpu.make_async_copy(source, target, staged.at[n])
        for n, (source, target) in enumerate(
            [(span_row, span), (occupation_row, occupations), (corner_table, corners)]
        )
    ]
    for copy in scalars:
        copy.start()
    chunks = (BOX - FIRST) // CHUNK
    copies = []
    for c in range(chunks):
        part = pl.ds((FIRST + c * CHUNK) * PLANE, CHUNK * PLANE)
        room = pl.ds(c * CHUNK * PLANE, CHUNK * PLANE)
        copies.append(
            pltpu.make_async_copy(orbitals.at[0, :, part], buffer.at[:, room], arrived.at[c])
        )
        copies[c].start()
    sub = lax.rem(own, len(blocks))
    fills = [
        pltpu.make_async_copy(outer.at[sub ^ d], block, filled.at[d])
        for d, block in enumerate(blocks)
    ]
    for fill in fills:
        fill.start()
    for copy in scalars:
        copy.wait()
    first_z, first_x, first_y = span[0, 0], span[0, 1], span[0, 2]
    len_z, len_x, len_y = span[0, 3], span[0, 4], span[0, 5]
    begin = jnp.minimum(first_z, BOX - CORE)
    orbital = lax.broadcasted_iota(jnp.int32, (orbital_count, LANES), 0)
    weight = jnp.zeros((orbital_count, LANES), jnp.int32)
    for o in range(orbital_count):
        weight = jnp.where(orbital == o, occupations[0, o], weight)
    sign = 1
    for length in (len_z, len_x, len_y):
        sign = jnp.where(length == CORE, sign, -sign)
    weight = (weight * sign).astype(jnp.float32)
    groups = CHUNK * GROUPS // 8
    tiles = WIDE // LANES
    ahead = chunks - CORE // CHUNK
    for c in range(ahead):
        copies[c].wait()
    for c in range(CORE // CHUNK):
        copies[c + ahead].wait()

        def add_rows(b, carry, c=c):
            for q in range(tiles):
                cells = []
                for s in range(8):
                    line = (begin - FIRST) * GROUPS + (c * groups + b) * 8 + s
                    lane = pl.multiple_of(line * WIDE + q * LANES, LANES)
                    values = buffer[:, pl.ds(lane, LANES)].astype(jnp.float32)
                    values = values * values * weight
                    cells.append(sum(values[8 * h : 8 * h + 8] for h in range(orbital_count // 8)))
                at = pl.multiple_of((c * groups + b) * 8, 8)
                sums[pl.ds(at, 8), q * LANES : (q + 1) * LANES] = row_sums(cells)
            return carry

        lax.fori_loop(0, groups, add_rows, 0, unroll=True)
        count = 8 * groups
        for r in range(8):
            line = sums[c * count : (c + 1) * count, r * BOX : (r + 1) * BOX]
            rows[pl.ds(8 * c * count + r, count, stride=8), 0:BOX] = line

    start_z = lax.rem(corners[0, own] + first_z, depth) - base(own)
    start_x = lax.rem(corners[1, own] + first_x, count_x)
    start_y = lax.rem(corners[2, own] + first_y, count_y)
    row = lax.broadcasted_iota(jnp.int32, (8, LANES), 0)
    lane = lax.broadcasted_iota(jnp.int32, (8, LANES), 1)
    first = jnp.where(lane[0:1] == 0, start_x, start_y).astype(jnp.float32)

    many = at_once(slots)

    def pack(step, carry):
        turned = []
        for h in range(many):
            p = lax.rem(many * step + h - start_z + depth, depth)
            local = jnp.minimum(p + first_z - begin, CORE - 1)
            cells = rows[pl.ds(local * BOX + first_x, CORE), :]
            for q in range(4):
                turn = lax.rem(32 * q - first_y + LANES, LANES)
                turned.append(pltpu.roll(cells[8 * q : 8 * q + 8], turn, 1))
        for h in range(many):
            k = many * step + h
            held = lax.rem(k - start_z + depth, depth) < len_z
            packed = jnp.zeros((8, LANES), jnp.float32)
            for q in range(4):
                keep = (row + 8 * q < len_x) & (lane >= 32 * q) & (lane < 32 * q + len_y) & held
                packed = jnp.where(keep, turned[4 * h + q], packed)
            for s in range(8):
                out[k, :, s * LANES : (s + 1) * LANES] = packed[s : s + 1]
            out[k, :, PACK:PIECE] = first
        return carry

    repeated(slots // many, pack)
    for fill in fills:
        fill.wait()


def core_pieces(device, corners, span, occupations, orbitals, outer, slots, base, counts):
    orbital_count = orbitals.shape[1]
    return small_call(
        lambda *refs: core_kernel(base, *counts, *refs),
        8,
        out_shape=[kept((slots, 1, PIECE))] + [kept(outer.shape[1:])] * outer.shape[0],
        in_specs=in_smem(1) + anywhere(5),
        out_specs=in_vmem(1 + outer.shape[0]),
        scratch_shapes=[
            pltpu.VMEM((orbital_count, (BOX - FIRST) * PLANE), orbitals.dtype),
            pltpu.VMEM((CORE * GROUPS, WIDE), jnp.float32),
            pltpu.VMEM((CORE * BOX + CORE, LANES), jnp.float32),
            pltpu.SMEM(corners.shape, jnp.int32),
            pltpu.SMEM(span.shape, jnp.int32),
            pltpu.SMEM(occupations.shape, jnp.int32),
            pltpu.SemaphoreType.DMA(((BOX - FIRST) // CHUNK,)),
            pltpu.SemaphoreType.DMA((3,)),
            pltpu.SemaphoreType.DMA((outer.shape[0],)),
        ],
        cost_estimate=pl.CostEstimate(flops=40_000_000, bytes_accessed=4_000_000, transcendentals=0),
    )(device, corners, span, occupations, orbitals, outer)


def place_kernel(group, pieces, placed, packed):
    count_x, count_y = placed.shape
    groups = pieces.shape[0] // group
    column = lax.broadcasted_iota(jnp.int32, (count_x, CORE), 1)
    cell_x = lax.broadcasted_iota(jnp.int32, (count_x, CORE), 0)
    row = lax.broadcasted_iota(jnp.int32, (CORE, count_y), 0)
    cell_y = lax.broadcasted_iota(jnp.int32, (CORE, count_y), 1)
    lefts, rights = [], []
    for j in range(groups):
        total = pieces[j * group, :, 0:PACK]
        for m in range(1, group):
            total = total + pieces[j * group + m, :, 0:PACK]
        for s in range(8):
            packed[8 * j + s : 8 * j + s + 1, :] = total[:, s * LANES : (s + 1) * LANES]
        tile = packed[8 * j : 8 * j + 8, :]
        square = jnp.concatenate([tile[:, 32 * q : 32 * q + 32] for q in range(4)], axis=0)
        first = pieces[j * group, :, PACK : PACK + LANES].astype(jnp.int32)
        away_x = cell_x - first[:, 0:1]
        away_y = cell_y - first[:, 1:2]
        left = jnp.where(away_x < 0, away_x + count_x, away_x) == column
        right = jnp.where(away_y < 0, away_y + count_y, away_y) == row
        right = jnp.where(right, 1.0, 0.0).astype(jnp.bfloat16)
        high = square.astype(jnp.bfloat16)
        rest = square - high.astype(jnp.float32)
        middle = rest.astype(jnp.bfloat16)
        low = (rest - middle.astype(jnp.float32)).astype(jnp.bfloat16)
        lefts.append(jnp.where(left, 1.0, 0.0).astype(jnp.bfloat16))
        rights.append([product(part, right).astype(jnp.bfloat16) for part in (high, middle, low)])
    left = jnp.concatenate(lefts, axis=1)
    total = product(left, jnp.concatenate([r[2] for r in rights], axis=0))
    for part in (1, 0):
        total = total + product(left, jnp.concatenate([r[part] for r in rights], axis=0))
    placed[...] = total


def placed_cores(pieces, group, count_x, count_y):
    return small_call(
        lambda *refs: place_kernel(group, *refs),
        12,
        out_shape=kept((count_x, count_y)),
        in_specs=in_vmem(1),
        out_specs=in_vmem(1)[0],
        scratch_shapes=[pltpu.VMEM((8 * (pieces.shape[0] // group), LANES), jnp.float32)],
    )(pieces)


def plane_kernel(device, placed, table_x, table_y, *refs):
    *blocks, spectrum, exchange, outer = refs
    sub = lax.rem(device[0], len(blocks))
    x_dev = placed.shape[0] // len(blocks)
    for d, block in enumerate(blocks):
        outer[pl.ds(pl.multiple_of((sub ^ d) * x_dev, 8), x_dev), :] = block[...]
    density = outer[...] + placed[...]
    exchange[...] = exchange_correlation(density)
    spectrum[...] = times_table(table_times(table_x, density), table_y)


def plane_spectrum(device, placed, table_x, table_y, blocks):
    return small_call(
        plane_kernel,
        12,
        out_shape=(kept(placed.shape), kept(placed.shape)),
        in_specs=in_smem(1) + in_vmem(3 + len(blocks)),
        out_specs=in_vmem(2),
        scratch_shapes=[pltpu.VMEM(placed.shape, jnp.float32)],
    )(device, placed, table_x, table_y, *blocks)


def wave_squares(index, count):
    folded = jnp.where(index > count // 2, index - count, index)
    wave = 2.0 * math.pi / (count * spacing) * folded.astype(jnp.float32)
    return wave * wave


def column_kernel(count_z, count_x, count_y, device, values, table, out):
    rows, lanes = values.shape
    deep = rows // count_z
    transformed = table_times(table, values[...])
    row = lax.broadcasted_iota(jnp.int32, (rows, 1), 0)
    lane = lax.broadcasted_iota(jnp.int32, (1, lanes), 1)
    assert deep == 1 or lanes == count_y
    cell = (device[0] * deep + row % deep) * lanes
    square = (
        wave_squares(row // deep, count_z) + wave_squares(cell // count_y, count_x)
    ) + wave_squares(device[0] * deep * lanes % count_y + lane, count_y)
    scale = 4.0 * math.pi / float(count_z * count_x * count_y)
    kernel = jnp.where(square > 0, scale / jnp.where(square > 0, square, 1.0), 0.0)
    out[...] = table_times(table, transformed * kernel)


def column_hartree(values, table, device, counts):
    return small_call(
        lambda *refs: column_kernel(*counts, *refs),
        12,
        out_shape=kept(values.shape),
        in_specs=in_smem(1) + in_vmem(2),
        out_specs=in_vmem(1)[0],
    )(device, values, table)


def window_kernel(fragment, device, corner_table, spectrum, exchange, table_x, table_y, *refs):
    *blocks, out, wide, cut, corners, staged = refs
    scalars = pltpu.make_async_copy(corner_table, corners, staged)
    scalars.start()
    slots = out.shape[0]
    count_x, count_y = spectrum.shape
    x_dev = count_x // len(blocks)
    plane = times_table(table_times(table_x, spectrum[...]), table_y) + exchange[...]
    tall = count_x + BOX
    tiles = count_y // LANES
    for t in range(tiles):
        part = plane[:, t * LANES : (t + 1) * LANES]
        wide[t * tall : t * tall + count_x, :] = part
        wide[t * tall + count_x : (t + 1) * tall, :] = part[0:BOX]
    sub = lax.rem(device[0], len(blocks))
    for d, block in enumerate(blocks):
        for t in range(tiles):
            at = pl.multiple_of(t * tall + (sub ^ d) * x_dev, 8)
            block[:, t * LANES : (t + 1) * LANES] = wide[pl.ds(at, x_dev), :]
    lane = lax.broadcasted_iota(jnp.int32, (BOX, LANES), 1)
    scalars.wait()

    many = at_once(slots)

    def cut_windows(step, carry):
        turned = []
        for h in range(many):
            f = fragment(many * step + h, device[0])
            x, y = corners[1, f], corners[2, f]
            tile = y // LANES
            over = y - tile * LANES
            near = wide[pl.ds(tile * tall + x, BOX), :]
            far = wide[pl.ds(lax.rem(tile + 1, tiles) * tall + x, BOX), :]
            turn = lax.rem(LANES - over, LANES)
            turned.append(pltpu.roll(jnp.where(lane < over, far, near), turn, 1))
        for h in range(many):
            at = pl.multiple_of((many * step + h) * BOX, 8)
            cut[pl.ds(at, BOX), :] = turned[h]
        return carry

    repeated(slots // many, cut_windows)
    count = slots * GROUPS
    flat = jnp.concatenate(
        [cut[pl.ds(r, count, stride=8), :][:, 0:BOX] for r in range(8)], axis=1
    )
    for k in range(slots):
        for g in range(GROUPS):
            out[k, :, g * WIDE : (g + 1) * WIDE] = flat[k * GROUPS + g : k * GROUPS + g + 1, :]


def plane_windows(
    device, corners, spectrum, exchange, table_x, table_y, blocks, slots, fragment
):
    count_x, count_y = spectrum.shape
    block = kept((count_x // blocks, count_y))
    return small_call(
        lambda *refs: window_kernel(fragment, *refs),
        12,
        out_shape=[block] * blocks + [kept((slots, 1, PLANE))],
        in_specs=in_smem(1) + anywhere(1) + in_vmem(4),
        out_specs=in_vmem(blocks + 1),
        scratch_shapes=[
            pltpu.VMEM((count_y // LANES * (count_x + BOX), LANES), jnp.float32),
            pltpu.VMEM((slots * BOX, LANES), jnp.float32),
            pltpu.SMEM(corners.shape, jnp.int32),
            pltpu.SemaphoreType.DMA,
        ],
    )(device, corners, spectrum, exchange, table_x, table_y)


def output_kernel(base, device, corners, windows, *refs):
    *blocks, box, potential, copied = refs
    depth = windows.shape[0]
    row = corners[0:1, :]
    own = lax.broadcasted_iota(jnp.int32, row.shape, 1) == device[0]
    first = jnp.sum(jnp.where(own, row, 0)) - base(device[0])
    sub = lax.rem(device[0], len(blocks))
    copies = [
        pltpu.make_async_copy(block, potential.at[sub ^ d], copied.at[BOX + d])
        for d, block in enumerate(blocks)
    ]
    tall = len(blocks)
    over = lax.rem(first, tall)
    for t in range(1, BOX // tall):
        z = pl.ds(lax.rem(first - over + t * tall, depth), tall)
        i = pl.ds(t * tall - over, tall)
        copies.append(pltpu.make_async_copy(windows.at[z], box.at[i], copied.at[t]))
    for q in range(tall):
        z = jnp.where(q < over, lax.rem(first - over + BOX, depth), first - over) + q
        i = jnp.where(q < over, BOX, 0) + q - over
        copies.append(pltpu.make_async_copy(windows.at[z], box.at[i], copied.at[BOX + tall + q]))
    for copy in copies:
        copy.start()
    for copy in copies:
        copy.wait()


def outputs(device, corners, windows, blocks, base):
    count = len(blocks)
    return small_call(
        lambda *refs: output_kernel(base, *refs),
        4,
        out_shape=(
            jax.ShapeDtypeStruct((BOX, 1, PLANE), jnp.float32),
            jax.ShapeDtypeStruct((count,) + blocks[0].shape, jnp.float32),
        ),
        in_specs=in_smem(1) + in_vmem(1) + anywhere(1 + count),
        out_specs=tuple(anywhere(2)),
        scratch_shapes=[pltpu.SemaphoreType.DMA((BOX + 2 * count,))],
    )(device, corners, windows, *blocks)


def body(orbitals, occupations, patch_sign, corners, core_span, outer_density):
    slab_count = lax.axis_size("slab")
    sub_count = lax.axis_size("sub")
    devices = slab_count * sub_count
    z_dev, x_dev, count_y = outer_density.shape
    count_x = x_dev * sub_count
    count_z = z_dev * slab_count
    device = lax.axis_index("slab") * sub_count + lax.axis_index("sub")
    table_x = hartley(count_x)
    table_y = hartley(count_y)
    per_device = count_x * count_y // devices
    deep = max(1, per_device // count_y)
    table_z = hartley(count_z, deep)

    device = jnp.reshape(device, (1,))
    assert z_dev == sub_count
    reach = (BOX + z_dev - 2) // z_dev + 1
    if slab_count <= reach:
        slots, group = devices, KINDS

        def base(own):
            return 0

        def fragment(slot, own):
            return slot

        def spread(pieces):
            return lax.all_to_all(pieces, AXES, 0, 0, tiled=True)

        collect = spread
    else:
        slots, group = reach * sub_count, sub_count

        def base(own):
            return own - lax.rem(own, sub_count)

        def fragment(slot, own):
            away = slot // sub_count * sub_count
            return lax.rem(base(own) - away + devices, devices) + lax.rem(slot, sub_count)

        def passed(pieces, sign):
            pieces = pieces.reshape((reach, sub_count) + pieces.shape[1:])
            pieces = lax.all_to_all(pieces, "sub", 1, 1, tiled=True)
            moved = [pieces[0]]
            for d in range(1, reach):
                ring = [(i, (i + sign * d) % slab_count) for i in range(slab_count)]
                moved.append(lax.ppermute(pieces[d], "slab", ring))
            return jnp.concatenate(moved, axis=0)

        def spread(pieces):
            return passed(pieces, 1)

        def collect(pieces):
            return passed(pieces, -1)

    counts = (count_z, count_x, count_y)
    corners = corners.T
    arguments = [
        pltpu.with_memory_space_constraint(argument, pltpu.HBM)
        for argument in (corners, core_span, occupations, orbitals, outer_density)
    ]

    def swapped(blocks):
        return [
            lax.ppermute(block, "sub", [(i, i ^ d) for i in range(sub_count)]) if d else block
            for d, block in enumerate(blocks)
        ]

    pieces, *blocks = core_pieces(device, *arguments, slots, base, counts)
    blocks = swapped(blocks)
    pieces = spread(pieces)
    placed = placed_cores(pieces, group, count_x, count_y)
    spectrum, exchange = plane_spectrum(device, placed, table_x, table_y, blocks)
    chunk = (devices, deep, per_device // deep)
    spectrum = lax.all_to_all(spectrum.reshape(chunk), AXES, 0, 0, tiled=True)
    spectrum = column_hartree(
        spectrum.reshape(devices * deep, per_device // deep), table_z, device, counts
    )
    spectrum = lax.all_to_all(spectrum.reshape(chunk), AXES, 0, 0, tiled=True)
    *blocks, windows = plane_windows(
        device,
        corners,
        spectrum.reshape(count_x, count_y),
        exchange,
        table_x,
        table_y,
        sub_count,
        slots,
        fragment,
    )
    blocks = swapped(blocks)
    windows = collect(windows)
    box, potential = outputs(device, corners, windows, blocks, base)
    return (box.reshape(1, BOX * PLANE), potential)


def solution(mesh):
    placed = (
        P(("slab", "sub"), None, None),
        P(("slab", "sub"), None),
        P(("slab", "sub")),
        P(),
        P(("slab", "sub"), None),
        P("slab", "sub", None),
    )
    return jax.shard_map(
        body,
        mesh=mesh,
        in_specs=placed,
        out_specs=(P(("slab", "sub"), None), P("slab", "sub", None)),
        check_vma=False,
    )
```

```python
import math

import jax
import jax.numpy as jnp
import numpy as np
from jax import lax
from jax.experimental import pallas as pl
from jax.experimental.pallas import tpu as pltpu
from jax.sharding import PartitionSpec as P

BOX = 48
CORE = 32
FIRST = 8
PLANE = BOX * BOX
GROUPS = 6
WIDE = PLANE // GROUPS
PACK = CORE * CORE
LANES = 128
PIECE = PACK + LANES
KINDS = 8

spacing = 0.35
floor_density = 0.001

AXES = ("slab", "sub")


def exchange_correlation(density):
    clipped = jnp.maximum(density, floor_density)
    root = jnp.exp(jnp.log(clipped) * (1.0 / 3.0))
    radius = (0.75 / math.pi) ** (1.0 / 3.0) / root
    exchange = -((3.0 / math.pi) ** (1.0 / 3.0)) * root
    inverse = 1.0 / (radius + 7.8)
    return exchange - 0.44 * inverse - (0.44 / 3.0) * radius * inverse * inverse


def split_table(table):
    high = table.astype(np.float32).astype(jnp.bfloat16)
    low = (table - high.astype(np.float64)).astype(np.float32).astype(jnp.bfloat16)
    return np.stack([high, low])


def hartley(count, repeat=1):
    index = np.arange(count)
    angle = 2.0 * np.pi / count * (np.outer(index, index) % count)
    return split_table(np.kron(np.cos(angle) + np.sin(angle), np.eye(repeat)))


def parts(values):
    high = values.astype(jnp.bfloat16)
    low = (values - high.astype(jnp.float32)).astype(jnp.bfloat16)
    return high, low


def product(a, b):
    return jnp.dot(a, b, preferred_element_type=jnp.float32)


def table_times(table, values):
    high, low = parts(values)
    return product(table[0], high) + (product(table[0], low) + product(table[1], high))


def times_table(values, table):
    high, low = parts(values)
    return product(high, table[0]) + (product(high, table[1]) + product(low, table[0]))


def small_call(kernel, megabytes, **kwargs):
    limit = pltpu.CompilerParams(vmem_limit_bytes=megabytes * 2**20)
    return pl.pallas_call(kernel, compiler_params=limit, **kwargs)


def in_vmem(count):
    return [pl.BlockSpec(memory_space=pltpu.VMEM)] * count


def in_smem(count):
    return [pl.BlockSpec(memory_space=pltpu.SMEM)] * count


def anywhere(count):
    return [pl.BlockSpec(memory_space=pl.ANY)] * count


def at_once(slots):
    return next(n for n in (8, 4, 2, 1) if slots % n == 0)


def repeated(steps, step):
    together = next(n for n in (4, 3, 2, 1) if steps % n == 0)
    lax.fori_loop(0, steps, step, 0, unroll=together)


def kept(shape):
    return pltpu.VMEM(shape, jnp.float32)


def row_sums(tiles):
    row = lax.broadcasted_iota(jnp.int32, (8, LANES), 0)
    top = row < 4
    fours = [
        jnp.where(top, tiles[i], tiles[i + 4])
        + pltpu.roll(jnp.where(top, tiles[i + 4], tiles[i]), 4, 0)
        for i in range(4)
    ]
    for step in (2, 1):
        early = (row % (2 * step)) < step
        fours = [
            jnp.where(
                early,
                fours[i] + pltpu.roll(fours[i], 8 - step, 0),
                fours[i + step] + pltpu.roll(fours[i + step], step, 0),
            )
            for i in range(step)
        ]
    return fours[0]


CHUNK = 8


def core_kernel(
    base, depth, count_x, count_y, device, corner_table, span_row, occupation_row, orbitals,
    outer, out, *refs,
):
    *blocks, buffer, sums, rows, corners, span, occupations, arrived, staged, filled = refs
    own, slots, orbital_count = device[0], out.shape[0], orbitals.shape[1]
    scalars = [
        pltpu.make_async_copy(source, target, staged.at[n])
        for n, (source, target) in enumerate(
            [(span_row, span), (occupation_row, occupations), (corner_table, corners)]
        )
    ]
    for copy in scalars:
        copy.start()
    chunks = (BOX - FIRST) // CHUNK
    copies = []
    for c in range(chunks):
        part = pl.ds((FIRST + c * CHUNK) * PLANE, CHUNK * PLANE)
        room = pl.ds(c * CHUNK * PLANE, CHUNK * PLANE)
        copies.append(
            pltpu.make_async_copy(orbitals.at[0, :, part], buffer.at[:, room], arrived.at[c])
        )
        copies[c].start()
    sub = lax.rem(own, len(blocks))
    fills = [
        pltpu.make_async_copy(outer.at[sub ^ d], block, filled.at[d])
        for d, block in enumerate(blocks)
    ]
    for fill in fills:
        fill.start()
    for copy in scalars:
        copy.wait()
    first_z, first_x, first_y = span[0, 0], span[0, 1], span[0, 2]
    len_z, len_x, len_y = span[0, 3], span[0, 4], span[0, 5]
    begin = jnp.minimum(first_z, BOX - CORE)
    orbital = lax.broadcasted_iota(jnp.int32, (orbital_count, LANES), 0)
    weight = jnp.zeros((orbital_count, LANES), jnp.int32)
    for o in range(orbital_count):
        weight = jnp.where(orbital == o, occupations[0, o], weight)
    sign = 1
    for length in (len_z, len_x, len_y):
        sign = jnp.where(length == CORE, sign, -sign)
    weight = (weight * sign).astype(jnp.float32)
    groups = CHUNK * GROUPS // 8
    tiles = WIDE // LANES
    ahead = chunks - CORE // CHUNK
    for c in range(ahead):
        copies[c].wait()
    for c in range(CORE // CHUNK):
        copies[c + ahead].wait()

        def add_rows(b, carry, c=c):
            for q in range(tiles):
                cells = []
                for s in range(8):
                    line = (begin - FIRST) * GROUPS + (c * groups + b) * 8 + s
                    lane = pl.multiple_of(line * WIDE + q * LANES, LANES)
                    values = buffer[:, pl.ds(lane, LANES)].astype(jnp.float32)
                    values = values * values * weight
                    cells.append(sum(values[8 * h : 8 * h + 8] for h in range(orbital_count // 8)))
                at = pl.multiple_of((c * groups + b) * 8, 8)
                sums[pl.ds(at, 8), q * LANES : (q + 1) * LANES] = row_sums(cells)
            return carry

        lax.fori_loop(0, groups, add_rows, 0, unroll=True)
        count = 8 * groups
        for r in range(8):
            line = sums[c * count : (c + 1) * count, r * BOX : (r + 1) * BOX]
            rows[pl.ds(8 * c * count + r, count, stride=8), 0:BOX] = line

    start_z = lax.rem(corners[0, own] + first_z, depth) - base(own)
    start_x = lax.rem(corners[1, own] + first_x, count_x)
    start_y = lax.rem(corners[2, own] + first_y, count_y)
    row = lax.broadcasted_iota(jnp.int32, (8, LANES), 0)
    lane = lax.broadcasted_iota(jnp.int32, (8, LANES), 1)
    first = jnp.where(lane[0:1] == 0, start_x, start_y).astype(jnp.float32)

    many = at_once(slots)

    def pack(step, carry):
        turned = []
        for h in range(many):
            p = lax.rem(many * step + h - start_z + depth, depth)
            local = jnp.minimum(p + first_z - begin, CORE - 1)
            cells = rows[pl.ds(local * BOX + first_x, CORE), :]
            for q in range(4):
                turn = lax.rem(32 * q - first_y + LANES, LANES)
                turned.append(pltpu.roll(cells[8 * q : 8 * q + 8], turn, 1))
        for h in range(many):
            k = many * step + h
            held = lax.rem(k - start_z + depth, depth) < len_z
            packed = jnp.zeros((8, LANES), jnp.float32)
            for q in range(4):
                keep = (row + 8 * q < len_x) & (lane >= 32 * q) & (lane < 32 * q + len_y) & held
                packed = jnp.where(keep, turned[4 * h + q], packed)
            for s in range(8):
                out[k, :, s * LANES : (s + 1) * LANES] = packed[s : s + 1]
            out[k, :, PACK:PIECE] = first
        return carry

    repeated(slots // many, pack)
    for fill in fills:
        fill.wait()


def core_pieces(device, corners, span, occupations, orbitals, outer, slots, base, counts):
    orbital_count = orbitals.shape[1]
    return small_call(
        lambda *refs: core_kernel(base, *counts, *refs),
        8,
        out_shape=[kept((slots, 1, PIECE))] + [kept(outer.shape[1:])] * outer.shape[0],
        in_specs=in_smem(1) + anywhere(5),
        out_specs=in_vmem(1 + outer.shape[0]),
        scratch_shapes=[
            pltpu.VMEM((orbital_count, (BOX - FIRST) * PLANE), orbitals.dtype),
            pltpu.VMEM((CORE * GROUPS, WIDE), jnp.float32),
            pltpu.VMEM((CORE * BOX + CORE, LANES), jnp.float32),
            pltpu.SMEM(corners.shape, jnp.int32),
            pltpu.SMEM(span.shape, jnp.int32),
            pltpu.SMEM(occupations.shape, jnp.int32),
            pltpu.SemaphoreType.DMA(((BOX - FIRST) // CHUNK,)),
            pltpu.SemaphoreType.DMA((3,)),
            pltpu.SemaphoreType.DMA((outer.shape[0],)),
        ],
        cost_estimate=pl.CostEstimate(flops=40_000_000, bytes_accessed=4_000_000, transcendentals=0),
    )(device, corners, span, occupations, orbitals, outer)


def place_kernel(group, pieces, placed, packed):
    count_x, count_y = placed.shape
    groups = pieces.shape[0] // group
    row = lax.broadcasted_iota(jnp.int32, (CORE, count_y), 0)
    cell_y = lax.broadcasted_iota(jnp.int32, (CORE, count_y), 1)
    lane = lax.broadcasted_iota(jnp.int32, (1, groups * CORE), 1)
    first_x = jnp.zeros((1, groups * CORE), jnp.int32)
    highs, lows = [], []
    for j in range(groups):
        total = pieces[j * group, :, 0:PACK]
        for m in range(1, group):
            total = total + pieces[j * group + m, :, 0:PACK]
        for s in range(8):
            packed[8 * j + s : 8 * j + s + 1, :] = total[:, s * LANES : (s + 1) * LANES]
        tile = packed[8 * j : 8 * j + 8, :]
        square = jnp.concatenate([tile[:, 32 * q : 32 * q + 32] for q in range(4)], axis=0)
        first = pieces[j * group, :, PACK : PACK + LANES].astype(jnp.int32)
        first_x = jnp.where(lane // CORE == j, first[:, 0:1], first_x)
        away = cell_y - first[:, 1:2]
        right = jnp.where(away < 0, away + count_y, away) == row
        right = jnp.where(right, 1.0, 0.0).astype(jnp.bfloat16)
        high, low = parts(square)
        highs.append(product(high, right).astype(jnp.bfloat16))
        lows.append(product(low, right).astype(jnp.bfloat16))
    away = lax.broadcasted_iota(jnp.int32, (count_x, groups * CORE), 0) - first_x
    left = jnp.where(away < 0, away + count_x, away) == lane % CORE
    left = jnp.where(left, 1.0, 0.0).astype(jnp.bfloat16)
    total = product(left, jnp.concatenate(lows, axis=0))
    total = total + product(left, jnp.concatenate(highs, axis=0))
    placed[...] = total


def placed_cores(pieces, group, count_x, count_y):
    return small_call(
        lambda *refs: place_kernel(group, *refs),
        12,
        out_shape=kept((count_x, count_y)),
        in_specs=in_vmem(1),
        out_specs=in_vmem(1)[0],
        scratch_shapes=[pltpu.VMEM((8 * (pieces.shape[0] // group), LANES), jnp.float32)],
    )(pieces)


def plane_kernel(device, placed, table_x, table_y, *refs):
    *blocks, spectrum, exchange, outer = refs
    sub = lax.rem(device[0], len(blocks))
    x_dev = placed.shape[0] // len(blocks)
    for d, block in enumerate(blocks):
        outer[pl.ds(pl.multiple_of((sub ^ d) * x_dev, 8), x_dev), :] = block[...]
    density = outer[...] + placed[...]
    exchange[...] = exchange_correlation(density)
    spectrum[...] = times_table(table_times(table_x, density), table_y)


def plane_spectrum(device, placed, table_x, table_y, blocks):
    return small_call(
        plane_kernel,
        12,
        out_shape=(kept(placed.shape), kept(placed.shape)),
        in_specs=in_smem(1) + in_vmem(3 + len(blocks)),
        out_specs=in_vmem(2),
        scratch_shapes=[pltpu.VMEM(placed.shape, jnp.float32)],
    )(device, placed, table_x, table_y, *blocks)


def wave_squares(index, count):
    folded = jnp.where(index > count // 2, index - count, index)
    wave = 2.0 * math.pi / (count * spacing) * folded.astype(jnp.float32)
    return wave * wave


def column_kernel(count_z, count_x, count_y, device, values, table, out):
    rows, lanes = values.shape
    deep = rows // count_z
    transformed = table_times(table, values[...])
    row = lax.broadcasted_iota(jnp.int32, (rows, 1), 0)
    lane = lax.broadcasted_iota(jnp.int32, (1, lanes), 1)
    assert deep == 1 or lanes == count_y
    cell = (device[0] * deep + row % deep) * lanes
    square = (
        wave_squares(row // deep, count_z) + wave_squares(cell // count_y, count_x)
    ) + wave_squares(device[0] * deep * lanes % count_y + lane, count_y)
    scale = 4.0 * math.pi / float(count_z * count_x * count_y)
    kernel = jnp.where(square > 0, scale / jnp.where(square > 0, square, 1.0), 0.0)
    out[...] = table_times(table, transformed * kernel)


def column_hartree(values, table, device, counts):
    return small_call(
        lambda *refs: column_kernel(*counts, *refs),
        12,
        out_shape=kept(values.shape),
        in_specs=in_smem(1) + in_vmem(2),
        out_specs=in_vmem(1)[0],
    )(device, values, table)


def window_kernel(fragment, device, corner_table, spectrum, exchange, table_x, table_y, *refs):
    *blocks, out, wide, cut, corners, staged = refs
    scalars = pltpu.make_async_copy(corner_table, corners, staged)
    scalars.start()
    slots = out.shape[0]
    count_x, count_y = spectrum.shape
    x_dev = count_x // len(blocks)
    plane = times_table(table_times(table_x, spectrum[...]), table_y) + exchange[...]
    tall = count_x + BOX
    tiles = count_y // LANES
    for t in range(tiles):
        part = plane[:, t * LANES : (t + 1) * LANES]
        wide[t * tall : t * tall + count_x, :] = part
        wide[t * tall + count_x : (t + 1) * tall, :] = part[0:BOX]
    sub = lax.rem(device[0], len(blocks))
    for d, block in enumerate(blocks):
        for t in range(tiles):
            at = pl.multiple_of(t * tall + (sub ^ d) * x_dev, 8)
            block[:, t * LANES : (t + 1) * LANES] = wide[pl.ds(at, x_dev), :]
    lane = lax.broadcasted_iota(jnp.int32, (BOX, LANES), 1)
    scalars.wait()

    many = at_once(slots)

    def cut_windows(step, carry):
        turned = []
        for h in range(many):
            f = fragment(many * step + h, device[0])
            x, y = corners[1, f], corners[2, f]
            tile = y // LANES
            over = y - tile * LANES
            near = wide[pl.ds(tile * tall + x, BOX), :]
            far = wide[pl.ds(lax.rem(tile + 1, tiles) * tall + x, BOX), :]
            turn = lax.rem(LANES - over, LANES)
            turned.append(pltpu.roll(jnp.where(lane < over, far, near), turn, 1))
        for h in range(many):
            at = pl.multiple_of((many * step + h) * BOX, 8)
            cut[pl.ds(at, BOX), :] = turned[h]
        return carry

    repeated(slots // many, cut_windows)
    count = slots * GROUPS
    flat = jnp.concatenate(
        [cut[pl.ds(r, count, stride=8), :][:, 0:BOX] for r in range(8)], axis=1
    )
    for k in range(slots):
        for g in range(GROUPS):
            out[k, :, g * WIDE : (g + 1) * WIDE] = flat[k * GROUPS + g : k * GROUPS + g + 1, :]


def plane_windows(
    device, corners, spectrum, exchange, table_x, table_y, blocks, slots, fragment
):
    count_x, count_y = spectrum.shape
    block = kept((count_x // blocks, count_y))
    return small_call(
        lambda *refs: window_kernel(fragment, *refs),
        12,
        out_shape=[block] * blocks + [kept((slots, 1, PLANE))],
        in_specs=in_smem(1) + anywhere(1) + in_vmem(4),
        out_specs=in_vmem(blocks + 1),
        scratch_shapes=[
            pltpu.VMEM((count_y // LANES * (count_x + BOX), LANES), jnp.float32),
            pltpu.VMEM((slots * BOX, LANES), jnp.float32),
            pltpu.SMEM(corners.shape, jnp.int32),
            pltpu.SemaphoreType.DMA,
        ],
    )(device, corners, spectrum, exchange, table_x, table_y)


def output_kernel(base, device, corners, windows, *refs):
    *blocks, box, potential, copied = refs
    depth = windows.shape[0]
    sub = lax.rem(device[0], len(blocks))
    first_copies = [
        pltpu.make_async_copy(block, potential.at[sub ^ d], copied.at[BOX + d])
        for d, block in enumerate(blocks)
    ]
    for copy in first_copies:
        copy.start()
    row = corners[0:1, :]
    own = lax.broadcasted_iota(jnp.int32, row.shape, 1) == device[0]
    first = jnp.sum(jnp.where(own, row, 0)) - base(device[0])
    copies = []
    tall = len(blocks)
    over = lax.rem(first, tall)
    for t in range(1, BOX // tall):
        z = pl.ds(lax.rem(first - over + t * tall, depth), tall)
        i = pl.ds(t * tall - over, tall)
        copies.append(pltpu.make_async_copy(windows.at[z], box.at[i], copied.at[t]))
    for q in range(tall):
        z = jnp.where(q < over, lax.rem(first - over + BOX, depth), first - over) + q
        i = jnp.where(q < over, BOX, 0) + q - over
        copies.append(pltpu.make_async_copy(windows.at[z], box.at[i], copied.at[BOX + tall + q]))
    for copy in copies:
        copy.start()
    for copy in first_copies + copies:
        copy.wait()


def outputs(device, corners, windows, blocks, base):
    count = len(blocks)
    return small_call(
        lambda *refs: output_kernel(base, *refs),
        4,
        out_shape=(
            jax.ShapeDtypeStruct((BOX, 1, PLANE), jnp.float32),
            jax.ShapeDtypeStruct((count,) + blocks[0].shape, jnp.float32),
        ),
        in_specs=in_smem(1) + in_vmem(1) + anywhere(1 + count),
        out_specs=tuple(anywhere(2)),
        scratch_shapes=[pltpu.SemaphoreType.DMA((BOX + 2 * count,))],
    )(device, corners, windows, *blocks)


def body(orbitals, occupations, patch_sign, corners, core_span, outer_density):
    slab_count = lax.axis_size("slab")
    sub_count = lax.axis_size("sub")
    devices = slab_count * sub_count
    z_dev, x_dev, count_y = outer_density.shape
    count_x = x_dev * sub_count
    count_z = z_dev * slab_count
    device = lax.axis_index("slab") * sub_count + lax.axis_index("sub")
    table_x = hartley(count_x)
    table_y = hartley(count_y)
    per_device = count_x * count_y // devices
    deep = max(1, per_device // count_y)
    table_z = hartley(count_z, deep)

    device = jnp.reshape(device, (1,))
    assert z_dev == sub_count
    reach = (BOX + z_dev - 2) // z_dev + 1
    if slab_count <= reach:
        slots, group = devices, KINDS

        def base(own):
            return 0

        def fragment(slot, own):
            return slot

        def spread(pieces):
            return lax.all_to_all(pieces, AXES, 0, 0, tiled=True)

        collect = spread
    else:
        slots, group = reach * sub_count, sub_count

        def base(own):
            return own - lax.rem(own, sub_count)

        def fragment(slot, own):
            away = slot // sub_count * sub_count
            return lax.rem(base(own) - away + devices, devices) + lax.rem(slot, sub_count)

        def passed(pieces, sign):
            pieces = pieces.reshape((reach, sub_count) + pieces.shape[1:])
            pieces = lax.all_to_all(pieces, "sub", 1, 1, tiled=True)
            moved = [pieces[0]]
            for d in range(1, reach):
                ring = [(i, (i + sign * d) % slab_count) for i in range(slab_count)]
                moved.append(lax.ppermute(pieces[d], "slab", ring))
            return jnp.concatenate(moved, axis=0)

        def spread(pieces):
            return passed(pieces, 1)

        def collect(pieces):
            return passed(pieces, -1)

    counts = (count_z, count_x, count_y)
    corners = corners.T
    arguments = [
        pltpu.with_memory_space_constraint(argument, pltpu.HBM)
        for argument in (corners, core_span, occupations, orbitals, outer_density)
    ]

    def swapped(blocks):
        return [
            lax.ppermute(block, "sub", [(i, i ^ d) for i in range(sub_count)]) if d else block
            for d, block in enumerate(blocks)
        ]

    pieces, *blocks = core_pieces(device, *arguments, slots, base, counts)
    blocks = swapped(blocks)
    pieces = spread(pieces)
    placed = placed_cores(pieces, group, count_x, count_y)
    spectrum, exchange = plane_spectrum(device, placed, table_x, table_y, blocks)
    chunk = (devices, deep, per_device // deep)
    spectrum = lax.all_to_all(spectrum.reshape(chunk), AXES, 0, 0, tiled=True)
    spectrum = column_hartree(
        spectrum.reshape(devices * deep, per_device // deep), table_z, device, counts
    )
    spectrum = lax.all_to_all(spectrum.reshape(chunk), AXES, 0, 0, tiled=True)
    *blocks, windows = plane_windows(
        device,
        corners,
        spectrum.reshape(count_x, count_y),
        exchange,
        table_x,
        table_y,
        sub_count,
        slots,
        fragment,
    )
    blocks = swapped(blocks)
    windows = collect(windows)
    box, potential = outputs(device, corners, windows, blocks, base)
    return (box.reshape(1, BOX * PLANE), potential)


def solution(mesh):
    placed = (
        P(("slab", "sub"), None, None),
        P(("slab", "sub"), None),
        P(("slab", "sub")),
        P(),
        P(("slab", "sub"), None),
        P("slab", "sub", None),
    )
    return jax.shard_map(
        body,
        mesh=mesh,
        in_specs=placed,
        out_specs=(P(("slab", "sub"), None), P("slab", "sub", None)),
        check_vma=False,
    )
```

```python
import math

import jax
import jax.numpy as jnp
import numpy as np
from jax import lax
from jax.experimental import pallas as pl
from jax.experimental.pallas import tpu as pltpu
from jax.sharding import PartitionSpec as P

BOX = 48
CORE = 32
FIRST = 8
PLANE = BOX * BOX
GROUPS = 6
WIDE = PLANE // GROUPS
PACK = CORE * CORE
LANES = 128
PIECE = PACK + LANES
KINDS = 8

spacing = 0.35
floor_density = 0.001

AXES = ("slab", "sub")


def exchange_correlation(density):
    clipped = jnp.maximum(density, floor_density)
    root = jnp.exp(jnp.log(clipped) * (1.0 / 3.0))
    radius = (0.75 / math.pi) ** (1.0 / 3.0) / root
    exchange = -((3.0 / math.pi) ** (1.0 / 3.0)) * root
    inverse = 1.0 / (radius + 7.8)
    return exchange - 0.44 * inverse - (0.44 / 3.0) * radius * inverse * inverse


def split_table(table):
    high = table.astype(np.float32).astype(jnp.bfloat16)
    low = (table - high.astype(np.float64)).astype(np.float32).astype(jnp.bfloat16)
    return np.stack([high, low])


def hartley(count, repeat=1):
    index = np.arange(count)
    angle = 2.0 * np.pi / count * (np.outer(index, index) % count)
    return split_table(np.kron(np.cos(angle) + np.sin(angle), np.eye(repeat)))


def parts(values):
    high = values.astype(jnp.bfloat16)
    low = (values - high.astype(jnp.float32)).astype(jnp.bfloat16)
    return high, low


def product(a, b):
    return jnp.dot(a, b, preferred_element_type=jnp.float32)


def table_times(table, values):
    high, low = parts(values)
    return product(table[0], high) + (product(table[0], low) + product(table[1], high))


def times_table(values, table):
    high, low = parts(values)
    return product(high, table[0]) + (product(high, table[1]) + product(low, table[0]))


def small_call(kernel, megabytes, **kwargs):
    limit = pltpu.CompilerParams(vmem_limit_bytes=megabytes * 2**20)
    return pl.pallas_call(kernel, compiler_params=limit, **kwargs)


def in_vmem(count):
    return [pl.BlockSpec(memory_space=pltpu.VMEM)] * count


def in_smem(count):
    return [pl.BlockSpec(memory_space=pltpu.SMEM)] * count


def anywhere(count):
    return [pl.BlockSpec(memory_space=pl.ANY)] * count


def at_once(slots):
    return next(n for n in (8, 4, 2, 1) if slots % n == 0)


def repeated(steps, step):
    together = next(n for n in (4, 3, 2, 1) if steps % n == 0)
    lax.fori_loop(0, steps, step, 0, unroll=together)


def kept(shape):
    return pltpu.VMEM(shape, jnp.float32)


def row_sums(tiles):
    row = lax.broadcasted_iota(jnp.int32, (8, LANES), 0)
    top = row < 4
    fours = [
        jnp.where(top, tiles[i], tiles[i + 4])
        + pltpu.roll(jnp.where(top, tiles[i + 4], tiles[i]), 4, 0)
        for i in range(4)
    ]
    for step in (2, 1):
        early = (row % (2 * step)) < step
        fours = [
            jnp.where(
                early,
                fours[i] + pltpu.roll(fours[i], 8 - step, 0),
                fours[i + step] + pltpu.roll(fours[i + step], step, 0),
            )
            for i in range(step)
        ]
    return fours[0]


CHUNK = 8


def core_kernel(
    base, depth, count_x, count_y, device, corner_table, span_row, occupation_row, orbitals,
    outer, out, *refs,
):
    *blocks, buffer, sums, rows, corners, span, occupations, arrived, staged, filled = refs
    own, slots, orbital_count = device[0], out.shape[0], orbitals.shape[1]
    scalars = [
        pltpu.make_async_copy(source, target, staged.at[n])
        for n, (source, target) in enumerate(
            [(span_row, span), (occupation_row, occupations), (corner_table, corners)]
        )
    ]
    for copy in scalars:
        copy.start()
    chunks = (BOX - FIRST) // CHUNK
    copies = []
    for c in range(chunks):
        part = pl.ds((FIRST + c * CHUNK) * PLANE, CHUNK * PLANE)
        room = pl.ds(c * CHUNK * PLANE, CHUNK * PLANE)
        copies.append(
            pltpu.make_async_copy(orbitals.at[0, :, part], buffer.at[:, room], arrived.at[c])
        )
        copies[c].start()
    sub = lax.rem(own, len(blocks))
    fills = [
        pltpu.make_async_copy(outer.at[sub ^ d], block, filled.at[d])
        for d, block in enumerate(blocks)
    ]
    for fill in fills:
        fill.start()
    for copy in scalars:
        copy.wait()
    first_z, first_x, first_y = span[0, 0], span[0, 1], span[0, 2]
    len_z, len_x, len_y = span[0, 3], span[0, 4], span[0, 5]
    begin = jnp.minimum(first_z, BOX - CORE)
    orbital = lax.broadcasted_iota(jnp.int32, (orbital_count, LANES), 0)
    weight = jnp.zeros((orbital_count, LANES), jnp.int32)
    for o in range(orbital_count):
        weight = jnp.where(orbital == o, occupations[0, o], weight)
    sign = 1
    for length in (len_z, len_x, len_y):
        sign = jnp.where(length == CORE, sign, -sign)
    weight = (weight * sign).astype(jnp.float32)
    groups = CHUNK * GROUPS // 8
    tiles = WIDE // LANES
    ahead = chunks - CORE // CHUNK
    for c in range(ahead):
        copies[c].wait()
    for c in range(CORE // CHUNK):
        copies[c + ahead].wait()

        def add_rows(b, carry, c=c):
            for q in range(tiles):
                cells = []
                for s in range(8):
                    line = (begin - FIRST) * GROUPS + (c * groups + b) * 8 + s
                    lane = pl.multiple_of(line * WIDE + q * LANES, LANES)
                    values = buffer[:, pl.ds(lane, LANES)].astype(jnp.float32)
                    values = values * values * weight
                    cells.append(sum(values[8 * h : 8 * h + 8] for h in range(orbital_count // 8)))
                at = pl.multiple_of((c * groups + b) * 8, 8)
                sums[pl.ds(at, 8), q * LANES : (q + 1) * LANES] = row_sums(cells)
            return carry

        lax.fori_loop(0, groups, add_rows, 0, unroll=True)
        count = 8 * groups
        for r in range(8):
            line = sums[c * count : (c + 1) * count, r * BOX : (r + 1) * BOX]
            rows[pl.ds(8 * c * count + r, count, stride=8), 0:BOX] = line

    start_z = lax.rem(corners[0, own] + first_z, depth) - base(own)
    start_x = lax.rem(corners[1, own] + first_x, count_x)
    start_y = lax.rem(corners[2, own] + first_y, count_y)
    row = lax.broadcasted_iota(jnp.int32, (8, LANES), 0)
    lane = lax.broadcasted_iota(jnp.int32, (8, LANES), 1)
    first = jnp.where(lane[0:1] == 0, start_x, start_y).astype(jnp.float32)

    many = at_once(slots)

    def pack(step, carry):
        turned = []
        for h in range(many):
            p = lax.rem(many * step + h - start_z + depth, depth)
            local = jnp.minimum(p + first_z - begin, CORE - 1)
            cells = rows[pl.ds(local * BOX + first_x, CORE), :]
            for q in range(4):
                turn = lax.rem(32 * q - first_y + LANES, LANES)
                turned.append(pltpu.roll(cells[8 * q : 8 * q + 8], turn, 1))
        for h in range(many):
            k = many * step + h
            held = lax.rem(k - start_z + depth, depth) < len_z
            packed = jnp.zeros((8, LANES), jnp.float32)
            for q in range(4):
                keep = (row + 8 * q < len_x) & (lane >= 32 * q) & (lane < 32 * q + len_y) & held
                packed = jnp.where(keep, turned[4 * h + q], packed)
            for s in range(8):
                out[k, :, s * LANES : (s + 1) * LANES] = packed[s : s + 1]
            out[k, :, PACK:PIECE] = first
        return carry

    repeated(slots // many, pack)
    for fill in fills:
        fill.wait()


def core_pieces(device, corners, span, occupations, orbitals, outer, slots, base, counts):
    orbital_count = orbitals.shape[1]
    return small_call(
        lambda *refs: core_kernel(base, *counts, *refs),
        8,
        out_shape=[kept((slots, 1, PIECE))] + [kept(outer.shape[1:])] * outer.shape[0],
        in_specs=in_smem(1) + anywhere(5),
        out_specs=in_vmem(1 + outer.shape[0]),
        scratch_shapes=[
            pltpu.VMEM((orbital_count, (BOX - FIRST) * PLANE), orbitals.dtype),
            pltpu.VMEM((CORE * GROUPS, WIDE), jnp.float32),
            pltpu.VMEM((CORE * BOX + CORE, LANES), jnp.float32),
            pltpu.SMEM(corners.shape, jnp.int32),
            pltpu.SMEM(span.shape, jnp.int32),
            pltpu.SMEM(occupations.shape, jnp.int32),
            pltpu.SemaphoreType.DMA(((BOX - FIRST) // CHUNK,)),
            pltpu.SemaphoreType.DMA((3,)),
            pltpu.SemaphoreType.DMA((outer.shape[0],)),
        ],
        cost_estimate=pl.CostEstimate(flops=40_000_000, bytes_accessed=4_000_000, transcendentals=0),
    )(device, corners, span, occupations, orbitals, outer)


def place_kernel(group, pieces, placed, packed):
    count_x, count_y = placed.shape
    groups = pieces.shape[0] // group
    column = lax.broadcasted_iota(jnp.int32, (count_x, CORE), 1)
    cell_x = lax.broadcasted_iota(jnp.int32, (count_x, CORE), 0)
    row = lax.broadcasted_iota(jnp.int32, (CORE, count_y), 0)
    cell_y = lax.broadcasted_iota(jnp.int32, (CORE, count_y), 1)
    lefts, rights = [], []
    for j in range(groups):
        total = pieces[j * group, :, 0:PACK]
        for m in range(1, group):
            total = total + pieces[j * group + m, :, 0:PACK]
        for s in range(8):
            packed[8 * j + s : 8 * j + s + 1, :] = total[:, s * LANES : (s + 1) * LANES]
        tile = packed[8 * j : 8 * j + 8, :]
        square = jnp.concatenate([tile[:, 32 * q : 32 * q + 32] for q in range(4)], axis=0)
        first = pieces[j * group, :, PACK : PACK + LANES].astype(jnp.int32)
        away_x = cell_x - first[:, 0:1]
        away_y = cell_y - first[:, 1:2]
        left = jnp.where(away_x < 0, away_x + count_x, away_x) == column
        right = jnp.where(away_y < 0, away_y + count_y, away_y) == row
        right = jnp.where(right, 1.0, 0.0).astype(jnp.bfloat16)
        high = square.astype(jnp.bfloat16)
        rest = square - high.astype(jnp.float32)
        middle = rest.astype(jnp.bfloat16)
        low = (rest - middle.astype(jnp.float32)).astype(jnp.bfloat16)
        lefts.append(jnp.where(left, 1.0, 0.0).astype(jnp.bfloat16))
        rights.append([product(part, right).astype(jnp.bfloat16) for part in (high, middle, low)])
    left = jnp.concatenate(lefts, axis=1)
    total = product(left, jnp.concatenate([r[2] for r in rights], axis=0))
    for part in (1, 0):
        total = total + product(left, jnp.concatenate([r[part] for r in rights], axis=0))
    placed[...] = total


def placed_cores(pieces, group, count_x, count_y):
    return small_call(
        lambda *refs: place_kernel(group, *refs),
        12,
        out_shape=kept((count_x, count_y)),
        in_specs=in_vmem(1),
        out_specs=in_vmem(1)[0],
        scratch_shapes=[pltpu.VMEM((8 * (pieces.shape[0] // group), LANES), jnp.float32)],
    )(pieces)


def plane_kernel(device, placed, table_x, table_y, *refs):
    *blocks, spectrum, exchange, outer = refs
    sub = lax.rem(device[0], len(blocks))
    x_dev = placed.shape[0] // len(blocks)
    for d, block in enumerate(blocks):
        outer[pl.ds(pl.multiple_of((sub ^ d) * x_dev, 8), x_dev), :] = block[...]
    density = outer[...] + placed[...]
    exchange[...] = exchange_correlation(density)
    spectrum[...] = times_table(table_times(table_x, density), table_y)


def plane_spectrum(device, placed, table_x, table_y, blocks):
    return small_call(
        plane_kernel,
        12,
        out_shape=(kept(placed.shape), kept(placed.shape)),
        in_specs=in_smem(1) + in_vmem(3 + len(blocks)),
        out_specs=in_vmem(2),
        scratch_shapes=[pltpu.VMEM(placed.shape, jnp.float32)],
    )(device, placed, table_x, table_y, *blocks)


def wave_squares(index, count):
    folded = jnp.where(index > count // 2, index - count, index)
    wave = 2.0 * math.pi / (count * spacing) * folded.astype(jnp.float32)
    return wave * wave


def column_kernel(count_z, count_x, count_y, device, values, table, out):
    rows, lanes = values.shape
    deep = rows // count_z
    transformed = table_times(table, values[...])
    row = lax.broadcasted_iota(jnp.int32, (rows, 1), 0)
    lane = lax.broadcasted_iota(jnp.int32, (1, lanes), 1)
    assert deep == 1 or lanes == count_y
    cell = (device[0] * deep + row % deep) * lanes
    square = (
        wave_squares(row // deep, count_z) + wave_squares(cell // count_y, count_x)
    ) + wave_squares(device[0] * deep * lanes % count_y + lane, count_y)
    scale = 4.0 * math.pi / float(count_z * count_x * count_y)
    kernel = jnp.where(square > 0, scale / jnp.where(square > 0, square, 1.0), 0.0)
    out[...] = table_times(table, transformed * kernel)


def column_hartree(values, table, device, counts):
    return small_call(
        lambda *refs: column_kernel(*counts, *refs),
        12,
        out_shape=kept(values.shape),
        in_specs=in_smem(1) + in_vmem(2),
        out_specs=in_vmem(1)[0],
    )(device, values, table)


def window_kernel(fragment, device, corner_table, spectrum, exchange, table_x, table_y, *refs):
    *blocks, out, wide, cut, corners, staged = refs
    scalars = pltpu.make_async_copy(corner_table, corners, staged)
    scalars.start()
    slots = out.shape[0]
    count_x, count_y = spectrum.shape
    x_dev = count_x // len(blocks)
    plane = times_table(table_times(table_x, spectrum[...]), table_y) + exchange[...]
    tall = count_x + BOX
    tiles = count_y // LANES
    for t in range(tiles):
        part = plane[:, t * LANES : (t + 1) * LANES]
        wide[t * tall : t * tall + count_x, :] = part
        wide[t * tall + count_x : (t + 1) * tall, :] = part[0:BOX]
    sub = lax.rem(device[0], len(blocks))
    for d, block in enumerate(blocks):
        for t in range(tiles):
            at = pl.multiple_of(t * tall + (sub ^ d) * x_dev, 8)
            block[:, t * LANES : (t + 1) * LANES] = wide[pl.ds(at, x_dev), :]
    lane = lax.broadcasted_iota(jnp.int32, (BOX, LANES), 1)
    scalars.wait()

    many = at_once(slots)

    def cut_windows(step, carry):
        turned = []
        for h in range(many):
            f = fragment(many * step + h, device[0])
            x, y = corners[1, f], corners[2, f]
            tile = y // LANES
            over = y - tile * LANES
            near = wide[pl.ds(tile * tall + x, BOX), :]
            far = wide[pl.ds(lax.rem(tile + 1, tiles) * tall + x, BOX), :]
            turn = lax.rem(LANES - over, LANES)
            turned.append(pltpu.roll(jnp.where(lane < over, far, near), turn, 1))
        for h in range(many):
            at = pl.multiple_of((many * step + h) * BOX, 8)
            cut[pl.ds(at, BOX), :] = turned[h]
        return carry

    repeated(slots // many, cut_windows)
    count = slots * GROUPS
    flat = jnp.concatenate(
        [cut[pl.ds(r, count, stride=8), :][:, 0:BOX] for r in range(8)], axis=1
    )
    for k in range(slots):
        for g in range(GROUPS):
            out[k, :, g * WIDE : (g + 1) * WIDE] = flat[k * GROUPS + g : k * GROUPS + g + 1, :]


def plane_windows(
    device, corners, spectrum, exchange, table_x, table_y, blocks, slots, fragment
):
    count_x, count_y = spectrum.shape
    block = kept((count_x // blocks, count_y))
    return small_call(
        lambda *refs: window_kernel(fragment, *refs),
        12,
        out_shape=[block] * blocks + [kept((slots, 1, PLANE))],
        in_specs=in_smem(1) + anywhere(1) + in_vmem(4),
        out_specs=in_vmem(blocks + 1),
        scratch_shapes=[
            pltpu.VMEM((count_y // LANES * (count_x + BOX), LANES), jnp.float32),
            pltpu.VMEM((slots * BOX, LANES), jnp.float32),
            pltpu.SMEM(corners.shape, jnp.int32),
            pltpu.SemaphoreType.DMA,
        ],
    )(device, corners, spectrum, exchange, table_x, table_y)


def block_kernel(device, *refs):
    *blocks, potential, copied = refs
    sub = lax.rem(device[0], len(blocks))
    copies = [
        pltpu.make_async_copy(block, potential.at[sub ^ d], copied.at[d])
        for d, block in enumerate(blocks)
    ]
    for copy in copies:
        copy.start()
    for copy in copies:
        copy.wait()


def grid_block(device, blocks):
    count = len(blocks)
    return small_call(
        block_kernel,
        4,
        out_shape=jax.ShapeDtypeStruct((count,) + blocks[0].shape, jnp.float32),
        in_specs=in_smem(1) + anywhere(count),
        out_specs=anywhere(1)[0],
        scratch_shapes=[pltpu.SemaphoreType.DMA((count,))],
    )(device, *blocks)


def output_kernel(base, tall, device, corners, windows, box, copied):
    depth = windows.shape[0]
    row = corners[0:1, :]
    own = lax.broadcasted_iota(jnp.int32, row.shape, 1) == device[0]
    first = jnp.sum(jnp.where(own, row, 0)) - base(device[0])
    copies = []
    over = lax.rem(first, tall)
    for t in range(1, BOX // tall):
        z = pl.ds(lax.rem(first - over + t * tall, depth), tall)
        i = pl.ds(t * tall - over, tall)
        copies.append(pltpu.make_async_copy(windows.at[z], box.at[i], copied.at[t]))
    for q in range(tall):
        z = jnp.where(q < over, lax.rem(first - over + BOX, depth), first - over) + q
        i = jnp.where(q < over, BOX, 0) + q - over
        copies.append(pltpu.make_async_copy(windows.at[z], box.at[i], copied.at[BOX + tall + q]))
    for copy in copies:
        copy.start()
    for copy in copies:
        copy.wait()


def box_planes(device, corners, windows, tall, base):
    return small_call(
        lambda *refs: output_kernel(base, tall, *refs),
        4,
        out_shape=jax.ShapeDtypeStruct((BOX, 1, PLANE), jnp.float32),
        in_specs=in_smem(1) + in_vmem(1) + anywhere(1),
        out_specs=anywhere(1)[0],
        scratch_shapes=[pltpu.SemaphoreType.DMA((BOX + 2 * tall,))],
    )(device, corners, windows)


def body(orbitals, occupations, patch_sign, corners, core_span, outer_density):
    slab_count = lax.axis_size("slab")
    sub_count = lax.axis_size("sub")
    devices = slab_count * sub_count
    z_dev, x_dev, count_y = outer_density.shape
    count_x = x_dev * sub_count
    count_z = z_dev * slab_count
    device = lax.axis_index("slab") * sub_count + lax.axis_index("sub")
    table_x = hartley(count_x)
    table_y = hartley(count_y)
    per_device = count_x * count_y // devices
    deep = max(1, per_device // count_y)
    table_z = hartley(count_z, deep)

    device = jnp.reshape(device, (1,))
    assert z_dev == sub_count
    reach = (BOX + z_dev - 2) // z_dev + 1
    if slab_count <= reach:
        slots, group = devices, KINDS

        def base(own):
            return 0

        def fragment(slot, own):
            return slot

        def spread(pieces):
            return lax.all_to_all(pieces, AXES, 0, 0, tiled=True)

        collect = spread
    else:
        slots, group = reach * sub_count, sub_count

        def base(own):
            return own - lax.rem(own, sub_count)

        def fragment(slot, own):
            away = slot // sub_count * sub_count
            return lax.rem(base(own) - away + devices, devices) + lax.rem(slot, sub_count)

        def passed(pieces, sign):
            pieces = pieces.reshape((reach, sub_count) + pieces.shape[1:])
            pieces = lax.all_to_all(pieces, "sub", 1, 1, tiled=True)
            moved = [pieces[0]]
            for d in range(1, reach):
                ring = [(i, (i + sign * d) % slab_count) for i in range(slab_count)]
                moved.append(lax.ppermute(pieces[d], "slab", ring))
            return jnp.concatenate(moved, axis=0)

        def spread(pieces):
            return passed(pieces, 1)

        def collect(pieces):
            return passed(pieces, -1)

    counts = (count_z, count_x, count_y)
    corners = corners.T
    arguments = [
        pltpu.with_memory_space_constraint(argument, pltpu.HBM)
        for argument in (corners, core_span, occupations, orbitals, outer_density)
    ]

    def swapped(blocks):
        return [
            lax.ppermute(block, "sub", [(i, i ^ d) for i in range(sub_count)]) if d else block
            for d, block in enumerate(blocks)
        ]

    pieces, *blocks = core_pieces(device, *arguments, slots, base, counts)
    blocks = swapped(blocks)
    pieces = spread(pieces)
    placed = placed_cores(pieces, group, count_x, count_y)
    spectrum, exchange = plane_spectrum(device, placed, table_x, table_y, blocks)
    chunk = (devices, deep, per_device // deep)
    spectrum = lax.all_to_all(spectrum.reshape(chunk), AXES, 0, 0, tiled=True)
    spectrum = column_hartree(
        spectrum.reshape(devices * deep, per_device // deep), table_z, device, counts
    )
    spectrum = lax.all_to_all(spectrum.reshape(chunk), AXES, 0, 0, tiled=True)
    *blocks, windows = plane_windows(
        device,
        corners,
        spectrum.reshape(count_x, count_y),
        exchange,
        table_x,
        table_y,
        sub_count,
        slots,
        fragment,
    )
    blocks = swapped(blocks)
    windows = collect(windows)
    potential = grid_block(device, blocks)
    box = box_planes(device, corners, windows, z_dev, base)
    return (box.reshape(1, BOX * PLANE), potential)


def solution(mesh):
    placed = (
        P(("slab", "sub"), None, None),
        P(("slab", "sub"), None),
        P(("slab", "sub")),
        P(),
        P(("slab", "sub"), None),
        P("slab", "sub", None),
    )
    return jax.shard_map(
        body,
        mesh=mesh,
        in_specs=placed,
        out_specs=(P(("slab", "sub"), None), P("slab", "sub", None)),
        check_vma=False,
    )
```
